32 devices in a mesh: dp: 8 (over y, x, core), mp: 4 (over z).
Axes of the slice: x: 2, y: 2, z: 4, core: 2. Of those that a mesh axis runs over, the one named last changes fastest.
Arguments:
- block_input: bfloat16 [16384, 768], P(('dp', 'mp')), may hold values from -6 to 6
- clusters: int32 [16384, 12], P(('dp', 'mp')), may hold values from 0 to 99
- ln1_gain: float32 [768], replicated, may hold values from 0.5 to 1.5
- ln1_bias: float32 [768], replicated, may hold values from -1.75 to 1.75
- w_query: bfloat16 [768, 768], replicated, may hold values from -0.875 to 0.875
- query_bias: float32 [768], replicated, may hold values from -8 to 8
- w_keyval: bfloat16 [768, 1536], replicated, may hold values from -0.21875 to 0.21875
- value_bias: float32 [768], replicated, may hold values from -0.625 to 0.625
- w_out: bfloat16 [768, 768], replicated, may hold values from -1.75 to 1.75
- out_bias: float32 [768], replicated, may hold values from -1.75 to 1.75
- ln2_gain: float32 [768], replicated, may hold values from 0.5 to 1.5
- ln2_bias: float32 [768], replicated, may hold values from -1.75 to 1.75
- w_up: bfloat16 [768, 3072], P(None, 'mp'), may hold values from -0.21875 to 0.21875
- up_bias: bfloat16 [3072], P('mp'), may hold values from -1.75 to 1.75
- w_down: bfloat16 [3072, 768], P('mp'), may hold values from -0.109375 to 0.109375
- down_bias: float32 [768], replicated, may hold values from -1.75 to 1.75
- cotangent: bfloat16 [16384, 768], P(('dp', 'mp')), may hold values from -6 to 6
Outputs:
- block_output: bfloat16 [16384, 768], P(('dp', 'mp'))
- input_grad: float32 [16384, 768], P(('dp', 'mp'))
- ln1_gain_grad: float32 [768], P(('dp', 'mp'))
- ln1_bias_grad: float32 [768], P(('dp', 'mp'))
- w_query_grad: float32 [768, 768], P(('dp', 'mp'))
- query_bias_grad: float32 [768], P(('dp', 'mp'))
- w_keyval_grad: float32 [768, 1536], P(('dp', 'mp'))
- value_bias_grad: float32 [768], P(('dp', 'mp'))
- w_out_grad: float32 [768, 768], P(('dp', 'mp'))
- out_bias_grad: float32 [768], P(('dp', 'mp'))
- ln2_gain_grad: float32 [768], P(('dp', 'mp'))
- ln2_bias_grad: float32 [768], P(('dp', 'mp'))
- w_up_grad: float32 [768, 3072], P('dp', 'mp')
- up_bias_grad: float32 [3072], P(('dp', 'mp'))
- w_down_grad: float32 [3072, 768], P('mp', 'dp')
- down_bias_grad: float32 [768], P(('dp', 'mp'))
The draws below stay inside these ranges and needn't reach their ends.
All inputs are finite; a program needn't handle non-finite values.
Results may differ from the reference program's by a relative error of at most 0.03.
Values may be sent and summed in bfloat16 or wider, within the bound.
A program may use at most 128 MiB of HBM per device.

```python
import math
import jax
import jax.numpy as jnp
import numpy as np
from jax import lax

D = 768
HEADS = 12
HEAD_DIM = 64
FF = 3072
CLUSTERS = 100
LEN = 2048
SEQS = 8
TOKENS = 16384


def place_ends(values, key, least, largest):
    shape = values.shape
    index_at = [jax.random.randint(jax.random.fold_in(key, axis), (), 0, shape[axis]) for axis in range(len(shape))]
    values = values.at[tuple(index_at)].set(least)
    longest = shape.index(max(shape))
    index_at[longest] = (index_at[longest] + 1) % shape[longest]
    return values.at[tuple(index_at)].set(largest)


def spiked(drawn, key, source, target, shards_of, factor):
    owner, partner = [(jnp.arange(drawn.shape[dim]) // (drawn.shape[dim] // shards_of)).reshape([-1 if axis == dim else 1 for axis in range(drawn.ndim)]) for dim in (source, target)]
    chosen = jax.random.permutation(key, shards_of)[partner]
    strong = (owner == chosen) | (owner == (partner + shards_of // 2) % shards_of)
    return jnp.where(strong, factor * drawn, drawn)


def levels(rng, extent, cuts, smallest, top_value):
    def one(axis_at, parts):
        draws = jax.random.uniform(jax.random.fold_in(jax.random.fold_in(rng, 6), axis_at), (parts,), jnp.float32, smallest / len(cuts), top_value / len(cuts))
        return jnp.repeat(jnp.exp(draws), extent[axis_at] // parts).reshape((-1,) + (1,) * (len(extent) - axis_at - 1))

    level = one(*cuts[0])
    for cut in cuts[1:]:
        level = level * one(*cut)
    return level


def rank_table(amount, lean):
    portions = [(1 << 20) // math.isqrt(standing ** lean) + 1 for standing in range(1, amount + 1)]
    scale = 1 + sum(portions) // (1 << 30)
    return np.cumsum(np.array([max(1, weight // scale) for weight in portions]))


def skewed_ids(own_key, dims, amount, lean):
    table = rank_table(amount, lean)
    pick = jax.random.randint(jax.random.fold_in(own_key, 1), dims, 0, int(table[amount - 1]))
    rank = jnp.searchsorted(jnp.asarray(table, jnp.int32), pick, side="right")
    return jax.random.permutation(jax.random.fold_in(own_key, 2), amount)[rank].astype(jnp.int32)


def bell_draw(own_key, extent, width, most, pieces=(), kind=jnp.bfloat16):
    drawn = width * jax.random.normal(own_key, extent, jnp.float32)
    if pieces:
        drawn = drawn * levels(own_key, extent, pieces, -0.22, 0.18)
    return jnp.clip(drawn, -most, most).astype(kind)


def heavy_noise(key, dims, width, most, pieces, heavy, held_as=jnp.bfloat16):
    values = width * jax.random.normal(key, dims, jnp.float32)
    if pieces:
        values = values * levels(key, dims, pieces, -0.22, 0.18)
    return jnp.clip(spiked(values, jax.random.fold_in(key, 3), *heavy), -most, most).astype(held_as)


def setup_inputs(seed: int = 0) -> dict:
    streams_of = jax.random.split(jax.random.key(seed), 18)
    block_input = bell_draw(streams_of[0], (TOKENS, D), 1.0, 6.0, ((0, 32),))
    clusters = place_ends(skewed_ids(streams_of[1], (TOKENS, HEADS), CLUSTERS, 2), jax.random.fold_in(streams_of[1], 3), 0, CLUSTERS - 1).astype(jnp.int32)
    ln1_gain = jnp.clip(1.0 + 0.1 * jax.random.normal(streams_of[2], (D,), jnp.float32), 0.5, 1.5)
    ln1_bias = bell_draw(streams_of[3], (D,), 0.3, 1.75, (), jnp.float32)
    w_query = bell_draw(streams_of[4], (D, D), (D // 16) ** -0.5, 0.875)
    query_bias = bell_draw(streams_of[5], (D,), 1.5, 8.0, (), jnp.float32)
    w_keyval = bell_draw(streams_of[6], (D, 2 * D), D ** -0.5, 0.21875)
    value_bias = bell_draw(streams_of[7], (D,), 0.1, 0.625, (), jnp.float32)
    w_out = bell_draw(streams_of[8], (D, D), (D // 64) ** -0.5, 1.75)
    out_bias = bell_draw(streams_of[9], (D,), 0.3, 1.75, (), jnp.float32)
    ln2_gain = jnp.clip(1.0 + 0.1 * jax.random.normal(streams_of[10], (D,), jnp.float32), 0.5, 1.5)
    ln2_bias = bell_draw(streams_of[11], (D,), 0.3, 1.75, (), jnp.float32)
    w_up = bell_draw(streams_of[12], (D, FF), D ** -0.5, 0.21875, ((1, 4),))
    up_bias = bell_draw(streams_of[13], (FF,), 0.3, 1.75, ((0, 4),))
    w_down = bell_draw(streams_of[14], (FF, D), FF ** -0.5, 0.109375, ((0, 4),))
    down_bias = bell_draw(streams_of[15], (D,), 0.3, 1.75, (), jnp.float32)
    cotangent = heavy_noise(streams_of[16], (TOKENS, D), 1.0, 6.0, ((0, 32),), (0, 1, 32, 2.75))
    return dict(block_input=block_input, clusters=clusters, ln1_gain=ln1_gain, ln1_bias=ln1_bias, w_query=w_query, query_bias=query_bias, w_keyval=w_keyval, value_bias=value_bias, w_out=w_out, out_bias=out_bias, ln2_gain=ln2_gain, ln2_bias=ln2_bias, w_up=w_up, up_bias=up_bias, w_down=w_down, down_bias=down_bias, cotangent=cotangent)


@jax.custom_vjp
def low(v):
    return lax.optimization_barrier(v.astype(jnp.bfloat16)).astype(jnp.float32)

@jax.custom_vjp
def low_back(v):
    return v

def low_keep(v):
    return (low(v), None)

def low_pass(kept, grad):
    return (grad,)

def back_keep(v):
    return (v, None)

def back_low(kept, grad):
    return (low(grad),)
low.defvjp(low_keep, low_pass)
low_back.defvjp(back_keep, back_low)
epsilon = 1e-05

def matmul(left, right):
    return jnp.dot(left, right, precision=lax.Precision.HIGHEST)

def layer_norm(inputs, gain_vec, offset):
    center = inputs - lax.optimization_barrier(jnp.mean(inputs, axis=-1, keepdims=True))
    factor = lax.rsqrt(lax.optimization_barrier(jnp.mean(center * center, axis=-1, keepdims=True)) + epsilon)
    return center * factor * gain_vec + offset

def sequence_block(params, inputs, assigned):
    ln1_gain, ln1_bias, w_query, query_bias, w_keyval, value_bias, w_out, out_bias, ln2_gain, ln2_bias, w_up, up_bias, w_down, down_bias = params
    length = inputs.shape[0]
    first = low(layer_norm(inputs, ln1_gain, ln1_bias))
    queries = low(low_back(matmul(first, w_query) + query_bias))
    keyval = low(low_back(matmul(first, w_keyval) + jnp.concatenate([jnp.zeros_like(value_bias), value_bias])))
    membership = (assigned.T[:, None, :] == jnp.arange(CLUSTERS, dtype=jnp.int32)[None, :, None]).astype(jnp.float32)
    query_sums = jnp.einsum('hct,thd->hcd', membership, queries.reshape(length, HEADS, HEAD_DIM), precision=lax.Precision.HIGHEST)
    cluster_sizes = lax.optimization_barrier(jnp.sum(membership, axis=2))
    centroids = low(low_back(query_sums / jnp.maximum(cluster_sizes, 1.0)[:, :, None]))
    key_rows = keyval[:, :D].reshape(length, HEADS, HEAD_DIM)
    value_rows = keyval[:, D:].reshape(length, HEADS, HEAD_DIM)
    scores = low_back(HEAD_DIM ** (-0.5) * jnp.einsum('hcd,jhd->hcj', centroids, key_rows, precision=lax.Precision.HIGHEST))
    probs = jax.nn.softmax(scores, axis=-1)
    summary = low(low_back(jnp.einsum('hcj,jhd->hcd', low(probs), value_rows, precision=lax.Precision.HIGHEST)))
    spread = low_back(jnp.einsum('hct,hcd->thd', membership, summary, precision=lax.Precision.HIGHEST).reshape(length, D))
    attended = low_back(matmul(spread, w_out) + out_bias)
    middle = inputs + attended
    second = low(layer_norm(middle, ln2_gain, ln2_bias))
    before = low_back(matmul(second, w_up) + up_bias)
    hidden = low(jax.nn.gelu(before, approximate=False))
    result = low_back(matmul(hidden, w_down) + down_bias)
    return middle + result

def reference(block_input, clusters, ln1_gain, ln1_bias, w_query, query_bias, w_keyval, value_bias, w_out, out_bias, ln2_gain, ln2_bias, w_up, up_bias, w_down, down_bias, cotangent):
    params = tuple((item.astype(jnp.float32) for item in (ln1_gain, ln1_bias, w_query, query_bias, w_keyval, value_bias, w_out, out_bias, ln2_gain, ln2_bias, w_up, up_bias, w_down, down_bias)))
    inputs = block_input.astype(jnp.float32).reshape(SEQS, LEN, D)
    assigned = clusters.reshape(SEQS, LEN, HEADS)

    def forward(weights, acts):

        def mapped(pair):
            return sequence_block(weights, pair[0], pair[1])
        return lax.map(jax.checkpoint(mapped), (acts, assigned))
    output, pullback = jax.vjp(forward, params, inputs)
    param_grads, input_grad = pullback(cotangent.astype(jnp.float32).reshape(SEQS, LEN, D))
    return (output.reshape(TOKENS, D).astype(jnp.bfloat16), input_grad.reshape(TOKENS, D), param_grads[0], param_grads[1], param_grads[2], param_grads[3], param_grads[4], param_grads[5], param_grads[6], param_grads[7], param_grads[8], param_grads[9], param_grads[10], param_grads[11], param_grads[12], param_grads[13])
```

```python
import math

import jax
import jax.numpy as jnp
from jax import lax
from jax.sharding import PartitionSpec as P

CLUSTERS = 100


epsilon = 1e-05


def norm_forward(inputs, gain_vec, offset):
    center = inputs - jnp.mean(inputs, axis=-1, keepdims=True)
    factor = lax.rsqrt(jnp.mean(center * center, axis=-1, keepdims=True) + epsilon)
    standard = center * factor
    return (standard * gain_vec + offset, standard, factor)


def norm_backward(upstream, standard, factor, gain_vec):
    scaled = upstream * gain_vec
    centred = scaled - jnp.mean(scaled, axis=-1, keepdims=True)
    centred = centred - standard * jnp.mean(scaled * standard, axis=-1, keepdims=True)
    return (factor * centred, jnp.sum(upstream * standard, axis=0), jnp.sum(upstream, axis=0))


def gelu_parts(before):
    cumulative = 0.5 * (1.0 + jax.scipy.special.erf(before / math.sqrt(2.0)))
    density = jnp.exp(-0.5 * before * before) / math.sqrt(2.0 * math.pi)
    return (before * cumulative, cumulative + before * density)


def on_device(
    block_input,
    clusters,
    ln1_gain,
    ln1_bias,
    w_query,
    query_bias,
    w_keyval,
    value_bias,
    w_out,
    out_bias,
    ln2_gain,
    ln2_bias,
    w_up,
    up_bias,
    w_down,
    down_bias,
    cotangent,
):
    group_size = lax.axis_size("mp")
    tok_rows = block_input.shape[0]
    model_width = block_input.shape[1]
    head_count = clusters.shape[1]
    head_dim = model_width // head_count
    local_heads = head_count // group_size
    score_scale = float(head_dim) ** (-0.5)
    inputs = block_input.astype(jnp.float32)
    normed_one, standard_one, factor_one = norm_forward(inputs, ln1_gain, ln1_bias)
    first = normed_one.astype(jnp.bfloat16)
    queries = (jnp.dot(first, w_query, preferred_element_type=jnp.float32) + query_bias).astype(
        jnp.bfloat16
    )
    keyval = jnp.dot(first, w_keyval, preferred_element_type=jnp.float32)
    keyval = (keyval + jnp.concatenate([jnp.zeros_like(value_bias), value_bias])).astype(
        jnp.bfloat16
    )
    member_float = (
        clusters.T[:, None, :] == jnp.arange(CLUSTERS, dtype=jnp.int32)[None, :, None]
    ).astype(jnp.float32)
    membership = member_float.astype(jnp.bfloat16)
    query_sums = jnp.einsum(
        "hct,thd->hcd",
        membership,
        queries.reshape(tok_rows, head_count, head_dim),
        preferred_element_type=jnp.float32,
    )
    cluster_sizes = jnp.sum(member_float, axis=2)
    sums_and_sizes = lax.psum_scatter(
        jnp.concatenate([query_sums, cluster_sizes[:, :, None]], axis=2),
        "mp",
        scatter_dimension=0,
        tiled=True,
    )
    query_sums = sums_and_sizes[:, :, :head_dim]
    cluster_sizes = sums_and_sizes[:, :, head_dim]
    divisor = jnp.maximum(cluster_sizes, 1.0)
    centroids = (query_sums / divisor[:, :, None]).astype(jnp.bfloat16)
    packed = keyval.reshape(tok_rows, 2, group_size, local_heads * head_dim)
    arrived = lax.all_to_all(packed, "mp", split_axis=2, concat_axis=0, tiled=True)
    length = arrived.shape[0]
    key_rows = arrived[:, 0, 0].reshape(length, local_heads, head_dim)
    value_rows = arrived[:, 1, 0].reshape(length, local_heads, head_dim)
    scores = score_scale * jnp.einsum(
        "hcd,jhd->hcj", centroids, key_rows, preferred_element_type=jnp.float32
    )
    score_peak = jnp.max(scores, axis=-1, keepdims=True)
    exponent = jnp.exp(scores - score_peak)
    denominator = jnp.sum(exponent, axis=-1, keepdims=True)
    probs = exponent / denominator
    logsum = score_peak + jnp.log(denominator)
    summary = jnp.einsum(
        "hcj,jhd->hcd", probs.astype(jnp.bfloat16), value_rows, preferred_element_type=jnp.float32
    ).astype(jnp.bfloat16)
    everyone = lax.all_gather(summary, "mp", axis=0, tiled=True)
    spread = (
        jnp.einsum("hct,hcd->thd", membership, everyone, preferred_element_type=jnp.float32)
        .astype(jnp.bfloat16)
        .reshape(tok_rows, model_width)
    )
    attended = jnp.dot(spread, w_out, preferred_element_type=jnp.float32) + out_bias
    middle = inputs + attended
    normed_two, standard_two, factor_two = norm_forward(middle, ln2_gain, ln2_bias)
    second = normed_two.astype(jnp.bfloat16)
    gathered = lax.all_gather(second, "mp", axis=0, tiled=True)
    before = jnp.dot(gathered, w_up, preferred_element_type=jnp.float32) + up_bias.astype(
        jnp.float32
    )
    activated, gelu_slope = gelu_parts(before)
    hidden = activated.astype(jnp.bfloat16)
    result = lax.psum_scatter(
        jnp.dot(hidden, w_down, preferred_element_type=jnp.float32).astype(jnp.bfloat16),
        "mp",
        scatter_dimension=0,
        tiled=True,
    ).astype(jnp.float32)
    block_output = (middle + result + down_bias).astype(jnp.bfloat16)
    upstream = cotangent.astype(jnp.float32)
    grad_down_bias = jnp.sum(upstream, axis=0)
    grad_rows = lax.all_gather(cotangent, "mp", axis=0, tiled=True)
    grad_down_t = jnp.einsum("td,tf->df", grad_rows, hidden, preferred_element_type=jnp.float32)
    grad_hidden = jnp.einsum("td,fd->tf", grad_rows, w_down, preferred_element_type=jnp.float32)
    grad_before = (grad_hidden * gelu_slope).astype(jnp.bfloat16)
    bias_part = jnp.sum(grad_before.astype(jnp.float32), axis=0)
    grad_up = jnp.einsum("td,tf->df", gathered, grad_before, preferred_element_type=jnp.float32)
    grad_second = lax.psum_scatter(
        jnp.einsum("tf,df->td", grad_before, w_up, preferred_element_type=jnp.float32).astype(
            jnp.bfloat16
        ),
        "mp",
        scatter_dimension=0,
        tiled=True,
    ).astype(jnp.float32)
    grad_up_bias = lax.dynamic_update_slice(
        jnp.zeros((group_size * bias_part.shape[0],), jnp.float32),
        bias_part,
        (lax.axis_index("mp") * bias_part.shape[0],),
    )
    middle_norm_grad, grad_gain_two, grad_shift_two = norm_backward(
        grad_second, standard_two, factor_two, ln2_gain
    )
    grad_middle = upstream + middle_norm_grad
    attn_grad = grad_middle.astype(jnp.bfloat16)
    grad_out_bias = jnp.sum(attn_grad.astype(jnp.float32), axis=0)
    grad_w_out = jnp.einsum("td,te->de", spread, attn_grad, preferred_element_type=jnp.float32)
    grad_spread = jnp.einsum(
        "te,de->td", attn_grad, w_out, preferred_element_type=jnp.float32
    ).astype(jnp.bfloat16)
    summary_grad = jnp.einsum(
        "hct,thd->hcd",
        membership,
        grad_spread.reshape(tok_rows, head_count, head_dim),
        preferred_element_type=jnp.float32,
    )
    summary_grad = lax.psum_scatter(
        summary_grad.astype(jnp.bfloat16), "mp", scatter_dimension=0, tiled=True
    )
    scores_again = score_scale * jnp.einsum(
        "hcd,jhd->hcj", centroids, key_rows, preferred_element_type=jnp.float32
    )
    probs_again = jnp.exp(scores_again - logsum)
    grad_values = jnp.einsum(
        "hcj,hcd->jhd",
        probs_again.astype(jnp.bfloat16),
        summary_grad,
        preferred_element_type=jnp.float32,
    )
    grad_probs = jnp.einsum(
        "hcd,jhd->hcj", summary_grad, value_rows, preferred_element_type=jnp.float32
    )
    grad_scores = probs_again * (
        grad_probs - jnp.sum(probs_again * grad_probs, axis=-1, keepdims=True)
    )
    grad_scores = grad_scores.astype(jnp.bfloat16)
    grad_centroids = (
        score_scale
        * jnp.einsum("hcj,jhd->hcd", grad_scores, key_rows, preferred_element_type=jnp.float32)
    ).astype(jnp.bfloat16)
    grad_keys = score_scale * jnp.einsum(
        "hcj,hcd->jhd", grad_scores, centroids, preferred_element_type=jnp.float32
    )
    grad_kv = jnp.concatenate(
        [
            grad_keys.reshape(length, local_heads * head_dim),
            grad_values.reshape(length, local_heads * head_dim),
        ],
        axis=1,
    ).astype(jnp.bfloat16)
    kv_width = 2 * local_heads * head_dim
    per_member = (grad_centroids.astype(jnp.float32) / divisor[:, :, None]).astype(jnp.bfloat16)
    member_rows = per_member.size // kv_width
    outgoing = jnp.concatenate(
        [
            grad_kv.reshape(group_size, tok_rows, kv_width),
            jnp.broadcast_to(
                per_member.reshape(1, member_rows, kv_width), (group_size, member_rows, kv_width)
            ),
        ],
        axis=1,
    )
    incoming = lax.all_to_all(outgoing, "mp", split_axis=0, concat_axis=0, tiled=True)
    returned = incoming[:, :tok_rows].reshape(group_size, tok_rows, 2, local_heads * head_dim)
    grad_keyval = returned.transpose(1, 2, 0, 3).reshape(tok_rows, 2 * model_width)
    all_member = (
        incoming[:, tok_rows:]
        .reshape(head_count, CLUSTERS, head_dim)
        .astype(jnp.float32)
    )
    grad_queries = jnp.einsum(
        "hct,hcd->thd", member_float, all_member, precision=lax.Precision.HIGHEST
    )
    grad_queries = grad_queries.reshape(tok_rows, model_width).astype(jnp.bfloat16)
    grad_query_bias = jnp.sum(grad_queries.astype(jnp.float32), axis=0)
    grad_value_bias = jnp.sum(grad_keyval[:, model_width:].astype(jnp.float32), axis=0)
    grad_w_query = jnp.einsum("td,te->de", first, grad_queries, preferred_element_type=jnp.float32)
    grad_w_keyval = jnp.einsum("td,te->de", first, grad_keyval, preferred_element_type=jnp.float32)
    grad_first = jnp.einsum("te,de->td", grad_queries, w_query, preferred_element_type=jnp.float32)
    grad_first = grad_first + jnp.einsum(
        "te,de->td", grad_keyval, w_keyval, preferred_element_type=jnp.float32
    )
    input_norm_grad, grad_gain_one, grad_shift_one = norm_backward(
        grad_first, standard_one, factor_one, ln1_gain
    )
    input_grad = grad_middle + input_norm_grad
    vectors = jnp.stack(
        [
            grad_gain_one,
            grad_shift_one,
            grad_query_bias,
            grad_value_bias,
            grad_out_bias,
            grad_gain_two,
            grad_shift_two,
            grad_down_bias,
        ],
        axis=1,
    )
    up_bias_cols = grad_up_bias.reshape(model_width, -1)
    packed_grads = jnp.concatenate(
        [grad_w_query, grad_w_keyval, grad_w_out, vectors, up_bias_cols], axis=1
    )
    reduced = lax.psum_scatter(
        lax.psum_scatter(packed_grads, "dp", scatter_dimension=0, tiled=True),
        "mp",
        scatter_dimension=0,
        tiled=True,
    )
    ff_grads = lax.psum_scatter(
        jnp.concatenate([grad_up, grad_down_t], axis=1), "dp", scatter_dimension=0, tiled=True
    )
    ff_width = grad_up.shape[1]
    up_share = ff_grads[:, :ff_width]
    down_share = ff_grads[:, ff_width:].T
    col = 0
    pieces = []
    for width in (model_width, 2 * model_width, model_width):
        pieces.append(reduced[:, col : col + width])
        col += width
    vec = [reduced[:, col + i] for i in range(8)]
    col += 8
    up_bias_share = reduced[:, col:].reshape(-1)
    return (
        block_output,
        input_grad,
        vec[0],
        vec[1],
        pieces[0],
        vec[2],
        pieces[1],
        vec[3],
        pieces[2],
        vec[4],
        vec[5],
        vec[6],
        up_share,
        up_bias_share,
        down_share,
        vec[7],
    )


def solution(mesh):
    placed = (
        P(("dp", "mp"), None),
        P(("dp", "mp"), None),
        P(),
        P(),
        P(),
        P(),
        P(),
        P(),
        P(),
        P(),
        P(),
        P(),
        P(None, "mp"),
        P("mp"),
        P("mp", None),
        P(),
        P(("dp", "mp"), None),
    )
    return jax.shard_map(
        on_device,
        mesh=mesh,
        in_specs=placed,
        out_specs=(
            P(("dp", "mp"), None),
            P(("dp", "mp"), None),
            P(("dp", "mp")),
            P(("dp", "mp")),
            P(("dp", "mp"), None),
            P(("dp", "mp")),
            P(("dp", "mp"), None),
            P(("dp", "mp")),
            P(("dp", "mp"), None),
            P(("dp", "mp")),
            P(("dp", "mp")),
            P(("dp", "mp")),
            P("dp", "mp"),
            P(("dp", "mp")),
            P("mp", "dp"),
            P(("dp", "mp")),
        ),
        check_vma=False,
    )
```

```python
import math

import jax
import jax.numpy as jnp
from jax import lax
from jax.sharding import PartitionSpec as P


CLUSTERS = 100


epsilon = 1e-05


def norm_forward(inputs, gain_vec, offset):
    center = inputs - jnp.mean(inputs, axis=-1, keepdims=True)
    factor = lax.rsqrt(jnp.mean(center * center, axis=-1, keepdims=True) + epsilon)
    standard = center * factor
    return (standard * gain_vec + offset, standard, factor)


def norm_backward(upstream, standard, factor, gain_vec):
    scaled = upstream * gain_vec
    centred = scaled - jnp.mean(scaled, axis=-1, keepdims=True)
    centred = centred - standard * jnp.mean(scaled * standard, axis=-1, keepdims=True)
    return (factor * centred, jnp.sum(upstream * standard, axis=0), jnp.sum(upstream, axis=0))


def gelu_parts(before):
    cumulative = 0.5 * (1.0 + jax.scipy.special.erf(before / math.sqrt(2.0)))
    density = jnp.exp(-0.5 * before * before) / math.sqrt(2.0 * math.pi)
    return (before * cumulative, cumulative + before * density)


def ring_shift(x, group_size):
    return lax.ppermute(x, "mp", [(i, (i + 1) % group_size) for i in range(group_size)])


def ring_gather(x, group_size):
    me = lax.axis_index("mp")
    out = jnp.zeros((group_size,) + x.shape, x.dtype)
    out = lax.dynamic_update_index_in_dim(out, x, me, 0)
    cur = x
    for step in range(1, group_size):
        cur = ring_shift(cur, group_size)
        out = lax.dynamic_update_index_in_dim(
            out, cur, jnp.remainder(me + group_size - step, group_size), 0
        )
    return out.reshape((group_size * x.shape[0],) + x.shape[1:])


def ring_reduce(partial, group_size, wire_dtype):
    me = lax.axis_index("mp")
    blocks = partial.reshape((group_size, -1) + partial.shape[1:])

    def block(owner):
        return lax.dynamic_index_in_dim(
            blocks, jnp.remainder(owner + 2 * group_size, group_size), 0, keepdims=False
        )

    acc = block(me - 1).astype(wire_dtype)
    for step in range(1, group_size - 1):
        arrived = ring_shift(acc, group_size)
        acc = (arrived.astype(jnp.float32) + block(me - 1 - step)).astype(wire_dtype)
    arrived = ring_shift(acc, group_size)
    return arrived.astype(jnp.float32) + block(me)


def scatter_sum(partial, group_size):
    pieces = partial.reshape((group_size, -1) + partial.shape[1:])
    arrived = lax.all_to_all(pieces, "mp", split_axis=0, concat_axis=0, tiled=True)
    return jnp.sum(arrived, axis=0)


def broadcast_gather(local, group_size):
    sent = jnp.broadcast_to(local[None], (group_size,) + local.shape)
    arrived = lax.all_to_all(sent, "mp", split_axis=0, concat_axis=0, tiled=True)
    return arrived.reshape((group_size * local.shape[0],) + local.shape[1:])


def block_body(
    block_input,
    clusters,
    ln1_gain,
    ln1_bias,
    w_query,
    query_bias,
    w_keyval,
    value_bias,
    w_out,
    out_bias,
    ln2_gain,
    ln2_bias,
    w_up,
    up_bias,
    w_down,
    down_bias,
    cotangent,
):
    group_size = lax.axis_size("mp")
    tok_rows = block_input.shape[0]
    model_width = block_input.shape[1]
    head_count = clusters.shape[1]
    head_dim = model_width // head_count
    local_heads = head_count // group_size
    score_scale = float(head_dim) ** (-0.5)

    grad_rows = ring_gather(cotangent, group_size)

    inputs = block_input.astype(jnp.float32)
    normed_one, standard_one, factor_one = norm_forward(inputs, ln1_gain, ln1_bias)
    first = normed_one.astype(jnp.bfloat16)
    queries = (
        jnp.dot(first, w_query, preferred_element_type=jnp.float32) + query_bias
    ).astype(jnp.bfloat16)
    keyval = jnp.dot(first, w_keyval, preferred_element_type=jnp.float32)
    keyval = (keyval + jnp.concatenate([jnp.zeros_like(value_bias), value_bias])).astype(
        jnp.bfloat16
    )
    member_float = (
        clusters.T[:, None, :] == jnp.arange(CLUSTERS, dtype=jnp.int32)[None, :, None]
    ).astype(jnp.float32)
    membership = member_float.astype(jnp.bfloat16)
    query_sums = jnp.einsum(
        "hct,thd->hcd",
        membership,
        queries.reshape(tok_rows, head_count, head_dim),
        preferred_element_type=jnp.float32,
    )
    cluster_sizes = jnp.sum(member_float, axis=2)
    packed = keyval.reshape(tok_rows, 2, group_size, local_heads * head_dim)

    sums_and_sizes = scatter_sum(
        jnp.concatenate([query_sums, cluster_sizes[:, :, None]], axis=2), group_size
    )
    arrived = lax.all_to_all(packed, "mp", split_axis=2, concat_axis=0, tiled=True)

    query_sums = sums_and_sizes[:, :, :head_dim]
    cluster_sizes = sums_and_sizes[:, :, head_dim]
    divisor = jnp.maximum(cluster_sizes, 1.0)
    centroids = (query_sums / divisor[:, :, None]).astype(jnp.bfloat16)
    length = arrived.shape[0]
    key_rows = arrived[:, 0, 0].reshape(length, local_heads, head_dim)
    value_rows = arrived[:, 1, 0].reshape(length, local_heads, head_dim)
    scores = score_scale * jnp.einsum(
        "hcd,jhd->hcj", centroids, key_rows, preferred_element_type=jnp.float32
    )
    score_peak = jnp.max(scores, axis=-1, keepdims=True)
    exponent = jnp.exp(scores - score_peak)
    denominator = jnp.sum(exponent, axis=-1, keepdims=True)
    probs = exponent / denominator
    logsum = score_peak + jnp.log(denominator)
    summary = jnp.einsum(
        "hcj,jhd->hcd",
        probs.astype(jnp.bfloat16),
        value_rows,
        preferred_element_type=jnp.float32,
    ).astype(jnp.bfloat16)

    everyone = broadcast_gather(summary, group_size)

    spread = (
        jnp.einsum("hct,hcd->thd", membership, everyone, preferred_element_type=jnp.float32)
        .astype(jnp.bfloat16)
        .reshape(tok_rows, model_width)
    )
    attended = jnp.dot(spread, w_out, preferred_element_type=jnp.float32) + out_bias
    middle = inputs + attended
    normed_two, standard_two, factor_two = norm_forward(middle, ln2_gain, ln2_bias)
    second = normed_two.astype(jnp.bfloat16)
    residual = lax.optimization_barrier(middle + down_bias)

    gathered = lax.all_gather(second, "mp", axis=0, tiled=True)

    before = jnp.dot(gathered, w_up, preferred_element_type=jnp.float32) + up_bias.astype(
        jnp.float32
    )
    activated, gelu_slope = gelu_parts(before)
    hidden = activated.astype(jnp.bfloat16)
    grad_hidden = jnp.einsum("td,fd->tf", grad_rows, w_down, preferred_element_type=jnp.float32)
    grad_before = (grad_hidden * gelu_slope).astype(jnp.bfloat16)
    grad_second = lax.psum_scatter(
        jnp.einsum("tf,df->td", grad_before, w_up, preferred_element_type=jnp.float32).astype(
            jnp.bfloat16
        ),
        "mp",
        scatter_dimension=0,
        tiled=True,
    ).astype(jnp.float32)

    out_partial = jnp.dot(hidden, w_down, preferred_element_type=jnp.float32)
    result = ring_reduce(out_partial, group_size, jnp.bfloat16)
    block_output = (residual + result).astype(jnp.bfloat16)

    upstream = cotangent.astype(jnp.float32)
    grad_down_bias = jnp.sum(upstream, axis=0)
    grad_down_t = jnp.einsum("td,tf->df", grad_rows, hidden, preferred_element_type=jnp.float32)
    bias_part = jnp.sum(grad_before.astype(jnp.float32), axis=0)
    grad_up = jnp.einsum("td,tf->df", gathered, grad_before, preferred_element_type=jnp.float32)
    grad_up_bias = lax.dynamic_update_slice(
        jnp.zeros((group_size * bias_part.shape[0],), jnp.float32),
        bias_part,
        (lax.axis_index("mp") * bias_part.shape[0],),
    )
    ff_grads = lax.psum_scatter(
        jnp.concatenate([grad_up, grad_down_t], axis=1), "dp", scatter_dimension=0, tiled=True
    )

    middle_norm_grad, grad_gain_two, grad_shift_two = norm_backward(
        grad_second, standard_two, factor_two, ln2_gain
    )
    grad_middle = upstream + middle_norm_grad
    attn_grad = grad_middle.astype(jnp.bfloat16)
    grad_out_bias = jnp.sum(attn_grad.astype(jnp.float32), axis=0)
    grad_w_out = jnp.einsum("td,te->de", spread, attn_grad, preferred_element_type=jnp.float32)
    grad_spread = jnp.einsum(
        "te,de->td", attn_grad, w_out, preferred_element_type=jnp.float32
    ).astype(jnp.bfloat16)
    summary_grad = jnp.einsum(
        "hct,thd->hcd",
        membership,
        grad_spread.reshape(tok_rows, head_count, head_dim),
        preferred_element_type=jnp.float32,
    )

    summary_grad = scatter_sum(summary_grad, group_size).astype(jnp.bfloat16)

    scores_again = score_scale * jnp.einsum(
        "hcd,jhd->hcj", centroids, key_rows, preferred_element_type=jnp.float32
    )
    probs_again = jnp.exp(scores_again - logsum)
    grad_values = jnp.einsum(
        "hcj,hcd->jhd",
        probs_again.astype(jnp.bfloat16),
        summary_grad,
        preferred_element_type=jnp.float32,
    )
    grad_probs = jnp.einsum(
        "hcd,jhd->hcj", summary_grad, value_rows, preferred_element_type=jnp.float32
    )
    grad_scores = probs_again * (
        grad_probs - jnp.sum(probs_again * grad_probs, axis=-1, keepdims=True)
    )
    grad_scores = grad_scores.astype(jnp.bfloat16)
    grad_centroids = (
        score_scale
        * jnp.einsum("hcj,jhd->hcd", grad_scores, key_rows, preferred_element_type=jnp.float32)
    ).astype(jnp.bfloat16)
    grad_keys = score_scale * jnp.einsum(
        "hcj,hcd->jhd", grad_scores, centroids, preferred_element_type=jnp.float32
    )
    grad_kv = jnp.concatenate(
        [
            grad_keys.reshape(length, local_heads * head_dim),
            grad_values.reshape(length, local_heads * head_dim),
        ],
        axis=1,
    ).astype(jnp.bfloat16)
    kv_width = 2 * local_heads * head_dim
    per_member = (grad_centroids.astype(jnp.float32) / divisor[:, :, None]).astype(
        jnp.bfloat16
    )
    member_rows = per_member.size // kv_width
    outgoing = jnp.concatenate(
        [
            grad_kv.reshape(group_size, tok_rows, kv_width),
            jnp.broadcast_to(
                per_member.reshape(1, member_rows, kv_width),
                (group_size, member_rows, kv_width),
            ),
        ],
        axis=1,
    )

    incoming = lax.all_to_all(outgoing, "mp", split_axis=0, concat_axis=0, tiled=True)

    returned = incoming[:, :tok_rows].reshape(group_size, tok_rows, 2, local_heads * head_dim)
    grad_keyval = returned.transpose(1, 2, 0, 3).reshape(tok_rows, 2 * model_width)
    all_member = (
        incoming[:, tok_rows:].reshape(head_count, CLUSTERS, head_dim).astype(jnp.float32)
    )
    grad_queries = jnp.einsum(
        "hct,hcd->thd", member_float, all_member, precision=lax.Precision.HIGHEST
    )
    grad_queries = grad_queries.reshape(tok_rows, model_width).astype(jnp.bfloat16)
    grad_query_bias = jnp.sum(grad_queries.astype(jnp.float32), axis=0)
    grad_value_bias = jnp.sum(grad_keyval[:, model_width:].astype(jnp.float32), axis=0)
    grad_w_query = jnp.einsum("td,te->de", first, grad_queries, preferred_element_type=jnp.float32)
    grad_w_keyval = jnp.einsum("td,te->de", first, grad_keyval, preferred_element_type=jnp.float32)
    grad_first = jnp.einsum("te,de->td", grad_queries, w_query, preferred_element_type=jnp.float32)
    grad_first = grad_first + jnp.einsum(
        "te,de->td", grad_keyval, w_keyval, preferred_element_type=jnp.float32
    )
    input_norm_grad, grad_gain_one, grad_shift_one = norm_backward(
        grad_first, standard_one, factor_one, ln1_gain
    )
    input_grad = grad_middle + input_norm_grad
    vectors = jnp.stack(
        [
            grad_gain_one,
            grad_shift_one,
            grad_query_bias,
            grad_value_bias,
            grad_out_bias,
            grad_gain_two,
            grad_shift_two,
            grad_down_bias,
        ],
        axis=1,
    )
    up_bias_cols = grad_up_bias.reshape(model_width, -1)
    packed_grads = jnp.concatenate(
        [grad_w_query, grad_w_keyval, grad_w_out, vectors, up_bias_cols], axis=1
    )

    reduced = scatter_sum(
        lax.psum_scatter(packed_grads, "dp", scatter_dimension=0, tiled=True), group_size
    )
    ff_width = grad_up.shape[1]
    up_share = ff_grads[:, :ff_width]
    down_share = ff_grads[:, ff_width:].T
    col = 0
    pieces = []
    for width in (model_width, 2 * model_width, model_width):
        pieces.append(reduced[:, col : col + width])
        col += width
    vec = [reduced[:, col + i] for i in range(8)]
    col += 8
    up_bias_share = reduced[:, col:].reshape(-1)
    return (
        block_output,
        input_grad,
        vec[0],
        vec[1],
        pieces[0],
        vec[2],
        pieces[1],
        vec[3],
        pieces[2],
        vec[4],
        vec[5],
        vec[6],
        up_share,
        up_bias_share,
        down_share,
        vec[7],
    )


def solution(mesh):
    placed = (
        P(("dp", "mp"), None),
        P(("dp", "mp"), None),
        P(),
        P(),
        P(),
        P(),
        P(),
        P(),
        P(),
        P(),
        P(),
        P(),
        P(None, "mp"),
        P("mp"),
        P("mp", None),
        P(),
        P(("dp", "mp"), None),
    )
    return jax.shard_map(
        block_body,
        mesh=mesh,
        in_specs=placed,
        out_specs=(
            P(("dp", "mp"), None),
            P(("dp", "mp"), None),
            P(("dp", "mp")),
            P(("dp", "mp")),
            P(("dp", "mp"), None),
            P(("dp", "mp")),
            P(("dp", "mp"), None),
            P(("dp", "mp")),
            P(("dp", "mp"), None),
            P(("dp", "mp")),
            P(("dp", "mp")),
            P(("dp", "mp")),
            P("dp", "mp"),
            P(("dp", "mp")),
            P("mp", "dp"),
            P(("dp", "mp")),
        ),
        check_vma=False,
    )
```

```python
import math

import jax
import jax.numpy as jnp
from jax import lax
from jax.sharding import PartitionSpec as P


CLUSTERS = 100


epsilon = 1e-05


def norm_forward(inputs, gain_vec, offset):
    center = inputs - jnp.mean(inputs, axis=-1, keepdims=True)
    factor = lax.rsqrt(jnp.mean(center * center, axis=-1, keepdims=True) + epsilon)
    standard = center * factor
    return (standard * gain_vec + offset, standard, factor)


def norm_backward(upstream, standard, factor, gain_vec):
    scaled = upstream * gain_vec
    centred = scaled - jnp.mean(scaled, axis=-1, keepdims=True)
    centred = centred - standard * jnp.mean(scaled * standard, axis=-1, keepdims=True)
    return (factor * centred, jnp.sum(upstream * standard, axis=0), jnp.sum(upstream, axis=0))


def gelu_parts(before):
    cumulative = 0.5 * (1.0 + jax.scipy.special.erf(before / math.sqrt(2.0)))
    density = jnp.exp(-0.5 * before * before) / math.sqrt(2.0 * math.pi)
    return (before * cumulative, cumulative + before * density)


def ring_shift(x, group_size):
    return lax.ppermute(x, "mp", [(i, (i + 1) % group_size) for i in range(group_size)])


def ring_gather(x, group_size):
    me = lax.axis_index("mp")
    out = jnp.zeros((group_size,) + x.shape, x.dtype)
    out = lax.dynamic_update_index_in_dim(out, x, me, 0)
    cur = x
    for step in range(1, group_size):
        cur = ring_shift(cur, group_size)
        out = lax.dynamic_update_index_in_dim(
            out, cur, jnp.remainder(me + group_size - step, group_size), 0
        )
    return out.reshape((group_size * x.shape[0],) + x.shape[1:])


def ring_reduce(partial, group_size, wire_dtype, after):
    me = lax.axis_index("mp")
    blocks, _ = lax.optimization_barrier(
        (partial.reshape((group_size, -1) + partial.shape[1:]), after)
    )

    def block(owner):
        return lax.dynamic_index_in_dim(
            blocks, jnp.remainder(owner + 2 * group_size, group_size), 0, keepdims=False
        )

    acc = block(me - 1).astype(wire_dtype)
    for step in range(1, group_size - 1):
        arrived = ring_shift(acc, group_size)
        acc = (arrived.astype(jnp.float32) + block(me - 1 - step)).astype(wire_dtype)
    arrived = ring_shift(acc, group_size)
    return arrived.astype(jnp.float32) + block(me)


def scatter_sum(partial, group_size):
    pieces = partial.reshape((group_size, -1) + partial.shape[1:])
    arrived = lax.all_to_all(pieces, "mp", split_axis=0, concat_axis=0, tiled=True)
    return jnp.sum(arrived, axis=0)


def broadcast_gather(local, group_size):
    sent = jnp.broadcast_to(local[None], (group_size,) + local.shape)
    arrived = lax.all_to_all(sent, "mp", split_axis=0, concat_axis=0, tiled=True)
    return arrived.reshape((group_size * local.shape[0],) + local.shape[1:])


def block_body(
    block_input,
    clusters,
    ln1_gain,
    ln1_bias,
    w_query,
    query_bias,
    w_keyval,
    value_bias,
    w_out,
    out_bias,
    ln2_gain,
    ln2_bias,
    w_up,
    up_bias,
    w_down,
    down_bias,
    cotangent,
):
    group_size = lax.axis_size("mp")
    tok_rows = block_input.shape[0]
    model_width = block_input.shape[1]
    head_count = clusters.shape[1]
    head_dim = model_width // head_count
    local_heads = head_count // group_size
    score_scale = float(head_dim) ** (-0.5)

    grad_rows = ring_gather(cotangent, group_size)

    inputs = block_input.astype(jnp.float32)
    normed_one, standard_one, factor_one = norm_forward(inputs, ln1_gain, ln1_bias)
    first = normed_one.astype(jnp.bfloat16)
    queries = (
        jnp.dot(first, w_query, preferred_element_type=jnp.float32) + query_bias
    ).astype(jnp.bfloat16)
    keyval = jnp.dot(first, w_keyval, preferred_element_type=jnp.float32)
    keyval = (keyval + jnp.concatenate([jnp.zeros_like(value_bias), value_bias])).astype(
        jnp.bfloat16
    )
    member_float = (
        clusters.T[:, None, :] == jnp.arange(CLUSTERS, dtype=jnp.int32)[None, :, None]
    ).astype(jnp.float32)
    membership = member_float.astype(jnp.bfloat16)
    query_sums = jnp.einsum(
        "hct,thd->hcd",
        membership,
        queries.reshape(tok_rows, head_count, head_dim),
        preferred_element_type=jnp.float32,
    )
    cluster_sizes = jnp.sum(member_float, axis=2)
    packed = keyval.reshape(tok_rows, 2, group_size, local_heads * head_dim)

    sums_and_sizes = scatter_sum(
        jnp.concatenate([query_sums, cluster_sizes[:, :, None]], axis=2), group_size
    )
    arrived = lax.all_to_all(packed, "mp", split_axis=2, concat_axis=0, tiled=True)

    query_sums = sums_and_sizes[:, :, :head_dim]
    cluster_sizes = sums_and_sizes[:, :, head_dim]
    divisor = jnp.maximum(cluster_sizes, 1.0)
    centroids = (query_sums / divisor[:, :, None]).astype(jnp.bfloat16)
    length = arrived.shape[0]
    key_rows = arrived[:, 0, 0].reshape(length, local_heads, head_dim)
    value_rows = arrived[:, 1, 0].reshape(length, local_heads, head_dim)
    scores = score_scale * jnp.einsum(
        "hcd,jhd->hcj", centroids, key_rows, preferred_element_type=jnp.float32
    )
    score_peak = jnp.max(scores, axis=-1, keepdims=True)
    exponent = jnp.exp(scores - score_peak)
    denominator = jnp.sum(exponent, axis=-1, keepdims=True)
    probs = exponent / denominator
    logsum = score_peak + jnp.log(denominator)
    summary = jnp.einsum(
        "hcj,jhd->hcd",
        probs.astype(jnp.bfloat16),
        value_rows,
        preferred_element_type=jnp.float32,
    ).astype(jnp.bfloat16)

    everyone = broadcast_gather(summary, group_size)

    spread = (
        jnp.einsum("hct,hcd->thd", membership, everyone, preferred_element_type=jnp.float32)
        .astype(jnp.bfloat16)
        .reshape(tok_rows, model_width)
    )
    attended = jnp.dot(spread, w_out, preferred_element_type=jnp.float32) + out_bias
    middle = inputs + attended
    normed_two, standard_two, factor_two = norm_forward(middle, ln2_gain, ln2_bias)
    second = normed_two.astype(jnp.bfloat16)
    residual = lax.optimization_barrier(middle + down_bias)

    gathered = lax.all_gather(second, "mp", axis=0, tiled=True)

    before = jnp.dot(gathered, w_up, preferred_element_type=jnp.float32) + up_bias.astype(
        jnp.float32
    )
    activated, gelu_slope = gelu_parts(before)
    hidden = activated.astype(jnp.bfloat16)
    grad_hidden = jnp.einsum("td,fd->tf", grad_rows, w_down, preferred_element_type=jnp.float32)
    grad_before = (grad_hidden * gelu_slope).astype(jnp.bfloat16)
    grad_second = lax.psum_scatter(
        jnp.einsum("tf,df->td", grad_before, w_up, preferred_element_type=jnp.float32).astype(
            jnp.bfloat16
        ),
        "mp",
        scatter_dimension=0,
        tiled=True,
    ).astype(jnp.float32)

    out_partial = jnp.dot(hidden, w_down, preferred_element_type=jnp.float32)

    upstream = cotangent.astype(jnp.float32)
    grad_down_bias = jnp.sum(upstream, axis=0)
    grad_down_t = jnp.einsum("td,tf->df", grad_rows, hidden, preferred_element_type=jnp.float32)
    bias_part = jnp.sum(grad_before.astype(jnp.float32), axis=0)
    grad_up = jnp.einsum("td,tf->df", gathered, grad_before, preferred_element_type=jnp.float32)
    grad_up_bias = lax.dynamic_update_slice(
        jnp.zeros((group_size * bias_part.shape[0],), jnp.float32),
        bias_part,
        (lax.axis_index("mp") * bias_part.shape[0],),
    )
    ff_grads = lax.psum_scatter(
        jnp.stack([grad_up, grad_down_t]), "dp", scatter_dimension=1, tiled=True
    )

    middle_norm_grad, grad_gain_two, grad_shift_two = norm_backward(
        grad_second, standard_two, factor_two, ln2_gain
    )
    grad_middle = upstream + middle_norm_grad
    attn_grad = grad_middle.astype(jnp.bfloat16)
    grad_out_bias = jnp.sum(attn_grad.astype(jnp.float32), axis=0)
    grad_w_out = jnp.einsum("td,te->de", spread, attn_grad, preferred_element_type=jnp.float32)
    grad_spread = jnp.einsum(
        "te,de->td", attn_grad, w_out, preferred_element_type=jnp.float32
    ).astype(jnp.bfloat16)
    summary_grad = jnp.einsum(
        "hct,thd->hcd",
        membership,
        grad_spread.reshape(tok_rows, head_count, head_dim),
        preferred_element_type=jnp.float32,
    )

    summary_grad = scatter_sum(summary_grad, group_size).astype(jnp.bfloat16)

    scores_again = score_scale * jnp.einsum(
        "hcd,jhd->hcj", centroids, key_rows, preferred_element_type=jnp.float32
    )
    probs_again = jnp.exp(scores_again - logsum)
    grad_values = jnp.einsum(
        "hcj,hcd->jhd",
        probs_again.astype(jnp.bfloat16),
        summary_grad,
        preferred_element_type=jnp.float32,
    )
    grad_probs = jnp.einsum(
        "hcd,jhd->hcj", summary_grad, value_rows, preferred_element_type=jnp.float32
    )
    grad_scores = probs_again * (
        grad_probs - jnp.sum(probs_again * grad_probs, axis=-1, keepdims=True)
    )
    grad_scores = grad_scores.astype(jnp.bfloat16)
    grad_centroids = (
        score_scale
        * jnp.einsum("hcj,jhd->hcd", grad_scores, key_rows, preferred_element_type=jnp.float32)
    ).astype(jnp.bfloat16)
    grad_keys = score_scale * jnp.einsum(
        "hcj,hcd->jhd", grad_scores, centroids, preferred_element_type=jnp.float32
    )
    grad_kv = jnp.concatenate(
        [
            grad_keys.reshape(length, local_heads * head_dim),
            grad_values.reshape(length, local_heads * head_dim),
        ],
        axis=1,
    ).astype(jnp.bfloat16)
    kv_width = 2 * local_heads * head_dim
    per_member = (grad_centroids.astype(jnp.float32) / divisor[:, :, None]).astype(
        jnp.bfloat16
    )
    member_rows = per_member.size // kv_width
    outgoing = jnp.concatenate(
        [
            grad_kv.reshape(group_size, tok_rows, kv_width),
            jnp.broadcast_to(
                per_member.reshape(1, member_rows, kv_width),
                (group_size, member_rows, kv_width),
            ),
        ],
        axis=1,
    )

    incoming = lax.all_to_all(outgoing, "mp", split_axis=0, concat_axis=0, tiled=True)

    result = ring_reduce(out_partial, group_size, jnp.bfloat16, incoming)
    block_output = (residual + result).astype(jnp.bfloat16)

    returned = incoming[:, :tok_rows].reshape(group_size, tok_rows, 2, local_heads * head_dim)
    grad_keyval = returned.transpose(1, 2, 0, 3).reshape(tok_rows, 2 * model_width)
    all_member = (
        incoming[:, tok_rows:].reshape(head_count, CLUSTERS, head_dim).astype(jnp.float32)
    )
    grad_queries = jnp.einsum(
        "hct,hcd->thd", member_float, all_member, precision=lax.Precision.HIGHEST
    )
    grad_queries = grad_queries.reshape(tok_rows, model_width).astype(jnp.bfloat16)
    grad_query_bias = jnp.sum(grad_queries.astype(jnp.float32), axis=0)
    grad_value_bias = jnp.sum(grad_keyval[:, model_width:].astype(jnp.float32), axis=0)
    grad_w_query = jnp.einsum("td,te->de", first, grad_queries, preferred_element_type=jnp.float32)
    grad_w_keyval = jnp.einsum("td,te->de", first, grad_keyval, preferred_element_type=jnp.float32)
    grad_first = jnp.einsum("te,de->td", grad_queries, w_query, preferred_element_type=jnp.float32)
    grad_first = grad_first + jnp.einsum(
        "te,de->td", grad_keyval, w_keyval, preferred_element_type=jnp.float32
    )
    input_norm_grad, grad_gain_one, grad_shift_one = norm_backward(
        grad_first, standard_one, factor_one, ln1_gain
    )
    input_grad = grad_middle + input_norm_grad
    vectors = jnp.stack(
        [
            grad_gain_one,
            grad_shift_one,
            grad_query_bias,
            grad_value_bias,
            grad_out_bias,
            grad_gain_two,
            grad_shift_two,
            grad_down_bias,
        ],
        axis=1,
    )
    up_bias_cols = grad_up_bias.reshape(model_width, -1)
    packed_grads = jnp.concatenate(
        [grad_w_query, grad_w_keyval, grad_w_out, vectors, up_bias_cols], axis=1
    )

    reduced = scatter_sum(
        lax.psum_scatter(packed_grads, "dp", scatter_dimension=0, tiled=True), group_size
    )
    up_share = ff_grads[0]
    down_share = ff_grads[1].T
    col = 0
    pieces = []
    for width in (model_width, 2 * model_width, model_width):
        pieces.append(reduced[:, col : col + width])
        col += width
    vec = [reduced[:, col + i] for i in range(8)]
    col += 8
    up_bias_share = reduced[:, col:].reshape(-1)
    return (
        block_output,
        input_grad,
        vec[0],
        vec[1],
        pieces[0],
        vec[2],
        pieces[1],
        vec[3],
        pieces[2],
        vec[4],
        vec[5],
        vec[6],
        up_share,
        up_bias_share,
        down_share,
        vec[7],
    )


def solution(mesh):
    placed = (
        P(("dp", "mp"), None),
        P(("dp", "mp"), None),
        P(),
        P(),
        P(),
        P(),
        P(),
        P(),
        P(),
        P(),
        P(),
        P(),
        P(None, "mp"),
        P("mp"),
        P("mp", None),
        P(),
        P(("dp", "mp"), None),
    )
    return jax.shard_map(
        block_body,
        mesh=mesh,
        in_specs=placed,
        out_specs=(
            P(("dp", "mp"), None),
            P(("dp", "mp"), None),
            P(("dp", "mp")),
            P(("dp", "mp")),
            P(("dp", "mp"), None),
            P(("dp", "mp")),
            P(("dp", "mp"), None),
            P(("dp", "mp")),
            P(("dp", "mp"), None),
            P(("dp", "mp")),
            P(("dp", "mp")),
            P(("dp", "mp")),
            P("dp", "mp"),
            P(("dp", "mp")),
            P("mp", "dp"),
            P(("dp", "mp")),
        ),
        check_vma=False,
    )
```

```python
import math

import jax
import jax.numpy as jnp
from jax import lax
from jax.sharding import PartitionSpec as P


CLUSTERS = 100


epsilon = 1e-05


def norm_forward(inputs, gain_vec, offset):
    center = inputs - jnp.mean(inputs, axis=-1, keepdims=True)
    factor = lax.rsqrt(jnp.mean(center * center, axis=-1, keepdims=True) + epsilon)
    standard = center * factor
    return (standard * gain_vec + offset, standard, factor)


def norm_backward(upstream, standard, factor, gain_vec):
    scaled = upstream * gain_vec
    centred = scaled - jnp.mean(scaled, axis=-1, keepdims=True)
    centred = centred - standard * jnp.mean(scaled * standard, axis=-1, keepdims=True)
    return (factor * centred, jnp.sum(upstream * standard, axis=0), jnp.sum(upstream, axis=0))


def gelu_parts(before):
    cumulative = 0.5 * (1.0 + jax.scipy.special.erf(before / math.sqrt(2.0)))
    density = jnp.exp(-0.5 * before * before) / math.sqrt(2.0 * math.pi)
    return (before * cumulative, cumulative + before * density)


def ring_shift(x, group_size):
    return lax.ppermute(x, "mp", [(i, (i + 1) % group_size) for i in range(group_size)])


def ring_gather(x, group_size):
    me = lax.axis_index("mp")
    out = jnp.zeros((group_size,) + x.shape, x.dtype)
    out = lax.dynamic_update_index_in_dim(out, x, me, 0)
    cur = x
    for step in range(1, group_size):
        cur = ring_shift(cur, group_size)
        out = lax.dynamic_update_index_in_dim(
            out, cur, jnp.remainder(me + group_size - step, group_size), 0
        )
    return out.reshape((group_size * x.shape[0],) + x.shape[1:])


def scatter_sum(partial, group_size):
    pieces = partial.reshape((group_size, -1) + partial.shape[1:])
    arrived = lax.all_to_all(pieces, "mp", split_axis=0, concat_axis=0, tiled=True)
    return jnp.sum(arrived, axis=0)


def broadcast_gather(local, group_size):
    sent = jnp.broadcast_to(local[None], (group_size,) + local.shape)
    arrived = lax.all_to_all(sent, "mp", split_axis=0, concat_axis=0, tiled=True)
    return arrived.reshape((group_size * local.shape[0],) + local.shape[1:])


def block_body(
    block_input,
    clusters,
    ln1_gain,
    ln1_bias,
    w_query,
    query_bias,
    w_keyval,
    value_bias,
    w_out,
    out_bias,
    ln2_gain,
    ln2_bias,
    w_up,
    up_bias,
    w_down,
    down_bias,
    cotangent,
):
    group_size = lax.axis_size("mp")
    tok_rows = block_input.shape[0]
    model_width = block_input.shape[1]
    head_count = clusters.shape[1]
    head_dim = model_width // head_count
    local_heads = head_count // group_size
    score_scale = float(head_dim) ** (-0.5)

    grad_rows = ring_gather(cotangent, group_size)

    inputs = block_input.astype(jnp.float32)
    normed_one, standard_one, factor_one = norm_forward(inputs, ln1_gain, ln1_bias)
    first = normed_one.astype(jnp.bfloat16)
    queries = (
        jnp.dot(first, w_query, preferred_element_type=jnp.float32) + query_bias
    ).astype(jnp.bfloat16)
    keyval = jnp.dot(first, w_keyval, preferred_element_type=jnp.float32)
    keyval = (keyval + jnp.concatenate([jnp.zeros_like(value_bias), value_bias])).astype(
        jnp.bfloat16
    )
    member_float = (
        clusters.T[:, None, :] == jnp.arange(CLUSTERS, dtype=jnp.int32)[None, :, None]
    ).astype(jnp.float32)
    membership = member_float.astype(jnp.bfloat16)
    query_sums = jnp.einsum(
        "hct,thd->hcd",
        membership,
        queries.reshape(tok_rows, head_count, head_dim),
        preferred_element_type=jnp.float32,
    )
    cluster_sizes = jnp.sum(member_float, axis=2)
    packed = keyval.reshape(tok_rows, 2, group_size, local_heads * head_dim)

    sums_and_sizes = scatter_sum(
        jnp.concatenate([query_sums, cluster_sizes[:, :, None]], axis=2), group_size
    )
    arrived = lax.all_to_all(packed, "mp", split_axis=2, concat_axis=0, tiled=True)

    query_sums = sums_and_sizes[:, :, :head_dim]
    cluster_sizes = sums_and_sizes[:, :, head_dim]
    divisor = jnp.maximum(cluster_sizes, 1.0)
    centroids = (query_sums / divisor[:, :, None]).astype(jnp.bfloat16)
    length = arrived.shape[0]
    key_rows = arrived[:, 0, 0].reshape(length, local_heads, head_dim)
    value_rows = arrived[:, 1, 0].reshape(length, local_heads, head_dim)
    scores = score_scale * jnp.einsum(
        "hcd,jhd->hcj", centroids, key_rows, preferred_element_type=jnp.float32
    )
    score_peak = jnp.max(scores, axis=-1, keepdims=True)
    exponent = jnp.exp(scores - score_peak)
    denominator = jnp.sum(exponent, axis=-1, keepdims=True)
    probs = exponent / denominator
    logsum = score_peak + jnp.log(denominator)
    summary = jnp.einsum(
        "hcj,jhd->hcd",
        probs.astype(jnp.bfloat16),
        value_rows,
        preferred_element_type=jnp.float32,
    ).astype(jnp.bfloat16)

    everyone = broadcast_gather(summary, group_size)

    spread = (
        jnp.einsum("hct,hcd->thd", membership, everyone, preferred_element_type=jnp.float32)
        .astype(jnp.bfloat16)
        .reshape(tok_rows, model_width)
    )
    attended = jnp.dot(spread, w_out, preferred_element_type=jnp.float32) + out_bias
    middle = inputs + attended
    normed_two, standard_two, factor_two = norm_forward(middle, ln2_gain, ln2_bias)
    second = normed_two.astype(jnp.bfloat16)
    residual = lax.optimization_barrier(middle + down_bias)

    gathered = lax.all_gather(second, "mp", axis=0, tiled=True)

    before = jnp.dot(gathered, w_up, preferred_element_type=jnp.float32) + up_bias.astype(
        jnp.float32
    )
    activated, gelu_slope = gelu_parts(before)
    hidden = activated.astype(jnp.bfloat16)
    grad_hidden = jnp.einsum("td,fd->tf", grad_rows, w_down, preferred_element_type=jnp.float32)
    grad_before = (grad_hidden * gelu_slope).astype(jnp.bfloat16)
    grad_second = lax.psum_scatter(
        jnp.einsum("tf,df->td", grad_before, w_up, preferred_element_type=jnp.float32).astype(
            jnp.bfloat16
        ),
        "mp",
        scatter_dimension=0,
        tiled=True,
    ).astype(jnp.float32)

    out_partial = jnp.dot(hidden, w_down, preferred_element_type=jnp.float32)

    upstream = cotangent.astype(jnp.float32)
    grad_down_bias = jnp.sum(upstream, axis=0)
    grad_down_t = jnp.einsum("td,tf->df", grad_rows, hidden, preferred_element_type=jnp.float32)
    bias_part = jnp.sum(grad_before.astype(jnp.float32), axis=0)
    grad_up = jnp.einsum("td,tf->df", gathered, grad_before, preferred_element_type=jnp.float32)
    grad_up_bias = lax.dynamic_update_slice(
        jnp.zeros((group_size * bias_part.shape[0],), jnp.float32),
        bias_part,
        (lax.axis_index("mp") * bias_part.shape[0],),
    )
    ff_grads = lax.psum_scatter(
        jnp.stack([grad_up, grad_down_t]), "dp", scatter_dimension=1, tiled=True
    )

    result = lax.psum_scatter(
        out_partial.astype(jnp.bfloat16), "mp", scatter_dimension=0, tiled=True
    ).astype(jnp.float32)
    block_output = (residual + result).astype(jnp.bfloat16)

    scores_again = score_scale * jnp.einsum(
        "hcd,jhd->hcj", centroids, key_rows, preferred_element_type=jnp.float32
    )
    probs_again = jnp.exp(scores_again - logsum)

    middle_norm_grad, grad_gain_two, grad_shift_two = norm_backward(
        grad_second, standard_two, factor_two, ln2_gain
    )
    grad_middle = upstream + middle_norm_grad
    attn_grad = grad_middle.astype(jnp.bfloat16)
    grad_out_bias = jnp.sum(attn_grad.astype(jnp.float32), axis=0)
    grad_w_out = jnp.einsum("td,te->de", spread, attn_grad, preferred_element_type=jnp.float32)
    grad_spread = jnp.einsum(
        "te,de->td", attn_grad, w_out, preferred_element_type=jnp.float32
    ).astype(jnp.bfloat16)
    summary_grad = jnp.einsum(
        "hct,thd->hcd",
        membership,
        grad_spread.reshape(tok_rows, head_count, head_dim),
        preferred_element_type=jnp.float32,
    )

    summary_grad = scatter_sum(summary_grad, group_size).astype(jnp.bfloat16)

    grad_values = jnp.einsum(
        "hcj,hcd->jhd",
        probs_again.astype(jnp.bfloat16),
        summary_grad,
        preferred_element_type=jnp.float32,
    )
    grad_probs = jnp.einsum(
        "hcd,jhd->hcj", summary_grad, value_rows, preferred_element_type=jnp.float32
    )
    grad_scores = probs_again * (
        grad_probs - jnp.sum(probs_again * grad_probs, axis=-1, keepdims=True)
    )
    grad_scores = grad_scores.astype(jnp.bfloat16)
    grad_centroids = (
        score_scale
        * jnp.einsum("hcj,jhd->hcd", grad_scores, key_rows, preferred_element_type=jnp.float32)
    ).astype(jnp.bfloat16)
    grad_keys = score_scale * jnp.einsum(
        "hcj,hcd->jhd", grad_scores, centroids, preferred_element_type=jnp.float32
    )
    grad_kv = jnp.concatenate(
        [
            grad_keys.reshape(length, local_heads * head_dim),
            grad_values.reshape(length, local_heads * head_dim),
        ],
        axis=1,
    ).astype(jnp.bfloat16)
    kv_width = 2 * local_heads * head_dim
    per_member = (grad_centroids.astype(jnp.float32) / divisor[:, :, None]).astype(
        jnp.bfloat16
    )
    member_rows = per_member.size // kv_width
    outgoing = jnp.concatenate(
        [
            grad_kv.reshape(group_size, tok_rows, kv_width),
            jnp.broadcast_to(
                per_member.reshape(1, member_rows, kv_width),
                (group_size, member_rows, kv_width),
            ),
        ],
        axis=1,
    )

    incoming = lax.all_to_all(outgoing, "mp", split_axis=0, concat_axis=0, tiled=True)

    returned = incoming[:, :tok_rows].reshape(group_size, tok_rows, 2, local_heads * head_dim)
    grad_keyval = returned.transpose(1, 2, 0, 3).reshape(tok_rows, 2 * model_width)
    all_member = (
        incoming[:, tok_rows:].reshape(head_count, CLUSTERS, head_dim).astype(jnp.float32)
    )
    grad_queries = jnp.einsum(
        "hct,hcd->thd", member_float, all_member, precision=lax.Precision.HIGHEST
    )
    grad_queries = grad_queries.reshape(tok_rows, model_width).astype(jnp.bfloat16)
    grad_query_bias = jnp.sum(grad_queries.astype(jnp.float32), axis=0)
    grad_value_bias = jnp.sum(grad_keyval[:, model_width:].astype(jnp.float32), axis=0)
    grad_w_query = jnp.einsum("td,te->de", first, grad_queries, preferred_element_type=jnp.float32)
    grad_w_keyval = jnp.einsum("td,te->de", first, grad_keyval, preferred_element_type=jnp.float32)
    grad_first = jnp.einsum("te,de->td", grad_queries, w_query, preferred_element_type=jnp.float32)
    grad_first = grad_first + jnp.einsum(
        "te,de->td", grad_keyval, w_keyval, preferred_element_type=jnp.float32
    )
    input_norm_grad, grad_gain_one, grad_shift_one = norm_backward(
        grad_first, standard_one, factor_one, ln1_gain
    )
    input_grad = grad_middle + input_norm_grad
    vectors = jnp.stack(
        [
            grad_gain_one,
            grad_shift_one,
            grad_query_bias,
            grad_value_bias,
            grad_out_bias,
            grad_gain_two,
            grad_shift_two,
            grad_down_bias,
        ],
        axis=1,
    )
    up_bias_cols = grad_up_bias.reshape(model_width, -1)
    packed_grads = jnp.concatenate(
        [grad_w_query, grad_w_keyval, grad_w_out, vectors, up_bias_cols], axis=1
    )

    reduced = scatter_sum(
        lax.psum_scatter(packed_grads, "dp", scatter_dimension=0, tiled=True), group_size
    )
    up_share = ff_grads[0]
    down_share = ff_grads[1].T
    col = 0
    pieces = []
    for width in (model_width, 2 * model_width, model_width):
        pieces.append(reduced[:, col : col + width])
        col += width
    vec = [reduced[:, col + i] for i in range(8)]
    col += 8
    up_bias_share = reduced[:, col:].reshape(-1)
    return (
        block_output,
        input_grad,
        vec[0],
        vec[1],
        pieces[0],
        vec[2],
        pieces[1],
        vec[3],
        pieces[2],
        vec[4],
        vec[5],
        vec[6],
        up_share,
        up_bias_share,
        down_share,
        vec[7],
    )


def solution(mesh):
    placed = (
        P(("dp", "mp"), None),
        P(("dp", "mp"), None),
        P(),
        P(),
        P(),
        P(),
        P(),
        P(),
        P(),
        P(),
        P(),
        P(),
        P(None, "mp"),
        P("mp"),
        P("mp", None),
        P(),
        P(("dp", "mp"), None),
    )
    return jax.shard_map(
        block_body,
        mesh=mesh,
        in_specs=placed,
        out_specs=(
            P(("dp", "mp"), None),
            P(("dp", "mp"), None),
            P(("dp", "mp")),
            P(("dp", "mp")),
            P(("dp", "mp"), None),
            P(("dp", "mp")),
            P(("dp", "mp"), None),
            P(("dp", "mp")),
            P(("dp", "mp"), None),
            P(("dp", "mp")),
            P(("dp", "mp")),
            P(("dp", "mp")),
            P("dp", "mp"),
            P(("dp", "mp")),
            P("mp", "dp"),
            P(("dp", "mp")),
        ),
        check_vma=False,
    )
```

```python
import math

import jax
import jax.numpy as jnp
from jax import lax
from jax.sharding import PartitionSpec as P


CLUSTERS = 100


epsilon = 1e-05


def norm_forward(inputs, gain_vec, offset):
    center = inputs - jnp.mean(inputs, axis=-1, keepdims=True)
    factor = lax.rsqrt(jnp.mean(center * center, axis=-1, keepdims=True) + epsilon)
    standard = center * factor
    return (standard * gain_vec + offset, standard, factor)


def norm_backward(upstream, standard, factor, gain_vec):
    scaled = upstream * gain_vec
    centred = scaled - jnp.mean(scaled, axis=-1, keepdims=True)
    centred = centred - standard * jnp.mean(scaled * standard, axis=-1, keepdims=True)
    return (factor * centred, jnp.sum(upstream * standard, axis=0), jnp.sum(upstream, axis=0))


def gelu_parts(before):
    cumulative = 0.5 * (1.0 + jax.scipy.special.erf(before / math.sqrt(2.0)))
    density = jnp.exp(-0.5 * before * before) / math.sqrt(2.0 * math.pi)
    return (before * cumulative, cumulative + before * density)


def ring_shift(x, group_size):
    return lax.ppermute(x, "mp", [(i, (i + 1) % group_size) for i in range(group_size)])


def ring_gather(x, group_size):
    me = lax.axis_index("mp")
    out = jnp.zeros((group_size,) + x.shape, x.dtype)
    out = lax.dynamic_update_index_in_dim(out, x, me, 0)
    cur = x
    for step in range(1, group_size):
        cur = ring_shift(cur, group_size)
        out = lax.dynamic_update_index_in_dim(
            out, cur, jnp.remainder(me + group_size - step, group_size), 0
        )
    return out.reshape((group_size * x.shape[0],) + x.shape[1:])


def scatter_sum(partial, group_size):
    pieces = partial.reshape((group_size, -1) + partial.shape[1:])
    arrived = lax.all_to_all(pieces, "mp", split_axis=0, concat_axis=0, tiled=True)
    return jnp.sum(arrived.astype(jnp.float32), axis=0)


def broadcast_gather(local, group_size):
    sent = jnp.broadcast_to(local[None], (group_size,) + local.shape)
    arrived = lax.all_to_all(sent, "mp", split_axis=0, concat_axis=0, tiled=True)
    return arrived.reshape((group_size * local.shape[0],) + local.shape[1:])


def block_body(
    block_input,
    clusters,
    ln1_gain,
    ln1_bias,
    w_query,
    query_bias,
    w_keyval,
    value_bias,
    w_out,
    out_bias,
    ln2_gain,
    ln2_bias,
    w_up,
    up_bias,
    w_down,
    down_bias,
    cotangent,
):
    group_size = lax.axis_size("mp")
    tok_rows = block_input.shape[0]
    model_width = block_input.shape[1]
    head_count = clusters.shape[1]
    head_dim = model_width // head_count
    local_heads = head_count // group_size
    score_scale = float(head_dim) ** (-0.5)

    grad_rows = ring_gather(cotangent, group_size)

    inputs = block_input.astype(jnp.float32)
    normed_one, standard_one, factor_one = norm_forward(inputs, ln1_gain, ln1_bias)
    first = normed_one.astype(jnp.bfloat16)
    queries = (
        jnp.dot(first, w_query, preferred_element_type=jnp.float32) + query_bias
    ).astype(jnp.bfloat16)
    keyval = jnp.dot(first, w_keyval, preferred_element_type=jnp.float32)
    keyval = (keyval + jnp.concatenate([jnp.zeros_like(value_bias), value_bias])).astype(
        jnp.bfloat16
    )
    member_float = (
        clusters.T[:, None, :] == jnp.arange(CLUSTERS, dtype=jnp.int32)[None, :, None]
    ).astype(jnp.float32)
    membership = member_float.astype(jnp.bfloat16)
    query_sums = jnp.einsum(
        "hct,thd->hcd",
        membership,
        queries.reshape(tok_rows, head_count, head_dim),
        preferred_element_type=jnp.float32,
    )
    cluster_sizes = jnp.sum(member_float, axis=2)
    packed = keyval.reshape(tok_rows, 2, group_size, local_heads * head_dim)

    sums_and_sizes = scatter_sum(
        jnp.concatenate([query_sums, cluster_sizes[:, :, None]], axis=2), group_size
    )
    arrived = lax.all_to_all(packed, "mp", split_axis=2, concat_axis=0, tiled=True)

    query_sums = sums_and_sizes[:, :, :head_dim]
    cluster_sizes = sums_and_sizes[:, :, head_dim]
    divisor = jnp.maximum(cluster_sizes, 1.0)
    centroids = (query_sums / divisor[:, :, None]).astype(jnp.bfloat16)
    length = arrived.shape[0]
    key_rows = arrived[:, 0, 0].reshape(length, local_heads, head_dim)
    value_rows = arrived[:, 1, 0].reshape(length, local_heads, head_dim)
    scores = score_scale * jnp.einsum(
        "hcd,jhd->hcj", centroids, key_rows, preferred_element_type=jnp.float32
    )
    score_peak = jnp.max(scores, axis=-1, keepdims=True)
    exponent = jnp.exp(scores - score_peak)
    denominator = jnp.sum(exponent, axis=-1, keepdims=True)
    probs = exponent / denominator
    logsum = score_peak + jnp.log(denominator)
    summary = jnp.einsum(
        "hcj,jhd->hcd",
        probs.astype(jnp.bfloat16),
        value_rows,
        preferred_element_type=jnp.float32,
    ).astype(jnp.bfloat16)

    everyone = broadcast_gather(summary, group_size)

    spread = (
        jnp.einsum("hct,hcd->thd", membership, everyone, preferred_element_type=jnp.float32)
        .astype(jnp.bfloat16)
        .reshape(tok_rows, model_width)
    )
    attended = jnp.dot(spread, w_out, preferred_element_type=jnp.float32) + out_bias
    middle = inputs + attended
    normed_two, standard_two, factor_two = norm_forward(middle, ln2_gain, ln2_bias)
    second = normed_two.astype(jnp.bfloat16)
    residual = lax.optimization_barrier(middle + down_bias)

    gathered = lax.all_gather(second, "mp", axis=0, tiled=True)

    before = jnp.dot(gathered, w_up, preferred_element_type=jnp.float32) + up_bias.astype(
        jnp.float32
    )
    activated, gelu_slope = gelu_parts(before)
    hidden = activated.astype(jnp.bfloat16)
    grad_hidden = jnp.einsum("td,fd->tf", grad_rows, w_down, preferred_element_type=jnp.float32)
    grad_before = (grad_hidden * gelu_slope).astype(jnp.bfloat16)
    grad_second = lax.psum_scatter(
        jnp.einsum("tf,df->td", grad_before, w_up, preferred_element_type=jnp.float32).astype(
            jnp.bfloat16
        ),
        "mp",
        scatter_dimension=0,
        tiled=True,
    ).astype(jnp.float32)

    out_partial = jnp.dot(hidden, w_down, preferred_element_type=jnp.float32)

    upstream = cotangent.astype(jnp.float32)
    grad_down_bias = jnp.sum(upstream, axis=0)
    grad_down_t = jnp.einsum("td,tf->df", grad_rows, hidden, preferred_element_type=jnp.float32)
    bias_part = jnp.sum(grad_before.astype(jnp.float32), axis=0)
    grad_up = jnp.einsum("td,tf->df", gathered, grad_before, preferred_element_type=jnp.float32)
    grad_up_bias = lax.dynamic_update_slice(
        jnp.zeros((group_size * bias_part.shape[0],), jnp.float32),
        bias_part,
        (lax.axis_index("mp") * bias_part.shape[0],),
    )

    scores_again = score_scale * jnp.einsum(
        "hcd,jhd->hcj", centroids, key_rows, preferred_element_type=jnp.float32
    )
    probs_again = jnp.exp(scores_again - logsum)

    middle_norm_grad, grad_gain_two, grad_shift_two = norm_backward(
        grad_second, standard_two, factor_two, ln2_gain
    )
    grad_middle = upstream + middle_norm_grad
    attn_grad = grad_middle.astype(jnp.bfloat16)
    grad_out_bias = jnp.sum(attn_grad.astype(jnp.float32), axis=0)
    grad_w_out = jnp.einsum("td,te->de", spread, attn_grad, preferred_element_type=jnp.float32)
    grad_spread = jnp.einsum(
        "te,de->td", attn_grad, w_out, preferred_element_type=jnp.float32
    ).astype(jnp.bfloat16)
    summary_grad = jnp.einsum(
        "hct,thd->hcd",
        membership,
        grad_spread.reshape(tok_rows, head_count, head_dim),
        preferred_element_type=jnp.float32,
    )

    ff_grads = lax.psum_scatter(
        jnp.stack([grad_up, grad_down_t, grad_w_out]), "dp", scatter_dimension=1, tiled=True
    )

    summary_grad = scatter_sum(summary_grad, group_size).astype(jnp.bfloat16)

    grad_values = jnp.einsum(
        "hcj,hcd->jhd",
        probs_again.astype(jnp.bfloat16),
        summary_grad,
        preferred_element_type=jnp.float32,
    )
    grad_probs = jnp.einsum(
        "hcd,jhd->hcj", summary_grad, value_rows, preferred_element_type=jnp.float32
    )
    grad_scores = probs_again * (
        grad_probs - jnp.sum(probs_again * grad_probs, axis=-1, keepdims=True)
    )
    grad_scores = grad_scores.astype(jnp.bfloat16)
    grad_centroids = (
        score_scale
        * jnp.einsum("hcj,jhd->hcd", grad_scores, key_rows, preferred_element_type=jnp.float32)
    ).astype(jnp.bfloat16)
    grad_keys = score_scale * jnp.einsum(
        "hcj,hcd->jhd", grad_scores, centroids, preferred_element_type=jnp.float32
    )
    grad_kv = jnp.concatenate(
        [
            grad_keys.reshape(length, local_heads * head_dim),
            grad_values.reshape(length, local_heads * head_dim),
        ],
        axis=1,
    ).astype(jnp.bfloat16)
    kv_width = 2 * local_heads * head_dim
    per_member = (grad_centroids.astype(jnp.float32) / divisor[:, :, None]).astype(
        jnp.bfloat16
    )
    member_rows = per_member.size // kv_width
    outgoing = jnp.concatenate(
        [
            grad_kv.reshape(group_size, tok_rows, kv_width),
            jnp.broadcast_to(
                per_member.reshape(1, member_rows, kv_width),
                (group_size, member_rows, kv_width),
            ),
        ],
        axis=1,
    )

    incoming = lax.all_to_all(outgoing, "mp", split_axis=0, concat_axis=0, tiled=True)

    out_pieces, _ = lax.optimization_barrier((out_partial.astype(jnp.bfloat16), incoming))
    result = scatter_sum(out_pieces, group_size)
    block_output = (residual + result).astype(jnp.bfloat16)

    returned = incoming[:, :tok_rows].reshape(group_size, tok_rows, 2, local_heads * head_dim)
    grad_keyval = returned.transpose(1, 2, 0, 3).reshape(tok_rows, 2 * model_width)
    all_member = (
        incoming[:, tok_rows:].reshape(head_count, CLUSTERS, head_dim).astype(jnp.float32)
    )
    grad_queries = jnp.einsum(
        "hct,hcd->thd", member_float, all_member, precision=lax.Precision.HIGHEST
    )
    grad_queries = grad_queries.reshape(tok_rows, model_width).astype(jnp.bfloat16)
    grad_query_bias = jnp.sum(grad_queries.astype(jnp.float32), axis=0)
    grad_value_bias = jnp.sum(grad_keyval[:, model_width:].astype(jnp.float32), axis=0)
    grad_w_query = jnp.einsum("td,te->de", first, grad_queries, preferred_element_type=jnp.float32)
    grad_w_keyval = jnp.einsum("td,te->de", first, grad_keyval, preferred_element_type=jnp.float32)
    grad_first = jnp.einsum("te,de->td", grad_queries, w_query, preferred_element_type=jnp.float32)
    grad_first = grad_first + jnp.einsum(
        "te,de->td", grad_keyval, w_keyval, preferred_element_type=jnp.float32
    )
    input_norm_grad, grad_gain_one, grad_shift_one = norm_backward(
        grad_first, standard_one, factor_one, ln1_gain
    )
    input_grad = grad_middle + input_norm_grad
    vectors = jnp.stack(
        [
            grad_gain_one,
            grad_shift_one,
            grad_query_bias,
            grad_value_bias,
            grad_out_bias,
            grad_gain_two,
            grad_shift_two,
            grad_down_bias,
        ],
        axis=1,
    )
    up_bias_cols = grad_up_bias.reshape(model_width, -1)
    packed_grads = jnp.concatenate([grad_w_query, grad_w_keyval, vectors, up_bias_cols], axis=1)

    dp_reduced = lax.psum_scatter(packed_grads, "dp", scatter_dimension=0, tiled=True)
    attn_width = grad_w_query.shape[1] + grad_w_keyval.shape[1]
    reduced = scatter_sum(
        jnp.concatenate(
            [dp_reduced[:, :attn_width], ff_grads[2], dp_reduced[:, attn_width:]], axis=1
        ),
        group_size,
    )
    up_share = ff_grads[0]
    down_share = ff_grads[1].T
    col = 0
    pieces = []
    for width in (model_width, 2 * model_width, model_width):
        pieces.append(reduced[:, col : col + width])
        col += width
    vec = [reduced[:, col + i] for i in range(8)]
    col += 8
    up_bias_share = reduced[:, col:].reshape(-1)
    return (
        block_output,
        input_grad,
        vec[0],
        vec[1],
        pieces[0],
        vec[2],
        pieces[1],
        vec[3],
        pieces[2],
        vec[4],
        vec[5],
        vec[6],
        up_share,
        up_bias_share,
        down_share,
        vec[7],
    )


def solution(mesh):
    placed = (
        P(("dp", "mp"), None),
        P(("dp", "mp"), None),
        P(),
        P(),
        P(),
        P(),
        P(),
        P(),
        P(),
        P(),
        P(),
        P(),
        P(None, "mp"),
        P("mp"),
        P("mp", None),
        P(),
        P(("dp", "mp"), None),
    )
    return jax.shard_map(
        block_body,
        mesh=mesh,
        in_specs=placed,
        out_specs=(
            P(("dp", "mp"), None),
            P(("dp", "mp"), None),
            P(("dp", "mp")),
            P(("dp", "mp")),
            P(("dp", "mp"), None),
            P(("dp", "mp")),
            P(("dp", "mp"), None),
            P(("dp", "mp")),
            P(("dp", "mp"), None),
            P(("dp", "mp")),
            P(("dp", "mp")),
            P(("dp", "mp")),
            P("dp", "mp"),
            P(("dp", "mp")),
            P("mp", "dp"),
            P(("dp", "mp")),
        ),
        check_vma=False,
    )
```

```python
import math

import jax
import jax.numpy as jnp
from jax import lax
from jax.sharding import PartitionSpec as P


CLUSTERS = 100


epsilon = 1e-05


def norm_forward(inputs, gain_vec, offset):
    center = inputs - jnp.mean(inputs, axis=-1, keepdims=True)
    factor = lax.rsqrt(jnp.mean(center * center, axis=-1, keepdims=True) + epsilon)
    standard = center * factor
    return (standard * gain_vec + offset, standard, factor)


def norm_backward(upstream, standard, factor, gain_vec):
    scaled = upstream * gain_vec
    centred = scaled - jnp.mean(scaled, axis=-1, keepdims=True)
    centred = centred - standard * jnp.mean(scaled * standard, axis=-1, keepdims=True)
    return (factor * centred, jnp.sum(upstream * standard, axis=0), jnp.sum(upstream, axis=0))


def gelu_parts(before):
    cumulative = 0.5 * (1.0 + jax.scipy.special.erf(before / math.sqrt(2.0)))
    density = jnp.exp(-0.5 * before * before) / math.sqrt(2.0 * math.pi)
    return (before * cumulative, cumulative + before * density)


def ring_shift(x, group_size):
    return lax.ppermute(x, "mp", [(i, (i + 1) % group_size) for i in range(group_size)])


def ring_gather(x, group_size):
    me = lax.axis_index("mp")
    out = jnp.zeros((group_size,) + x.shape, x.dtype)
    out = lax.dynamic_update_index_in_dim(out, x, me, 0)
    cur = x
    for step in range(1, group_size):
        cur = ring_shift(cur, group_size)
        out = lax.dynamic_update_index_in_dim(
            out, cur, jnp.remainder(me + group_size - step, group_size), 0
        )
    return out.reshape((group_size * x.shape[0],) + x.shape[1:])


def scatter_sum(partial, group_size):
    pieces = partial.reshape((group_size, -1) + partial.shape[1:])
    arrived = lax.all_to_all(pieces, "mp", split_axis=0, concat_axis=0, tiled=True)
    return jnp.sum(arrived.astype(jnp.float32), axis=0)


def broadcast_gather(local, group_size):
    sent = jnp.broadcast_to(local[None], (group_size,) + local.shape)
    arrived = lax.all_to_all(sent, "mp", split_axis=0, concat_axis=0, tiled=True)
    return arrived.reshape((group_size * local.shape[0],) + local.shape[1:])


def block_body(
    block_input,
    clusters,
    ln1_gain,
    ln1_bias,
    w_query,
    query_bias,
    w_keyval,
    value_bias,
    w_out,
    out_bias,
    ln2_gain,
    ln2_bias,
    w_up,
    up_bias,
    w_down,
    down_bias,
    cotangent,
):
    group_size = lax.axis_size("mp")
    tok_rows = block_input.shape[0]
    model_width = block_input.shape[1]
    head_count = clusters.shape[1]
    head_dim = model_width // head_count
    local_heads = head_count // group_size
    score_scale = float(head_dim) ** (-0.5)

    grad_rows = ring_gather(cotangent, group_size)

    inputs = block_input.astype(jnp.float32)
    normed_one, standard_one, factor_one = norm_forward(inputs, ln1_gain, ln1_bias)
    first = normed_one.astype(jnp.bfloat16)
    queries = (
        jnp.dot(first, w_query, preferred_element_type=jnp.float32) + query_bias
    ).astype(jnp.bfloat16)
    keyval = jnp.dot(first, w_keyval, preferred_element_type=jnp.float32)
    keyval = (keyval + jnp.concatenate([jnp.zeros_like(value_bias), value_bias])).astype(
        jnp.bfloat16
    )
    member_float = (
        clusters.T[:, None, :] == jnp.arange(CLUSTERS, dtype=jnp.int32)[None, :, None]
    ).astype(jnp.float32)
    membership = member_float.astype(jnp.bfloat16)
    query_sums = jnp.einsum(
        "hct,thd->hcd",
        membership,
        queries.reshape(tok_rows, head_count, head_dim),
        preferred_element_type=jnp.float32,
    )
    cluster_sizes = jnp.sum(member_float, axis=2)
    packed = keyval.reshape(tok_rows, 2, group_size, local_heads * head_dim)

    arrived = lax.all_to_all(packed, "mp", split_axis=2, concat_axis=0, tiled=True)
    sums_and_sizes = scatter_sum(
        jnp.concatenate([query_sums, cluster_sizes[:, :, None]], axis=2), group_size
    )

    query_sums = sums_and_sizes[:, :, :head_dim]
    cluster_sizes = sums_and_sizes[:, :, head_dim]
    divisor = jnp.maximum(cluster_sizes, 1.0)
    centroids = (query_sums / divisor[:, :, None]).astype(jnp.bfloat16)
    length = arrived.shape[0]
    key_rows = arrived[:, 0, 0].reshape(length, local_heads, head_dim)
    value_rows = arrived[:, 1, 0].reshape(length, local_heads, head_dim)
    scores = score_scale * jnp.einsum(
        "hcd,jhd->hcj", centroids, key_rows, preferred_element_type=jnp.float32
    )
    score_peak = jnp.max(scores, axis=-1, keepdims=True)
    exponent = jnp.exp(scores - score_peak)
    denominator = jnp.sum(exponent, axis=-1, keepdims=True)
    probs = exponent / denominator
    logsum = score_peak + jnp.log(denominator)
    summary = jnp.einsum(
        "hcj,jhd->hcd",
        probs.astype(jnp.bfloat16),
        value_rows,
        preferred_element_type=jnp.float32,
    ).astype(jnp.bfloat16)

    everyone = broadcast_gather(summary, group_size)

    spread = (
        jnp.einsum("hct,hcd->thd", membership, everyone, preferred_element_type=jnp.float32)
        .astype(jnp.bfloat16)
        .reshape(tok_rows, model_width)
    )
    attended = jnp.dot(spread, w_out, preferred_element_type=jnp.float32) + out_bias
    middle = inputs + attended
    normed_two, standard_two, factor_two = norm_forward(middle, ln2_gain, ln2_bias)
    second = normed_two.astype(jnp.bfloat16)
    residual = lax.optimization_barrier(middle + down_bias)

    gathered = lax.all_gather(second, "mp", axis=0, tiled=True)

    before = jnp.dot(gathered, w_up, preferred_element_type=jnp.float32) + up_bias.astype(
        jnp.float32
    )
    activated, gelu_slope = gelu_parts(before)
    hidden = activated.astype(jnp.bfloat16)
    grad_hidden = jnp.einsum("td,fd->tf", grad_rows, w_down, preferred_element_type=jnp.float32)
    grad_before = (grad_hidden * gelu_slope).astype(jnp.bfloat16)
    grad_second = lax.psum_scatter(
        jnp.einsum("tf,df->td", grad_before, w_up, preferred_element_type=jnp.float32).astype(
            jnp.bfloat16
        ),
        "mp",
        scatter_dimension=0,
        tiled=True,
    ).astype(jnp.float32)

    out_partial = jnp.dot(hidden, w_down, preferred_element_type=jnp.float32)

    upstream = cotangent.astype(jnp.float32)
    grad_down_bias = jnp.sum(upstream, axis=0)
    grad_down_t = jnp.einsum("td,tf->df", grad_rows, hidden, preferred_element_type=jnp.float32)
    bias_part = jnp.sum(grad_before.astype(jnp.float32), axis=0)
    grad_up = jnp.einsum("td,tf->df", gathered, grad_before, preferred_element_type=jnp.float32)
    grad_up_bias = lax.dynamic_update_slice(
        jnp.zeros((group_size * bias_part.shape[0],), jnp.float32),
        bias_part,
        (lax.axis_index("mp") * bias_part.shape[0],),
    )

    scores_again = score_scale * jnp.einsum(
        "hcd,jhd->hcj", centroids, key_rows, preferred_element_type=jnp.float32
    )
    probs_again = jnp.exp(scores_again - logsum)

    middle_norm_grad, grad_gain_two, grad_shift_two = norm_backward(
        grad_second, standard_two, factor_two, ln2_gain
    )
    grad_middle = upstream + middle_norm_grad
    attn_grad = grad_middle.astype(jnp.bfloat16)
    grad_out_bias = jnp.sum(attn_grad.astype(jnp.float32), axis=0)
    grad_w_out = jnp.einsum("td,te->de", spread, attn_grad, preferred_element_type=jnp.float32)
    grad_spread = jnp.einsum(
        "te,de->td", attn_grad, w_out, preferred_element_type=jnp.float32
    ).astype(jnp.bfloat16)
    summary_grad = jnp.einsum(
        "hct,thd->hcd",
        membership,
        grad_spread.reshape(tok_rows, head_count, head_dim),
        preferred_element_type=jnp.float32,
    )

    ff_grads = lax.psum_scatter(
        jnp.stack([grad_up, grad_down_t, grad_w_out]), "dp", scatter_dimension=1, tiled=True
    )

    summary_grad = scatter_sum(summary_grad, group_size).astype(jnp.bfloat16)

    grad_values = jnp.einsum(
        "hcj,hcd->jhd",
        probs_again.astype(jnp.bfloat16),
        summary_grad,
        preferred_element_type=jnp.float32,
    )
    grad_probs = jnp.einsum(
        "hcd,jhd->hcj", summary_grad, value_rows, preferred_element_type=jnp.float32
    )
    grad_scores = probs_again * (
        grad_probs - jnp.sum(probs_again * grad_probs, axis=-1, keepdims=True)
    )
    grad_scores = grad_scores.astype(jnp.bfloat16)
    grad_centroids = (
        score_scale
        * jnp.einsum("hcj,jhd->hcd", grad_scores, key_rows, preferred_element_type=jnp.float32)
    ).astype(jnp.bfloat16)
    grad_keys = score_scale * jnp.einsum(
        "hcj,hcd->jhd", grad_scores, centroids, preferred_element_type=jnp.float32
    )
    grad_kv = jnp.concatenate(
        [
            grad_keys.reshape(length, local_heads * head_dim),
            grad_values.reshape(length, local_heads * head_dim),
        ],
        axis=1,
    ).astype(jnp.bfloat16)
    kv_width = 2 * local_heads * head_dim
    per_member = (grad_centroids.astype(jnp.float32) / divisor[:, :, None]).astype(
        jnp.bfloat16
    )
    member_rows = per_member.size // kv_width
    outgoing = jnp.concatenate(
        [
            grad_kv.reshape(group_size, tok_rows, kv_width),
            jnp.broadcast_to(
                per_member.reshape(1, member_rows, kv_width),
                (group_size, member_rows, kv_width),
            ),
        ],
        axis=1,
    )

    incoming = lax.all_to_all(outgoing, "mp", split_axis=0, concat_axis=0, tiled=True)

    out_pieces, _ = lax.optimization_barrier((out_partial.astype(jnp.bfloat16), incoming))
    result = scatter_sum(out_pieces, group_size)
    block_output = (residual + result).astype(jnp.bfloat16)

    returned = incoming[:, :tok_rows].reshape(group_size, tok_rows, 2, local_heads * head_dim)
    grad_keyval = returned.transpose(1, 2, 0, 3).reshape(tok_rows, 2 * model_width)
    all_member = (
        incoming[:, tok_rows:].reshape(head_count, CLUSTERS, head_dim).astype(jnp.float32)
    )
    grad_queries = jnp.einsum(
        "hct,hcd->thd", member_float, all_member, precision=lax.Precision.HIGHEST
    )
    grad_queries = grad_queries.reshape(tok_rows, model_width).astype(jnp.bfloat16)
    grad_query_bias = jnp.sum(grad_queries.astype(jnp.float32), axis=0)
    grad_value_bias = jnp.sum(grad_keyval[:, model_width:].astype(jnp.float32), axis=0)
    grad_w_attn = jnp.einsum(
        "td,te->de",
        first,
        jnp.concatenate([grad_queries, grad_keyval], axis=1),
        preferred_element_type=jnp.float32,
    )
    grad_first = jnp.einsum("te,de->td", grad_queries, w_query, preferred_element_type=jnp.float32)
    grad_first = grad_first + jnp.einsum(
        "te,de->td", grad_keyval, w_keyval, preferred_element_type=jnp.float32
    )
    input_norm_grad, grad_gain_one, grad_shift_one = norm_backward(
        grad_first, standard_one, factor_one, ln1_gain
    )
    input_grad = grad_middle + input_norm_grad
    vectors = jnp.stack(
        [
            grad_gain_one,
            grad_shift_one,
            grad_query_bias,
            grad_value_bias,
            grad_out_bias,
            grad_gain_two,
            grad_shift_two,
            grad_down_bias,
        ],
        axis=1,
    )
    up_bias_cols = grad_up_bias.reshape(model_width, -1)
    packed_grads = jnp.concatenate([grad_w_attn, vectors, up_bias_cols], axis=1)

    dp_reduced = lax.psum_scatter(packed_grads, "dp", scatter_dimension=0, tiled=True)
    attn_width = grad_w_attn.shape[1]
    reduced = scatter_sum(
        jnp.concatenate(
            [dp_reduced[:, :attn_width], ff_grads[2], dp_reduced[:, attn_width:]], axis=1
        ),
        group_size,
    )
    up_share = ff_grads[0]
    down_share = ff_grads[1].T
    col = 0
    pieces = []
    for width in (model_width, 2 * model_width, model_width):
        pieces.append(reduced[:, col : col + width])
        col += width
    vec = [reduced[:, col + i] for i in range(8)]
    col += 8
    up_bias_share = reduced[:, col:].reshape(-1)
    return (
        block_output,
        input_grad,
        vec[0],
        vec[1],
        pieces[0],
        vec[2],
        pieces[1],
        vec[3],
        pieces[2],
        vec[4],
        vec[5],
        vec[6],
        up_share,
        up_bias_share,
        down_share,
        vec[7],
    )


def solution(mesh):
    placed = (
        P(("dp", "mp"), None),
        P(("dp", "mp"), None),
        P(),
        P(),
        P(),
        P(),
        P(),
        P(),
        P(),
        P(),
        P(),
        P(),
        P(None, "mp"),
        P("mp"),
        P("mp", None),
        P(),
        P(("dp", "mp"), None),
    )
    return jax.shard_map(
        block_body,
        mesh=mesh,
        in_specs=placed,
        out_specs=(
            P(("dp", "mp"), None),
            P(("dp", "mp"), None),
            P(("dp", "mp")),
            P(("dp", "mp")),
            P(("dp", "mp"), None),
            P(("dp", "mp")),
            P(("dp", "mp"), None),
            P(("dp", "mp")),
            P(("dp", "mp"), None),
            P(("dp", "mp")),
            P(("dp", "mp")),
            P(("dp", "mp")),
            P("dp", "mp"),
            P(("dp", "mp")),
            P("mp", "dp"),
            P(("dp", "mp")),
        ),
        check_vma=False,
    )
```

```python
import math

import jax
import jax.numpy as jnp
from jax import lax
from jax.sharding import PartitionSpec as P


CLUSTERS = 100


epsilon = 1e-05


def norm_forward(inputs, gain_vec, offset):
    center = inputs - jnp.mean(inputs, axis=-1, keepdims=True)
    factor = lax.rsqrt(jnp.mean(center * center, axis=-1, keepdims=True) + epsilon)
    standard = center * factor
    return (standard * gain_vec + offset, standard, factor)


def norm_backward(upstream, standard, factor, gain_vec):
    scaled = upstream * gain_vec
    centred = scaled - jnp.mean(scaled, axis=-1, keepdims=True)
    centred = centred - standard * jnp.mean(scaled * standard, axis=-1, keepdims=True)
    return (factor * centred, jnp.sum(upstream * standard, axis=0), jnp.sum(upstream, axis=0))


def gelu_parts(before):
    cumulative = 0.5 * (1.0 + jax.scipy.special.erf(before / math.sqrt(2.0)))
    density = jnp.exp(-0.5 * before * before) / math.sqrt(2.0 * math.pi)
    return (before * cumulative, cumulative + before * density)


def ring_shift(x, group_size):
    return lax.ppermute(x, "mp", [(i, (i + 1) % group_size) for i in range(group_size)])


def ring_gather(x, group_size):
    me = lax.axis_index("mp")
    out = jnp.zeros((group_size,) + x.shape, x.dtype)
    out = lax.dynamic_update_index_in_dim(out, x, me, 0)
    cur = x
    for step in range(1, group_size):
        cur = ring_shift(cur, group_size)
        out = lax.dynamic_update_index_in_dim(
            out, cur, jnp.remainder(me + group_size - step, group_size), 0
        )
    return out.reshape((group_size * x.shape[0],) + x.shape[1:])


def scatter_sum(partial, group_size):
    pieces = partial.reshape((group_size, -1) + partial.shape[1:])
    arrived = lax.all_to_all(pieces, "mp", split_axis=0, concat_axis=0, tiled=True)
    return jnp.sum(arrived.astype(jnp.float32), axis=0)


def broadcast_gather(local, group_size):
    sent = jnp.broadcast_to(local[None], (group_size,) + local.shape)
    arrived = lax.all_to_all(sent, "mp", split_axis=0, concat_axis=0, tiled=True)
    return arrived.reshape((group_size * local.shape[0],) + local.shape[1:])


def block_body(
    block_input,
    clusters,
    ln1_gain,
    ln1_bias,
    w_query,
    query_bias,
    w_keyval,
    value_bias,
    w_out,
    out_bias,
    ln2_gain,
    ln2_bias,
    w_up,
    up_bias,
    w_down,
    down_bias,
    cotangent,
):
    group_size = lax.axis_size("mp")
    tok_rows = block_input.shape[0]
    model_width = block_input.shape[1]
    head_count = clusters.shape[1]
    head_dim = model_width // head_count
    local_heads = head_count // group_size
    score_scale = float(head_dim) ** (-0.5)

    grad_rows = ring_gather(cotangent, group_size)

    inputs = block_input.astype(jnp.float32)
    normed_one, standard_one, factor_one = norm_forward(inputs, ln1_gain, ln1_bias)
    first = normed_one.astype(jnp.bfloat16)
    queries = (
        jnp.dot(first, w_query, preferred_element_type=jnp.float32) + query_bias
    ).astype(jnp.bfloat16)
    keyval = jnp.dot(first, w_keyval, preferred_element_type=jnp.float32)
    keyval = (keyval + jnp.concatenate([jnp.zeros_like(value_bias), value_bias])).astype(
        jnp.bfloat16
    )
    member_float = (
        clusters.T[:, None, :] == jnp.arange(CLUSTERS, dtype=jnp.int32)[None, :, None]
    ).astype(jnp.float32)
    membership = member_float.astype(jnp.bfloat16)
    query_sums = jnp.einsum(
        "hct,thd->hcd",
        membership,
        queries.reshape(tok_rows, head_count, head_dim),
        preferred_element_type=jnp.float32,
    )
    cluster_sizes = jnp.sum(member_float, axis=2)
    packed = keyval.reshape(tok_rows, 2, group_size, local_heads * head_dim)

    arrived = lax.all_to_all(packed, "mp", split_axis=2, concat_axis=0, tiled=True)
    sums_and_sizes = scatter_sum(
        jnp.concatenate([query_sums, cluster_sizes[:, :, None]], axis=2), group_size
    )

    query_sums = sums_and_sizes[:, :, :head_dim]
    cluster_sizes = sums_and_sizes[:, :, head_dim]
    divisor = jnp.maximum(cluster_sizes, 1.0)
    centroids = (query_sums / divisor[:, :, None]).astype(jnp.bfloat16)
    length = arrived.shape[0]
    key_rows = arrived[:, 0, 0].reshape(length, local_heads, head_dim)
    value_rows = arrived[:, 1, 0].reshape(length, local_heads, head_dim)
    scores = score_scale * jnp.einsum(
        "hcd,jhd->hcj", centroids, key_rows, preferred_element_type=jnp.float32
    )
    score_peak = jnp.max(scores, axis=-1, keepdims=True)
    exponent = jnp.exp(scores - score_peak)
    denominator = jnp.sum(exponent, axis=-1, keepdims=True)
    probs = exponent / denominator
    logsum = score_peak + jnp.log(denominator)
    summary = jnp.einsum(
        "hcj,jhd->hcd",
        probs.astype(jnp.bfloat16),
        value_rows,
        preferred_element_type=jnp.float32,
    ).astype(jnp.bfloat16)

    everyone = broadcast_gather(summary, group_size)

    spread = (
        jnp.einsum("hct,hcd->thd", membership, everyone, preferred_element_type=jnp.float32)
        .astype(jnp.bfloat16)
        .reshape(tok_rows, model_width)
    )
    attended = jnp.dot(spread, w_out, preferred_element_type=jnp.float32) + out_bias
    middle = inputs + attended
    normed_two, standard_two, factor_two = norm_forward(middle, ln2_gain, ln2_bias)
    second = normed_two.astype(jnp.bfloat16)
    residual = lax.optimization_barrier(middle + down_bias)

    gathered = lax.all_gather(second, "mp", axis=0, tiled=True)

    before = jnp.dot(gathered, w_up, preferred_element_type=jnp.float32) + up_bias.astype(
        jnp.float32
    )
    activated, gelu_slope = gelu_parts(before)
    hidden = activated.astype(jnp.bfloat16)
    grad_hidden = jnp.einsum("td,fd->tf", grad_rows, w_down, preferred_element_type=jnp.float32)
    grad_before = (grad_hidden * gelu_slope).astype(jnp.bfloat16)
    grad_second = lax.psum_scatter(
        jnp.einsum("tf,df->td", grad_before, w_up, preferred_element_type=jnp.float32).astype(
            jnp.bfloat16
        ),
        "mp",
        scatter_dimension=0,
        tiled=True,
    ).astype(jnp.float32)

    out_partial = jnp.dot(hidden, w_down, preferred_element_type=jnp.float32)

    upstream = cotangent.astype(jnp.float32)
    grad_down_bias = jnp.sum(upstream, axis=0)
    grad_down_t = jnp.einsum("td,tf->df", grad_rows, hidden, preferred_element_type=jnp.float32)
    bias_part = jnp.sum(grad_before.astype(jnp.float32), axis=0)
    grad_up = jnp.einsum("td,tf->df", gathered, grad_before, preferred_element_type=jnp.float32)
    grad_up_bias = lax.dynamic_update_slice(
        jnp.zeros((group_size * bias_part.shape[0],), jnp.float32),
        bias_part,
        (lax.axis_index("mp") * bias_part.shape[0],),
    )

    scores_again = score_scale * jnp.einsum(
        "hcd,jhd->hcj", centroids, key_rows, preferred_element_type=jnp.float32
    )
    probs_again = jnp.exp(scores_again - logsum)

    middle_norm_grad, grad_gain_two, grad_shift_two = norm_backward(
        grad_second, standard_two, factor_two, ln2_gain
    )
    grad_middle = upstream + middle_norm_grad
    attn_grad = grad_middle.astype(jnp.bfloat16)
    grad_out_bias = jnp.sum(attn_grad.astype(jnp.float32), axis=0)
    grad_w_out = jnp.einsum("td,te->de", spread, attn_grad, preferred_element_type=jnp.float32)
    grad_spread = jnp.einsum(
        "te,de->td", attn_grad, w_out, preferred_element_type=jnp.float32
    ).astype(jnp.bfloat16)
    summary_grad = jnp.einsum(
        "hct,thd->hcd",
        membership,
        grad_spread.reshape(tok_rows, head_count, head_dim),
        preferred_element_type=jnp.float32,
    )

    ff_grads = lax.psum_scatter(
        jnp.stack([grad_up, grad_down_t, grad_w_out]), "dp", scatter_dimension=1, tiled=True
    )

    summary_grad = scatter_sum(summary_grad, group_size).astype(jnp.bfloat16)

    grad_values = jnp.einsum(
        "hcj,hcd->jhd",
        probs_again.astype(jnp.bfloat16),
        summary_grad,
        preferred_element_type=jnp.float32,
    )
    half_width = local_heads * head_dim
    values_out = grad_values.astype(jnp.bfloat16).reshape(group_size, tok_rows, half_width)

    values_in = lax.all_to_all(values_out, "mp", split_axis=0, concat_axis=0, tiled=True)

    grad_probs = jnp.einsum(
        "hcd,jhd->hcj", summary_grad, value_rows, preferred_element_type=jnp.float32
    )
    grad_scores = probs_again * (
        grad_probs - jnp.sum(probs_again * grad_probs, axis=-1, keepdims=True)
    )
    grad_scores = grad_scores.astype(jnp.bfloat16)
    grad_centroids = (
        score_scale
        * jnp.einsum("hcj,jhd->hcd", grad_scores, key_rows, preferred_element_type=jnp.float32)
    ).astype(jnp.bfloat16)
    grad_keys = score_scale * jnp.einsum(
        "hcj,hcd->jhd", grad_scores, centroids, preferred_element_type=jnp.float32
    )
    per_member = (grad_centroids.astype(jnp.float32) / divisor[:, :, None]).astype(
        jnp.bfloat16
    )
    member_rows = per_member.size // half_width
    outgoing = jnp.concatenate(
        [
            grad_keys.astype(jnp.bfloat16).reshape(group_size, tok_rows, half_width),
            jnp.broadcast_to(
                per_member.reshape(1, member_rows, half_width),
                (group_size, member_rows, half_width),
            ),
        ],
        axis=1,
    )

    incoming = lax.all_to_all(outgoing, "mp", split_axis=0, concat_axis=0, tiled=True)

    out_pieces, _ = lax.optimization_barrier((out_partial.astype(jnp.bfloat16), incoming))
    result = scatter_sum(out_pieces, group_size)
    block_output = (residual + result).astype(jnp.bfloat16)

    keys_back = incoming[:, :tok_rows].transpose(1, 0, 2).reshape(tok_rows, model_width)
    values_back = values_in.transpose(1, 0, 2).reshape(tok_rows, model_width)
    grad_keyval = jnp.concatenate([keys_back, values_back], axis=1)
    all_member = (
        incoming[:, tok_rows:].reshape(head_count, CLUSTERS, head_dim).astype(jnp.float32)
    )
    grad_queries = jnp.einsum(
        "hct,hcd->thd", member_float, all_member, precision=lax.Precision.HIGHEST
    )
    grad_queries = grad_queries.reshape(tok_rows, model_width).astype(jnp.bfloat16)
    grad_query_bias = jnp.sum(grad_queries.astype(jnp.float32), axis=0)
    grad_value_bias = jnp.sum(grad_keyval[:, model_width:].astype(jnp.float32), axis=0)
    grad_w_attn = jnp.einsum(
        "td,te->de",
        first,
        jnp.concatenate([grad_queries, grad_keyval], axis=1),
        preferred_element_type=jnp.float32,
    )
    grad_first = jnp.einsum("te,de->td", grad_queries, w_query, preferred_element_type=jnp.float32)
    grad_first = grad_first + jnp.einsum(
        "te,de->td", grad_keyval, w_keyval, preferred_element_type=jnp.float32
    )
    input_norm_grad, grad_gain_one, grad_shift_one = norm_backward(
        grad_first, standard_one, factor_one, ln1_gain
    )
    input_grad = grad_middle + input_norm_grad
    vectors = jnp.stack(
        [
            grad_gain_one,
            grad_shift_one,
            grad_query_bias,
            grad_value_bias,
            grad_out_bias,
            grad_gain_two,
            grad_shift_two,
            grad_down_bias,
        ],
        axis=1,
    )
    up_bias_cols = grad_up_bias.reshape(model_width, -1)
    packed_grads = jnp.concatenate([grad_w_attn, vectors, up_bias_cols], axis=1)

    dp_reduced = lax.psum_scatter(packed_grads, "dp", scatter_dimension=0, tiled=True)
    attn_width = grad_w_attn.shape[1]
    reduced = scatter_sum(
        jnp.concatenate(
            [dp_reduced[:, :attn_width], ff_grads[2], dp_reduced[:, attn_width:]], axis=1
        ),
        group_size,
    )
    up_share = ff_grads[0]
    down_share = ff_grads[1].T
    col = 0
    pieces = []
    for width in (model_width, 2 * model_width, model_width):
        pieces.append(reduced[:, col : col + width])
        col += width
    vec = [reduced[:, col + i] for i in range(8)]
    col += 8
    up_bias_share = reduced[:, col:].reshape(-1)
    return (
        block_output,
        input_grad,
        vec[0],
        vec[1],
        pieces[0],
        vec[2],
        pieces[1],
        vec[3],
        pieces[2],
        vec[4],
        vec[5],
        vec[6],
        up_share,
        up_bias_share,
        down_share,
        vec[7],
    )


def solution(mesh):
    placed = (
        P(("dp", "mp"), None),
        P(("dp", "mp"), None),
        P(),
        P(),
        P(),
        P(),
        P(),
        P(),
        P(),
        P(),
        P(),
        P(),
        P(None, "mp"),
        P("mp"),
        P("mp", None),
        P(),
        P(("dp", "mp"), None),
    )
    return jax.shard_map(
        block_body,
        mesh=mesh,
        in_specs=placed,
        out_specs=(
            P(("dp", "mp"), None),
            P(("dp", "mp"), None),
            P(("dp", "mp")),
            P(("dp", "mp")),
            P(("dp", "mp"), None),
            P(("dp", "mp")),
            P(("dp", "mp"), None),
            P(("dp", "mp")),
            P(("dp", "mp"), None),
            P(("dp", "mp")),
            P(("dp", "mp")),
            P(("dp", "mp")),
            P("dp", "mp"),
            P(("dp", "mp")),
            P("mp", "dp"),
            P(("dp", "mp")),
        ),
        check_vma=False,
    )
```

```python
import math

import jax
import jax.numpy as jnp
from jax import lax
from jax.sharding import PartitionSpec as P


CLUSTERS = 100


epsilon = 1e-05


def norm_forward(inputs, gain_vec, offset):
    center = inputs - jnp.mean(inputs, axis=-1, keepdims=True)
    factor = lax.rsqrt(jnp.mean(center * center, axis=-1, keepdims=True) + epsilon)
    standard = center * factor
    return (standard * gain_vec + offset, standard, factor)


def norm_backward(upstream, standard, factor, gain_vec):
    scaled = upstream * gain_vec
    centred = scaled - jnp.mean(scaled, axis=-1, keepdims=True)
    centred = centred - standard * jnp.mean(scaled * standard, axis=-1, keepdims=True)
    return (factor * centred, jnp.sum(upstream * standard, axis=0), jnp.sum(upstream, axis=0))


def gelu_parts(before):
    cumulative = 0.5 * (1.0 + jax.scipy.special.erf(before / math.sqrt(2.0)))
    density = jnp.exp(-0.5 * before * before) / math.sqrt(2.0 * math.pi)
    return (before * cumulative, cumulative + before * density)


def scatter_sum(partial, group_size):
    pieces = partial.reshape((group_size, -1) + partial.shape[1:])
    arrived = lax.all_to_all(pieces, "mp", split_axis=0, concat_axis=0, tiled=True)
    return jnp.sum(arrived.astype(jnp.float32), axis=0)


def broadcast_gather(local, group_size):
    sent = jnp.broadcast_to(local[None], (group_size,) + local.shape)
    arrived = lax.all_to_all(sent, "mp", split_axis=0, concat_axis=0, tiled=True)
    return arrived.reshape((group_size * local.shape[0],) + local.shape[1:])


def block_body(
    block_input,
    clusters,
    ln1_gain,
    ln1_bias,
    w_query,
    query_bias,
    w_keyval,
    value_bias,
    w_out,
    out_bias,
    ln2_gain,
    ln2_bias,
    w_up,
    up_bias,
    w_down,
    down_bias,
    cotangent,
):
    group_size = lax.axis_size("mp")
    tok_rows = block_input.shape[0]
    model_width = block_input.shape[1]
    head_count = clusters.shape[1]
    head_dim = model_width // head_count
    local_heads = head_count // group_size
    score_scale = float(head_dim) ** (-0.5)

    grad_rows = lax.all_gather(cotangent, "mp", axis=0, tiled=True)

    inputs = block_input.astype(jnp.float32)
    normed_one, standard_one, factor_one = norm_forward(inputs, ln1_gain, ln1_bias)
    first = normed_one.astype(jnp.bfloat16)
    queries = (
        jnp.dot(first, w_query, preferred_element_type=jnp.float32) + query_bias
    ).astype(jnp.bfloat16)
    keyval = jnp.dot(first, w_keyval, preferred_element_type=jnp.float32)
    keyval = (keyval + jnp.concatenate([jnp.zeros_like(value_bias), value_bias])).astype(
        jnp.bfloat16
    )
    member_float = (
        clusters.T[:, None, :] == jnp.arange(CLUSTERS, dtype=jnp.int32)[None, :, None]
    ).astype(jnp.float32)
    membership = member_float.astype(jnp.bfloat16)
    query_sums = jnp.einsum(
        "hct,thd->hcd",
        membership,
        queries.reshape(tok_rows, head_count, head_dim),
        preferred_element_type=jnp.float32,
    )
    cluster_sizes = jnp.sum(member_float, axis=2)
    size_high = jnp.floor(cluster_sizes / 256.0)
    size_low = cluster_sizes - 256.0 * size_high
    partial = jnp.concatenate(
        [query_sums, size_high[:, :, None], size_low[:, :, None]], axis=2
    ).reshape(group_size, -1)
    partial_size = partial.shape[1]
    half_width = local_heads * head_dim
    extra_rows = -(-partial_size // (2 * half_width))
    partial = jnp.pad(partial, ((0, 0), (0, extra_rows * 2 * half_width - partial_size)))
    extra = (
        partial.reshape(group_size, extra_rows, 2, half_width)
        .transpose(1, 2, 0, 3)
        .astype(jnp.bfloat16)
    )
    packed = jnp.concatenate([keyval.reshape(tok_rows, 2, group_size, half_width), extra], axis=0)

    arrived = lax.all_to_all(packed, "mp", split_axis=2, concat_axis=0, tiled=True)

    blocks = arrived.reshape(group_size, tok_rows + extra_rows, 2, half_width)
    sums_and_sizes = jnp.sum(
        blocks[:, tok_rows:]
        .reshape(group_size, -1)[:, :partial_size]
        .reshape(group_size, local_heads, CLUSTERS, head_dim + 2)
        .astype(jnp.float32),
        axis=0,
    )
    query_sums = sums_and_sizes[:, :, :head_dim]
    cluster_sizes = 256.0 * sums_and_sizes[:, :, head_dim] + sums_and_sizes[:, :, head_dim + 1]
    divisor = jnp.maximum(cluster_sizes, 1.0)
    centroids = (query_sums / divisor[:, :, None]).astype(jnp.bfloat16)
    kv_rows = blocks[:, :tok_rows].reshape(group_size * tok_rows, 2, half_width)
    length = kv_rows.shape[0]
    key_rows = kv_rows[:, 0].reshape(length, local_heads, head_dim)
    value_rows = kv_rows[:, 1].reshape(length, local_heads, head_dim)
    scores = score_scale * jnp.einsum(
        "hcd,jhd->hcj", centroids, key_rows, preferred_element_type=jnp.float32
    )
    score_peak = jnp.max(scores, axis=-1, keepdims=True)
    exponent = jnp.exp(scores - score_peak)
    denominator = jnp.sum(exponent, axis=-1, keepdims=True)
    probs = exponent / denominator
    logsum = score_peak + jnp.log(denominator)
    summary = jnp.einsum(
        "hcj,jhd->hcd",
        probs.astype(jnp.bfloat16),
        value_rows,
        preferred_element_type=jnp.float32,
    ).astype(jnp.bfloat16)

    everyone = broadcast_gather(summary, group_size)

    spread = (
        jnp.einsum("hct,hcd->thd", membership, everyone, preferred_element_type=jnp.float32)
        .astype(jnp.bfloat16)
        .reshape(tok_rows, model_width)
    )
    attended = jnp.dot(spread, w_out, preferred_element_type=jnp.float32) + out_bias
    middle = inputs + attended
    normed_two, standard_two, factor_two = norm_forward(middle, ln2_gain, ln2_bias)
    second = normed_two.astype(jnp.bfloat16)
    residual = lax.optimization_barrier(middle + down_bias)

    gathered = lax.all_gather(second, "mp", axis=0, tiled=True)

    before = jnp.dot(gathered, w_up, preferred_element_type=jnp.float32) + up_bias.astype(
        jnp.float32
    )
    activated, gelu_slope = gelu_parts(before)
    hidden = activated.astype(jnp.bfloat16)
    grad_hidden = jnp.einsum("td,fd->tf", grad_rows, w_down, preferred_element_type=jnp.float32)
    grad_before = (grad_hidden * gelu_slope).astype(jnp.bfloat16)
    grad_second = lax.psum_scatter(
        jnp.einsum("tf,df->td", grad_before, w_up, preferred_element_type=jnp.float32).astype(
            jnp.bfloat16
        ),
        "mp",
        scatter_dimension=0,
        tiled=True,
    ).astype(jnp.float32)

    out_partial = jnp.dot(hidden, w_down, preferred_element_type=jnp.float32)

    upstream = cotangent.astype(jnp.float32)
    grad_down_bias = jnp.sum(upstream, axis=0)
    grad_down_t = jnp.einsum("td,tf->df", grad_rows, hidden, preferred_element_type=jnp.float32)
    bias_part = jnp.sum(grad_before.astype(jnp.float32), axis=0)
    grad_up = jnp.einsum("td,tf->df", gathered, grad_before, preferred_element_type=jnp.float32)
    grad_up_bias = lax.dynamic_update_slice(
        jnp.zeros((group_size * bias_part.shape[0],), jnp.float32),
        bias_part,
        (lax.axis_index("mp") * bias_part.shape[0],),
    )

    scores_again = score_scale * jnp.einsum(
        "hcd,jhd->hcj", centroids, key_rows, preferred_element_type=jnp.float32
    )
    probs_again = jnp.exp(scores_again - logsum)

    middle_norm_grad, grad_gain_two, grad_shift_two = norm_backward(
        grad_second, standard_two, factor_two, ln2_gain
    )
    grad_middle = upstream + middle_norm_grad
    attn_grad = grad_middle.astype(jnp.bfloat16)
    grad_out_bias = jnp.sum(attn_grad.astype(jnp.float32), axis=0)
    grad_w_out = jnp.einsum("td,te->de", spread, attn_grad, preferred_element_type=jnp.float32)
    grad_spread = jnp.einsum(
        "te,de->td", attn_grad, w_out, preferred_element_type=jnp.float32
    ).astype(jnp.bfloat16)
    summary_grad = jnp.einsum(
        "hct,thd->hcd",
        membership,
        grad_spread.reshape(tok_rows, head_count, head_dim),
        preferred_element_type=jnp.float32,
    )

    ff_grads = lax.psum_scatter(
        jnp.stack([grad_up, grad_down_t, grad_w_out]), "dp", scatter_dimension=1, tiled=True
    )

    summary_grad = scatter_sum(summary_grad, group_size).astype(jnp.bfloat16)

    grad_values = jnp.einsum(
        "hcj,hcd->jhd",
        probs_again.astype(jnp.bfloat16),
        summary_grad,
        preferred_element_type=jnp.float32,
    )
    half_width = local_heads * head_dim
    values_out = grad_values.astype(jnp.bfloat16).reshape(group_size, tok_rows, half_width)

    values_in = lax.all_to_all(values_out, "mp", split_axis=0, concat_axis=0, tiled=True)

    grad_probs = jnp.einsum(
        "hcd,jhd->hcj", summary_grad, value_rows, preferred_element_type=jnp.float32
    )
    grad_scores = probs_again * (
        grad_probs - jnp.sum(probs_again * grad_probs, axis=-1, keepdims=True)
    )
    grad_scores = grad_scores.astype(jnp.bfloat16)
    grad_centroids = (
        score_scale
        * jnp.einsum("hcj,jhd->hcd", grad_scores, key_rows, preferred_element_type=jnp.float32)
    ).astype(jnp.bfloat16)
    grad_keys = score_scale * jnp.einsum(
        "hcj,hcd->jhd", grad_scores, centroids, preferred_element_type=jnp.float32
    )
    per_member = (grad_centroids.astype(jnp.float32) / divisor[:, :, None]).astype(
        jnp.bfloat16
    )
    member_rows = per_member.size // half_width
    outgoing = jnp.concatenate(
        [
            grad_keys.astype(jnp.bfloat16).reshape(group_size, tok_rows, half_width),
            jnp.broadcast_to(
                per_member.reshape(1, member_rows, half_width),
                (group_size, member_rows, half_width),
            ),
        ],
        axis=1,
    )

    incoming = lax.all_to_all(outgoing, "mp", split_axis=0, concat_axis=0, tiled=True)

    out_pieces, _ = lax.optimization_barrier((out_partial.astype(jnp.bfloat16), incoming))
    result = scatter_sum(out_pieces, group_size)
    block_output = (residual + result).astype(jnp.bfloat16)

    keys_back = incoming[:, :tok_rows].transpose(1, 0, 2).reshape(tok_rows, model_width)
    values_back = values_in.transpose(1, 0, 2).reshape(tok_rows, model_width)
    grad_keyval = jnp.concatenate([keys_back, values_back], axis=1)
    all_member = (
        incoming[:, tok_rows:].reshape(head_count, CLUSTERS, head_dim).astype(jnp.float32)
    )
    grad_queries = jnp.einsum(
        "hct,hcd->thd", member_float, all_member, precision=lax.Precision.HIGHEST
    )
    grad_queries = grad_queries.reshape(tok_rows, model_width).astype(jnp.bfloat16)
    grad_query_bias = jnp.sum(grad_queries.astype(jnp.float32), axis=0)
    grad_value_bias = jnp.sum(grad_keyval[:, model_width:].astype(jnp.float32), axis=0)
    grad_w_attn = jnp.einsum(
        "td,te->de",
        first,
        jnp.concatenate([grad_queries, grad_keyval], axis=1),
        preferred_element_type=jnp.float32,
    )
    grad_first = jnp.einsum("te,de->td", grad_queries, w_query, preferred_element_type=jnp.float32)
    grad_first = grad_first + jnp.einsum(
        "te,de->td", grad_keyval, w_keyval, preferred_element_type=jnp.float32
    )
    input_norm_grad, grad_gain_one, grad_shift_one = norm_backward(
        grad_first, standard_one, factor_one, ln1_gain
    )
    input_grad = grad_middle + input_norm_grad
    vectors = jnp.stack(
        [
            grad_gain_one,
            grad_shift_one,
            grad_query_bias,
            grad_value_bias,
            grad_out_bias,
            grad_gain_two,
            grad_shift_two,
            grad_down_bias,
        ],
        axis=1,
    )
    up_bias_cols = grad_up_bias.reshape(model_width, -1)
    packed_grads = jnp.concatenate([grad_w_attn, vectors, up_bias_cols], axis=1)

    dp_reduced = lax.psum_scatter(packed_grads, "dp", scatter_dimension=0, tiled=True)
    attn_width = grad_w_attn.shape[1]
    reduced = scatter_sum(
        jnp.concatenate(
            [dp_reduced[:, :attn_width], ff_grads[2], dp_reduced[:, attn_width:]], axis=1
        ),
        group_size,
    )
    up_share = ff_grads[0]
    down_share = ff_grads[1].T
    col = 0
    pieces = []
    for width in (model_width, 2 * model_width, model_width):
        pieces.append(reduced[:, col : col + width])
        col += width
    vec = [reduced[:, col + i] for i in range(8)]
    col += 8
    up_bias_share = reduced[:, col:].reshape(-1)
    return (
        block_output,
        input_grad,
        vec[0],
        vec[1],
        pieces[0],
        vec[2],
        pieces[1],
        vec[3],
        pieces[2],
        vec[4],
        vec[5],
        vec[6],
        up_share,
        up_bias_share,
        down_share,
        vec[7],
    )


def solution(mesh):
    placed = (
        P(("dp", "mp"), None),
        P(("dp", "mp"), None),
        P(),
        P(),
        P(),
        P(),
        P(),
        P(),
        P(),
        P(),
        P(),
        P(),
        P(None, "mp"),
        P("mp"),
        P("mp", None),
        P(),
        P(("dp", "mp"), None),
    )
    return jax.shard_map(
        block_body,
        mesh=mesh,
        in_specs=placed,
        out_specs=(
            P(("dp", "mp"), None),
            P(("dp", "mp"), None),
            P(("dp", "mp")),
            P(("dp", "mp")),
            P(("dp", "mp"), None),
            P(("dp", "mp")),
            P(("dp", "mp"), None),
            P(("dp", "mp")),
            P(("dp", "mp"), None),
            P(("dp", "mp")),
            P(("dp", "mp")),
            P(("dp", "mp")),
            P("dp", "mp"),
            P(("dp", "mp")),
            P("mp", "dp"),
            P(("dp", "mp")),
        ),
        check_vma=False,
    )
```

```python
import math

import jax
import jax.numpy as jnp
from jax import lax
from jax.sharding import PartitionSpec as P


CLUSTERS = 100


epsilon = 1e-05


def norm_forward(inputs, gain_vec, offset):
    center = inputs - jnp.mean(inputs, axis=-1, keepdims=True)
    factor = lax.rsqrt(jnp.mean(center * center, axis=-1, keepdims=True) + epsilon)
    standard = center * factor
    return (standard * gain_vec + offset, standard, factor)


def norm_backward(upstream, standard, factor, gain_vec):
    scaled = upstream * gain_vec
    centred = scaled - jnp.mean(scaled, axis=-1, keepdims=True)
    centred = centred - standard * jnp.mean(scaled * standard, axis=-1, keepdims=True)
    return (factor * centred, jnp.sum(upstream * standard, axis=0), jnp.sum(upstream, axis=0))


def gelu_parts(before):
    cumulative = 0.5 * (1.0 + jax.scipy.special.erf(before / math.sqrt(2.0)))
    density = jnp.exp(-0.5 * before * before) / math.sqrt(2.0 * math.pi)
    return (before * cumulative, cumulative + before * density)


def scatter_sum(partial, group_size):
    pieces = partial.reshape((group_size, -1) + partial.shape[1:])
    arrived = lax.all_to_all(pieces, "mp", split_axis=0, concat_axis=0, tiled=True)
    return jnp.sum(arrived.astype(jnp.float32), axis=0)


def broadcast_gather(local, group_size):
    sent = jnp.broadcast_to(local[None], (group_size,) + local.shape)
    arrived = lax.all_to_all(sent, "mp", split_axis=0, concat_axis=0, tiled=True)
    return arrived.reshape((group_size * local.shape[0],) + local.shape[1:])


def block_body(
    block_input,
    clusters,
    ln1_gain,
    ln1_bias,
    w_query,
    query_bias,
    w_keyval,
    value_bias,
    w_out,
    out_bias,
    ln2_gain,
    ln2_bias,
    w_up,
    up_bias,
    w_down,
    down_bias,
    cotangent,
):
    group_size = lax.axis_size("mp")
    tok_rows = block_input.shape[0]
    model_width = block_input.shape[1]
    head_count = clusters.shape[1]
    head_dim = model_width // head_count
    local_heads = head_count // group_size
    score_scale = float(head_dim) ** (-0.5)

    grad_rows = lax.all_gather(cotangent, "mp", axis=0, tiled=True)

    inputs = block_input.astype(jnp.float32)
    normed_one, standard_one, factor_one = norm_forward(inputs, ln1_gain, ln1_bias)
    first = normed_one.astype(jnp.bfloat16)
    queries = (
        jnp.dot(first, w_query, preferred_element_type=jnp.float32) + query_bias
    ).astype(jnp.bfloat16)
    keyval = jnp.dot(first, w_keyval, preferred_element_type=jnp.float32)
    keyval = (keyval + jnp.concatenate([jnp.zeros_like(value_bias), value_bias])).astype(
        jnp.bfloat16
    )
    member_float = (
        clusters.T[:, None, :] == jnp.arange(CLUSTERS, dtype=jnp.int32)[None, :, None]
    ).astype(jnp.float32)
    membership = member_float.astype(jnp.bfloat16)
    query_sums = jnp.einsum(
        "hct,thd->hcd",
        membership,
        queries.reshape(tok_rows, head_count, head_dim),
        preferred_element_type=jnp.float32,
    )
    cluster_sizes = jnp.sum(member_float, axis=2)
    packed = keyval.reshape(tok_rows, 2, group_size, local_heads * head_dim)

    arrived = lax.all_to_all(packed, "mp", split_axis=2, concat_axis=0, tiled=True)
    sums_and_sizes = scatter_sum(
        jnp.concatenate([query_sums, cluster_sizes[:, :, None]], axis=2), group_size
    )

    query_sums = sums_and_sizes[:, :, :head_dim]
    cluster_sizes = sums_and_sizes[:, :, head_dim]
    divisor = jnp.maximum(cluster_sizes, 1.0)
    centroids = (query_sums / divisor[:, :, None]).astype(jnp.bfloat16)
    length = arrived.shape[0]
    key_rows = arrived[:, 0, 0].reshape(length, local_heads, head_dim)
    value_rows = arrived[:, 1, 0].reshape(length, local_heads, head_dim)
    scores = score_scale * jnp.einsum(
        "hcd,jhd->hcj", centroids, key_rows, preferred_element_type=jnp.float32
    )
    score_peak = jnp.max(scores, axis=-1, keepdims=True)
    exponent = jnp.exp(scores - score_peak)
    denominator = jnp.sum(exponent, axis=-1, keepdims=True)
    probs = exponent / denominator
    logsum = score_peak + jnp.log(denominator)
    summary = jnp.einsum(
        "hcj,jhd->hcd",
        probs.astype(jnp.bfloat16),
        value_rows,
        preferred_element_type=jnp.float32,
    ).astype(jnp.bfloat16)

    everyone = broadcast_gather(summary, group_size)

    spread = (
        jnp.einsum("hct,hcd->thd", membership, everyone, preferred_element_type=jnp.float32)
        .astype(jnp.bfloat16)
        .reshape(tok_rows, model_width)
    )
    attended = jnp.dot(spread, w_out, preferred_element_type=jnp.float32) + out_bias
    middle = inputs + attended
    normed_two, standard_two, factor_two = norm_forward(middle, ln2_gain, ln2_bias)
    second = normed_two.astype(jnp.bfloat16)
    residual = lax.optimization_barrier(middle + down_bias)

    gathered = lax.all_gather(second, "mp", axis=0, tiled=True)

    grad_hidden = lax.optimization_barrier(
        jnp.einsum("td,fd->tf", grad_rows, w_down, preferred_element_type=jnp.float32)
    )

    before = jnp.dot(gathered, w_up, preferred_element_type=jnp.float32) + up_bias.astype(
        jnp.float32
    )
    activated, gelu_slope = gelu_parts(before)
    hidden = activated.astype(jnp.bfloat16)
    grad_before = (grad_hidden * gelu_slope).astype(jnp.bfloat16)
    grad_second = lax.psum_scatter(
        jnp.einsum("tf,df->td", grad_before, w_up, preferred_element_type=jnp.float32).astype(
            jnp.bfloat16
        ),
        "mp",
        scatter_dimension=0,
        tiled=True,
    ).astype(jnp.float32)

    out_partial = jnp.dot(hidden, w_down, preferred_element_type=jnp.float32)

    upstream = cotangent.astype(jnp.float32)
    grad_down_bias = jnp.sum(upstream, axis=0)
    grad_down_t = jnp.einsum("td,tf->df", grad_rows, hidden, preferred_element_type=jnp.float32)
    bias_part = jnp.sum(grad_before.astype(jnp.float32), axis=0)
    grad_up = jnp.einsum("td,tf->df", gathered, grad_before, preferred_element_type=jnp.float32)
    grad_up_bias = lax.dynamic_update_slice(
        jnp.zeros((group_size * bias_part.shape[0],), jnp.float32),
        bias_part,
        (lax.axis_index("mp") * bias_part.shape[0],),
    )

    scores_again = score_scale * jnp.einsum(
        "hcd,jhd->hcj", centroids, key_rows, preferred_element_type=jnp.float32
    )
    probs_again = jnp.exp(scores_again - logsum)

    middle_norm_grad, grad_gain_two, grad_shift_two = norm_backward(
        grad_second, standard_two, factor_two, ln2_gain
    )
    grad_middle = upstream + middle_norm_grad
    attn_grad = grad_middle.astype(jnp.bfloat16)
    grad_out_bias = jnp.sum(attn_grad.astype(jnp.float32), axis=0)
    grad_w_out = jnp.einsum("td,te->de", spread, attn_grad, preferred_element_type=jnp.float32)
    grad_spread = jnp.einsum(
        "te,de->td", attn_grad, w_out, preferred_element_type=jnp.float32
    ).astype(jnp.bfloat16)
    summary_grad = jnp.einsum(
        "hct,thd->hcd",
        membership,
        grad_spread.reshape(tok_rows, head_count, head_dim),
        preferred_element_type=jnp.float32,
    )

    ff_grads = lax.psum_scatter(
        jnp.stack([grad_up, grad_down_t, grad_w_out]), "dp", scatter_dimension=1, tiled=True
    )

    summary_grad = scatter_sum(summary_grad, group_size).astype(jnp.bfloat16)

    grad_values = jnp.einsum(
        "hcj,hcd->jhd",
        probs_again.astype(jnp.bfloat16),
        summary_grad,
        preferred_element_type=jnp.float32,
    )
    half_width = local_heads * head_dim
    values_out = grad_values.astype(jnp.bfloat16).reshape(group_size, tok_rows, half_width)

    values_in = lax.all_to_all(values_out, "mp", split_axis=0, concat_axis=0, tiled=True)

    grad_probs = jnp.einsum(
        "hcd,jhd->hcj", summary_grad, value_rows, preferred_element_type=jnp.float32
    )
    grad_scores = probs_again * (
        grad_probs - jnp.sum(probs_again * grad_probs, axis=-1, keepdims=True)
    )
    grad_scores = grad_scores.astype(jnp.bfloat16)
    grad_centroids = (
        score_scale
        * jnp.einsum("hcj,jhd->hcd", grad_scores, key_rows, preferred_element_type=jnp.float32)
    ).astype(jnp.bfloat16)
    grad_keys = score_scale * jnp.einsum(
        "hcj,hcd->jhd", grad_scores, centroids, preferred_element_type=jnp.float32
    )
    per_member = (grad_centroids.astype(jnp.float32) / divisor[:, :, None]).astype(
        jnp.bfloat16
    )
    member_rows = per_member.size // half_width
    outgoing = jnp.concatenate(
        [
            grad_keys.astype(jnp.bfloat16).reshape(group_size, tok_rows, half_width),
            jnp.broadcast_to(
                per_member.reshape(1, member_rows, half_width),
                (group_size, member_rows, half_width),
            ),
        ],
        axis=1,
    )

    incoming = lax.all_to_all(outgoing, "mp", split_axis=0, concat_axis=0, tiled=True)

    out_pieces, _ = lax.optimization_barrier((out_partial.astype(jnp.bfloat16), incoming))
    result = scatter_sum(out_pieces, group_size)
    block_output = (residual + result).astype(jnp.bfloat16)

    keys_back = incoming[:, :tok_rows].transpose(1, 0, 2).reshape(tok_rows, model_width)
    values_back = values_in.transpose(1, 0, 2).reshape(tok_rows, model_width)
    grad_keyval = jnp.concatenate([keys_back, values_back], axis=1)
    all_member = (
        incoming[:, tok_rows:].reshape(head_count, CLUSTERS, head_dim).astype(jnp.float32)
    )
    grad_queries = jnp.einsum(
        "hct,hcd->thd", member_float, all_member, precision=lax.Precision.HIGHEST
    )
    grad_queries = grad_queries.reshape(tok_rows, model_width).astype(jnp.bfloat16)
    grad_query_bias = jnp.sum(grad_queries.astype(jnp.float32), axis=0)
    grad_value_bias = jnp.sum(grad_keyval[:, model_width:].astype(jnp.float32), axis=0)
    grad_w_attn = jnp.einsum(
        "td,te->de",
        first,
        jnp.concatenate([grad_queries, grad_keyval], axis=1),
        preferred_element_type=jnp.float32,
    )
    grad_first = jnp.einsum("te,de->td", grad_queries, w_query, preferred_element_type=jnp.float32)
    grad_first = grad_first + jnp.einsum(
        "te,de->td", grad_keyval, w_keyval, preferred_element_type=jnp.float32
    )
    input_norm_grad, grad_gain_one, grad_shift_one = norm_backward(
        grad_first, standard_one, factor_one, ln1_gain
    )
    input_grad = grad_middle + input_norm_grad
    vectors = jnp.stack(
        [
            grad_gain_one,
            grad_shift_one,
            grad_query_bias,
            grad_value_bias,
            grad_out_bias,
            grad_gain_two,
            grad_shift_two,
            grad_down_bias,
        ],
        axis=1,
    )
    up_bias_cols = grad_up_bias.reshape(model_width, -1)
    packed_grads = jnp.concatenate([grad_w_attn, vectors, up_bias_cols], axis=1)

    dp_reduced = lax.psum_scatter(packed_grads, "dp", scatter_dimension=0, tiled=True)
    attn_width = grad_w_attn.shape[1]
    reduced = scatter_sum(
        jnp.concatenate(
            [dp_reduced[:, :attn_width], ff_grads[2], dp_reduced[:, attn_width:]], axis=1
        ),
        group_size,
    )
    up_share = ff_grads[0]
    down_share = ff_grads[1].T
    col = 0
    pieces = []
    for width in (model_width, 2 * model_width, model_width):
        pieces.append(reduced[:, col : col + width])
        col += width
    vec = [reduced[:, col + i] for i in range(8)]
    col += 8
    up_bias_share = reduced[:, col:].reshape(-1)
    return (
        block_output,
        input_grad,
        vec[0],
        vec[1],
        pieces[0],
        vec[2],
        pieces[1],
        vec[3],
        pieces[2],
        vec[4],
        vec[5],
        vec[6],
        up_share,
        up_bias_share,
        down_share,
        vec[7],
    )


def solution(mesh):
    placed = (
        P(("dp", "mp"), None),
        P(("dp", "mp"), None),
        P(),
        P(),
        P(),
        P(),
        P(),
        P(),
        P(),
        P(),
        P(),
        P(),
        P(None, "mp"),
        P("mp"),
        P("mp", None),
        P(),
        P(("dp", "mp"), None),
    )
    return jax.shard_map(
        block_body,
        mesh=mesh,
        in_specs=placed,
        out_specs=(
            P(("dp", "mp"), None),
            P(("dp", "mp"), None),
            P(("dp", "mp")),
            P(("dp", "mp")),
            P(("dp", "mp"), None),
            P(("dp", "mp")),
            P(("dp", "mp"), None),
            P(("dp", "mp")),
            P(("dp", "mp"), None),
            P(("dp", "mp")),
            P(("dp", "mp")),
            P(("dp", "mp")),
            P("dp", "mp"),
            P(("dp", "mp")),
            P("mp", "dp"),
            P(("dp", "mp")),
        ),
        check_vma=False,
    )
```

```python
import math

import jax
import jax.numpy as jnp
from jax import lax
from jax.sharding import PartitionSpec as P


CLUSTERS = 100


epsilon = 1e-05


def norm_forward(inputs, gain_vec, offset):
    center = inputs - jnp.mean(inputs, axis=-1, keepdims=True)
    factor = lax.rsqrt(jnp.mean(center * center, axis=-1, keepdims=True) + epsilon)
    standard = center * factor
    return (standard * gain_vec + offset, standard, factor)


def norm_backward(upstream, standard, factor, gain_vec):
    scaled = upstream * gain_vec
    centred = scaled - jnp.mean(scaled, axis=-1, keepdims=True)
    centred = centred - standard * jnp.mean(scaled * standard, axis=-1, keepdims=True)
    return (factor * centred, jnp.sum(upstream * standard, axis=0), jnp.sum(upstream, axis=0))


def gelu_parts(before):
    cumulative = 0.5 * (1.0 + jax.scipy.special.erf(before / math.sqrt(2.0)))
    density = jnp.exp(-0.5 * before * before) / math.sqrt(2.0 * math.pi)
    return (before * cumulative, cumulative + before * density)


def scatter_sum(partial, group_size):
    pieces = partial.reshape((group_size, -1) + partial.shape[1:])
    arrived = lax.all_to_all(pieces, "mp", split_axis=0, concat_axis=0, tiled=True)
    return jnp.sum(arrived.astype(jnp.float32), axis=0)


def broadcast_gather(local, group_size):
    sent = jnp.broadcast_to(local[None], (group_size,) + local.shape)
    arrived = lax.all_to_all(sent, "mp", split_axis=0, concat_axis=0, tiled=True)
    return arrived.reshape((group_size * local.shape[0],) + local.shape[1:])


def block_body(
    block_input,
    clusters,
    ln1_gain,
    ln1_bias,
    w_query,
    query_bias,
    w_keyval,
    value_bias,
    w_out,
    out_bias,
    ln2_gain,
    ln2_bias,
    w_up,
    up_bias,
    w_down,
    down_bias,
    cotangent,
):
    group_size = lax.axis_size("mp")
    tok_rows = block_input.shape[0]
    model_width = block_input.shape[1]
    head_count = clusters.shape[1]
    head_dim = model_width // head_count
    local_heads = head_count // group_size
    score_scale = float(head_dim) ** (-0.5)

    grad_rows = lax.all_gather(cotangent, "mp", axis=0, tiled=True)

    inputs = block_input.astype(jnp.float32)
    normed_one, standard_one, factor_one = norm_forward(inputs, ln1_gain, ln1_bias)
    first = normed_one.astype(jnp.bfloat16)
    queries = (
        jnp.dot(first, w_query, preferred_element_type=jnp.float32) + query_bias
    ).astype(jnp.bfloat16)
    keyval = jnp.dot(first, w_keyval, preferred_element_type=jnp.float32)
    keyval = (keyval + jnp.concatenate([jnp.zeros_like(value_bias), value_bias])).astype(
        jnp.bfloat16
    )
    member_float = (
        clusters.T[:, None, :] == jnp.arange(CLUSTERS, dtype=jnp.int32)[None, :, None]
    ).astype(jnp.float32)
    membership = member_float.astype(jnp.bfloat16)
    query_sums = jnp.einsum(
        "hct,thd->hcd",
        membership,
        queries.reshape(tok_rows, head_count, head_dim),
        preferred_element_type=jnp.float32,
    )
    cluster_sizes = jnp.sum(member_float, axis=2)
    packed = keyval.reshape(tok_rows, 2, group_size, local_heads * head_dim)

    arrived = lax.all_to_all(packed, "mp", split_axis=2, concat_axis=0, tiled=True)
    sums_and_sizes = scatter_sum(
        jnp.concatenate([query_sums, cluster_sizes[:, :, None]], axis=2), group_size
    )

    query_sums = sums_and_sizes[:, :, :head_dim]
    cluster_sizes = sums_and_sizes[:, :, head_dim]
    divisor = jnp.maximum(cluster_sizes, 1.0)
    centroids = (query_sums / divisor[:, :, None]).astype(jnp.bfloat16)
    length = arrived.shape[0]
    key_rows = arrived[:, 0, 0].reshape(length, local_heads, head_dim)
    value_rows = arrived[:, 1, 0].reshape(length, local_heads, head_dim)
    scores = score_scale * jnp.einsum(
        "hcd,jhd->hcj", centroids, key_rows, preferred_element_type=jnp.float32
    )
    score_peak = jnp.max(scores, axis=-1, keepdims=True)
    exponent = jnp.exp(scores - score_peak)
    denominator = jnp.sum(exponent, axis=-1, keepdims=True)
    probs = exponent / denominator
    logsum = score_peak + jnp.log(denominator)
    summary = jnp.einsum(
        "hcj,jhd->hcd",
        probs.astype(jnp.bfloat16),
        value_rows,
        preferred_element_type=jnp.float32,
    ).astype(jnp.bfloat16)

    everyone = broadcast_gather(summary, group_size)

    spread = (
        jnp.einsum("hct,hcd->thd", membership, everyone, preferred_element_type=jnp.float32)
        .astype(jnp.bfloat16)
        .reshape(tok_rows, model_width)
    )
    attended = jnp.dot(spread, w_out, preferred_element_type=jnp.float32) + out_bias
    middle = inputs + attended
    normed_two, standard_two, factor_two = norm_forward(middle, ln2_gain, ln2_bias)
    second = normed_two.astype(jnp.bfloat16)
    residual = lax.optimization_barrier(middle + down_bias)

    gathered = lax.all_gather(second, "mp", axis=0, tiled=True)

    before = jnp.dot(gathered, w_up, preferred_element_type=jnp.float32) + up_bias.astype(
        jnp.float32
    )
    activated, gelu_slope = gelu_parts(before)
    hidden = activated.astype(jnp.bfloat16)
    grad_hidden = jnp.einsum("td,fd->tf", grad_rows, w_down, preferred_element_type=jnp.float32)
    grad_before = (grad_hidden * gelu_slope).astype(jnp.bfloat16)
    grad_second = lax.psum_scatter(
        jnp.einsum("tf,df->td", grad_before, w_up, preferred_element_type=jnp.float32).astype(
            jnp.bfloat16
        ),
        "mp",
        scatter_dimension=0,
        tiled=True,
    ).astype(jnp.float32)

    out_partial = jnp.dot(hidden, w_down, preferred_element_type=jnp.float32)

    upstream = cotangent.astype(jnp.float32)
    grad_down_bias = jnp.sum(upstream, axis=0)
    grad_down_t = jnp.einsum("td,tf->df", grad_rows, hidden, preferred_element_type=jnp.float32)
    bias_part = jnp.sum(grad_before.astype(jnp.float32), axis=0)
    grad_up = jnp.einsum("td,tf->df", gathered, grad_before, preferred_element_type=jnp.float32)
    grad_up_bias = lax.dynamic_update_slice(
        jnp.zeros((group_size * bias_part.shape[0],), jnp.float32),
        bias_part,
        (lax.axis_index("mp") * bias_part.shape[0],),
    )

    scores_again = score_scale * jnp.einsum(
        "hcd,jhd->hcj", centroids, key_rows, preferred_element_type=jnp.float32
    )
    probs_again = jnp.exp(scores_again - logsum)

    middle_norm_grad, grad_gain_two, grad_shift_two = norm_backward(
        grad_second, standard_two, factor_two, ln2_gain
    )
    grad_middle = upstream + middle_norm_grad
    attn_grad = grad_middle.astype(jnp.bfloat16)
    grad_out_bias = jnp.sum(attn_grad.astype(jnp.float32), axis=0)
    grad_w_out = jnp.einsum("td,te->de", spread, attn_grad, preferred_element_type=jnp.float32)
    grad_spread = jnp.einsum(
        "te,de->td", attn_grad, w_out, preferred_element_type=jnp.float32
    ).astype(jnp.bfloat16)
    summary_grad = jnp.einsum(
        "hct,thd->hcd",
        membership,
        grad_spread.reshape(tok_rows, head_count, head_dim),
        preferred_element_type=jnp.float32,
    )

    ff_grads = lax.psum_scatter(
        jnp.stack([grad_up, grad_down_t, grad_w_out]), "dp", scatter_dimension=1, tiled=True
    )

    summary_grad = scatter_sum(summary_grad, group_size).astype(jnp.bfloat16)

    grad_values = jnp.einsum(
        "hcj,hcd->jhd",
        probs_again.astype(jnp.bfloat16),
        summary_grad,
        preferred_element_type=jnp.float32,
    )
    half_width = local_heads * head_dim
    values_out = grad_values.astype(jnp.bfloat16).reshape(group_size, tok_rows, half_width)

    values_in = lax.all_to_all(values_out, "mp", split_axis=0, concat_axis=0, tiled=True)

    grad_probs = jnp.einsum(
        "hcd,jhd->hcj", summary_grad, value_rows, preferred_element_type=jnp.float32
    )
    grad_scores = probs_again * (
        grad_probs - jnp.sum(probs_again * grad_probs, axis=-1, keepdims=True)
    )
    grad_scores = grad_scores.astype(jnp.bfloat16)
    grad_centroids = (
        score_scale
        * jnp.einsum("hcj,jhd->hcd", grad_scores, key_rows, preferred_element_type=jnp.float32)
    ).astype(jnp.bfloat16)
    grad_keys = score_scale * jnp.einsum(
        "hcj,hcd->jhd", grad_scores, centroids, preferred_element_type=jnp.float32
    )
    per_member = (grad_centroids.astype(jnp.float32) / divisor[:, :, None]).astype(
        jnp.bfloat16
    )
    member_rows = per_member.size // half_width
    outgoing = jnp.concatenate(
        [
            grad_keys.astype(jnp.bfloat16).reshape(group_size, tok_rows, half_width),
            jnp.broadcast_to(
                per_member.reshape(1, member_rows, half_width),
                (group_size, member_rows, half_width),
            ),
        ],
        axis=1,
    )

    incoming = lax.all_to_all(outgoing, "mp", split_axis=0, concat_axis=0, tiled=True)

    out_pieces, _ = lax.optimization_barrier((out_partial.astype(jnp.bfloat16), incoming))
    result = scatter_sum(out_pieces, group_size)
    block_output = (residual + result).astype(jnp.bfloat16)

    keys_back = incoming[:, :tok_rows].transpose(1, 0, 2).reshape(tok_rows, model_width)
    values_back = values_in.transpose(1, 0, 2).reshape(tok_rows, model_width)
    grad_keyval = jnp.concatenate([keys_back, values_back], axis=1)
    all_member = (
        incoming[:, tok_rows:].reshape(head_count, CLUSTERS, head_dim).astype(jnp.float32)
    )
    grad_queries = jnp.einsum(
        "hct,hcd->thd", member_float, all_member, precision=lax.Precision.HIGHEST
    )
    grad_queries = grad_queries.reshape(tok_rows, model_width).astype(jnp.bfloat16)
    grad_query_bias = jnp.sum(grad_queries.astype(jnp.float32), axis=0)
    grad_value_bias = jnp.sum(grad_keyval[:, model_width:].astype(jnp.float32), axis=0)
    grad_w_attn = jnp.einsum(
        "td,te->de",
        first,
        jnp.concatenate([grad_queries, grad_keyval], axis=1),
        preferred_element_type=jnp.float32,
    )
    grad_first = jnp.einsum("te,de->td", grad_queries, w_query, preferred_element_type=jnp.float32)
    grad_first = grad_first + jnp.einsum(
        "te,de->td", grad_keyval, w_keyval, preferred_element_type=jnp.float32
    )
    input_norm_grad, grad_gain_one, grad_shift_one = norm_backward(
        grad_first, standard_one, factor_one, ln1_gain
    )
    input_grad = grad_middle + input_norm_grad
    vectors = jnp.stack(
        [
            grad_gain_one,
            grad_shift_one,
            grad_query_bias,
            grad_value_bias,
            grad_out_bias,
            grad_gain_two,
            grad_shift_two,
            grad_down_bias,
        ],
        axis=1,
    )
    up_bias_cols = grad_up_bias.reshape(model_width, -1)
    small_grads = jnp.concatenate([vectors, up_bias_cols], axis=1)

    dp_reduced = lax.psum_scatter(grad_w_attn, "dp", scatter_dimension=0, tiled=True)
    dp_rows = dp_reduced.shape[0]
    small_sum = lax.dynamic_slice_in_dim(
        lax.psum(small_grads, "dp"), lax.axis_index("dp") * dp_rows, dp_rows, 0
    )
    reduced = scatter_sum(jnp.concatenate([dp_reduced, ff_grads[2], small_sum], axis=1), group_size)
    up_share = ff_grads[0]
    down_share = ff_grads[1].T
    col = 0
    pieces = []
    for width in (model_width, 2 * model_width, model_width):
        pieces.append(reduced[:, col : col + width])
        col += width
    vec = [reduced[:, col + i] for i in range(8)]
    col += 8
    up_bias_share = reduced[:, col:].reshape(-1)
    return (
        block_output,
        input_grad,
        vec[0],
        vec[1],
        pieces[0],
        vec[2],
        pieces[1],
        vec[3],
        pieces[2],
        vec[4],
        vec[5],
        vec[6],
        up_share,
        up_bias_share,
        down_share,
        vec[7],
    )


def solution(mesh):
    placed = (
        P(("dp", "mp"), None),
        P(("dp", "mp"), None),
        P(),
        P(),
        P(),
        P(),
        P(),
        P(),
        P(),
        P(),
        P(),
        P(),
        P(None, "mp"),
        P("mp"),
        P("mp", None),
        P(),
        P(("dp", "mp"), None),
    )
    return jax.shard_map(
        block_body,
        mesh=mesh,
        in_specs=placed,
        out_specs=(
            P(("dp", "mp"), None),
            P(("dp", "mp"), None),
            P(("dp", "mp")),
            P(("dp", "mp")),
            P(("dp", "mp"), None),
            P(("dp", "mp")),
            P(("dp", "mp"), None),
            P(("dp", "mp")),
            P(("dp", "mp"), None),
            P(("dp", "mp")),
            P(("dp", "mp")),
            P(("dp", "mp")),
            P("dp", "mp"),
            P(("dp", "mp")),
            P("mp", "dp"),
            P(("dp", "mp")),
        ),
        check_vma=False,
    )
```

```python
import math

import jax
import jax.numpy as jnp
from jax import lax
from jax.sharding import PartitionSpec as P


CLUSTERS = 100


epsilon = 1e-05


def norm_forward(inputs, gain_vec, offset):
    center = inputs - jnp.mean(inputs, axis=-1, keepdims=True)
    factor = lax.rsqrt(jnp.mean(center * center, axis=-1, keepdims=True) + epsilon)
    standard = center * factor
    return (standard * gain_vec + offset, standard, factor)


def norm_backward(upstream, standard, factor, gain_vec):
    scaled = upstream * gain_vec
    centred = scaled - jnp.mean(scaled, axis=-1, keepdims=True)
    centred = centred - standard * jnp.mean(scaled * standard, axis=-1, keepdims=True)
    return (factor * centred, jnp.sum(upstream * standard, axis=0), jnp.sum(upstream, axis=0))


def gelu_parts(before):
    cumulative = 0.5 * (1.0 + jax.scipy.special.erf(before / math.sqrt(2.0)))
    density = jnp.exp(-0.5 * before * before) / math.sqrt(2.0 * math.pi)
    return (before * cumulative, cumulative + before * density)


def scatter_sum(partial, group_size):
    pieces = partial.reshape((group_size, -1) + partial.shape[1:])
    arrived = lax.all_to_all(pieces, "mp", split_axis=0, concat_axis=0, tiled=True)
    return jnp.sum(arrived.astype(jnp.float32), axis=0)


def broadcast_gather(local, group_size):
    sent = jnp.broadcast_to(local[None], (group_size,) + local.shape)
    arrived = lax.all_to_all(sent, "mp", split_axis=0, concat_axis=0, tiled=True)
    return arrived.reshape((group_size * local.shape[0],) + local.shape[1:])


def block_body(
    block_input,
    clusters,
    ln1_gain,
    ln1_bias,
    w_query,
    query_bias,
    w_keyval,
    value_bias,
    w_out,
    out_bias,
    ln2_gain,
    ln2_bias,
    w_up,
    up_bias,
    w_down,
    down_bias,
    cotangent,
):
    group_size = lax.axis_size("mp")
    tok_rows = block_input.shape[0]
    model_width = block_input.shape[1]
    head_count = clusters.shape[1]
    head_dim = model_width // head_count
    local_heads = head_count // group_size
    score_scale = float(head_dim) ** (-0.5)

    split = model_width // 2
    grad_rows = jnp.concatenate(
        [
            lax.all_gather(cotangent[:, :split], "mp", axis=0, tiled=True),
            lax.all_gather(cotangent[:, split:], "mp", axis=0, tiled=True),
        ],
        axis=1,
    )

    inputs = block_input.astype(jnp.float32)
    normed_one, standard_one, factor_one = norm_forward(inputs, ln1_gain, ln1_bias)
    first = normed_one.astype(jnp.bfloat16)
    queries = (
        jnp.dot(first, w_query, preferred_element_type=jnp.float32) + query_bias
    ).astype(jnp.bfloat16)
    keyval = jnp.dot(first, w_keyval, preferred_element_type=jnp.float32)
    keyval = (keyval + jnp.concatenate([jnp.zeros_like(value_bias), value_bias])).astype(
        jnp.bfloat16
    )
    member_float = (
        clusters.T[:, None, :] == jnp.arange(CLUSTERS, dtype=jnp.int32)[None, :, None]
    ).astype(jnp.float32)
    membership = member_float.astype(jnp.bfloat16)
    query_sums = jnp.einsum(
        "hct,thd->hcd",
        membership,
        queries.reshape(tok_rows, head_count, head_dim),
        preferred_element_type=jnp.float32,
    )
    cluster_sizes = jnp.sum(member_float, axis=2)
    packed = keyval.reshape(tok_rows, 2, group_size, local_heads * head_dim)

    arrived = lax.all_to_all(packed, "mp", split_axis=2, concat_axis=0, tiled=True)
    sums_and_sizes = scatter_sum(
        jnp.concatenate([query_sums, cluster_sizes[:, :, None]], axis=2), group_size
    )

    query_sums = sums_and_sizes[:, :, :head_dim]
    cluster_sizes = sums_and_sizes[:, :, head_dim]
    divisor = jnp.maximum(cluster_sizes, 1.0)
    centroids = (query_sums / divisor[:, :, None]).astype(jnp.bfloat16)
    length = arrived.shape[0]
    key_rows = arrived[:, 0, 0].reshape(length, local_heads, head_dim)
    value_rows = arrived[:, 1, 0].reshape(length, local_heads, head_dim)
    scores = score_scale * jnp.einsum(
        "hcd,jhd->hcj", centroids, key_rows, preferred_element_type=jnp.float32
    )
    score_peak = jnp.max(scores, axis=-1, keepdims=True)
    exponent = jnp.exp(scores - score_peak)
    denominator = jnp.sum(exponent, axis=-1, keepdims=True)
    probs = exponent / denominator
    logsum = score_peak + jnp.log(denominator)
    summary = jnp.einsum(
        "hcj,jhd->hcd",
        probs.astype(jnp.bfloat16),
        value_rows,
        preferred_element_type=jnp.float32,
    ).astype(jnp.bfloat16)

    everyone = broadcast_gather(summary, group_size)

    spread = (
        jnp.einsum("hct,hcd->thd", membership, everyone, preferred_element_type=jnp.float32)
        .astype(jnp.bfloat16)
        .reshape(tok_rows, model_width)
    )
    attended = jnp.dot(spread, w_out, preferred_element_type=jnp.float32) + out_bias
    middle = inputs + attended
    normed_two, standard_two, factor_two = norm_forward(middle, ln2_gain, ln2_bias)
    second = normed_two.astype(jnp.bfloat16)
    residual = lax.optimization_barrier(middle + down_bias)

    gathered = lax.all_gather(second, "mp", axis=0, tiled=True)

    before = jnp.dot(gathered, w_up, preferred_element_type=jnp.float32) + up_bias.astype(
        jnp.float32
    )
    activated, gelu_slope = gelu_parts(before)
    hidden = activated.astype(jnp.bfloat16)
    grad_hidden = jnp.einsum("td,fd->tf", grad_rows, w_down, preferred_element_type=jnp.float32)
    grad_before = (grad_hidden * gelu_slope).astype(jnp.bfloat16)
    grad_second = lax.psum_scatter(
        jnp.einsum("tf,df->td", grad_before, w_up, preferred_element_type=jnp.float32).astype(
            jnp.bfloat16
        ),
        "mp",
        scatter_dimension=0,
        tiled=True,
    ).astype(jnp.float32)

    out_partial = jnp.dot(hidden, w_down, preferred_element_type=jnp.float32)

    upstream = cotangent.astype(jnp.float32)
    grad_down_bias = jnp.sum(upstream, axis=0)
    grad_down_t = jnp.einsum("td,tf->df", grad_rows, hidden, preferred_element_type=jnp.float32)
    bias_part = jnp.sum(grad_before.astype(jnp.float32), axis=0)
    grad_up = jnp.einsum("td,tf->df", gathered, grad_before, preferred_element_type=jnp.float32)
    grad_up_bias = lax.dynamic_update_slice(
        jnp.zeros((group_size * bias_part.shape[0],), jnp.float32),
        bias_part,
        (lax.axis_index("mp") * bias_part.shape[0],),
    )

    scores_again = score_scale * jnp.einsum(
        "hcd,jhd->hcj", centroids, key_rows, preferred_element_type=jnp.float32
    )
    probs_again = jnp.exp(scores_again - logsum)

    middle_norm_grad, grad_gain_two, grad_shift_two = norm_backward(
        grad_second, standard_two, factor_two, ln2_gain
    )
    grad_middle = upstream + middle_norm_grad
    attn_grad = grad_middle.astype(jnp.bfloat16)
    grad_out_bias = jnp.sum(attn_grad.astype(jnp.float32), axis=0)
    grad_w_out = jnp.einsum("td,te->de", spread, attn_grad, preferred_element_type=jnp.float32)
    grad_spread = jnp.einsum(
        "te,de->td", attn_grad, w_out, preferred_element_type=jnp.float32
    ).astype(jnp.bfloat16)
    summary_grad = jnp.einsum(
        "hct,thd->hcd",
        membership,
        grad_spread.reshape(tok_rows, head_count, head_dim),
        preferred_element_type=jnp.float32,
    )

    ff_grads = lax.psum_scatter(
        jnp.stack([grad_up, grad_down_t, grad_w_out]), "dp", scatter_dimension=1, tiled=True
    )

    summary_grad = scatter_sum(summary_grad, group_size).astype(jnp.bfloat16)

    grad_values = jnp.einsum(
        "hcj,hcd->jhd",
        probs_again.astype(jnp.bfloat16),
        summary_grad,
        preferred_element_type=jnp.float32,
    )
    half_width = local_heads * head_dim
    values_out = grad_values.astype(jnp.bfloat16).reshape(group_size, tok_rows, half_width)

    values_in = lax.all_to_all(values_out, "mp", split_axis=0, concat_axis=0, tiled=True)

    grad_probs = jnp.einsum(
        "hcd,jhd->hcj", summary_grad, value_rows, preferred_element_type=jnp.float32
    )
    grad_scores = probs_again * (
        grad_probs - jnp.sum(probs_again * grad_probs, axis=-1, keepdims=True)
    )
    grad_scores = grad_scores.astype(jnp.bfloat16)
    grad_centroids = (
        score_scale
        * jnp.einsum("hcj,jhd->hcd", grad_scores, key_rows, preferred_element_type=jnp.float32)
    ).astype(jnp.bfloat16)
    grad_keys = score_scale * jnp.einsum(
        "hcj,hcd->jhd", grad_scores, centroids, preferred_element_type=jnp.float32
    )
    per_member = (grad_centroids.astype(jnp.float32) / divisor[:, :, None]).astype(
        jnp.bfloat16
    )
    member_rows = per_member.size // half_width
    outgoing = jnp.concatenate(
        [
            grad_keys.astype(jnp.bfloat16).reshape(group_size, tok_rows, half_width),
            jnp.broadcast_to(
                per_member.reshape(1, member_rows, half_width),
                (group_size, member_rows, half_width),
            ),
        ],
        axis=1,
    )

    incoming = lax.all_to_all(outgoing, "mp", split_axis=0, concat_axis=0, tiled=True)

    out_pieces, _ = lax.optimization_barrier((out_partial.astype(jnp.bfloat16), incoming))
    result = scatter_sum(out_pieces, group_size)
    block_output = (residual + result).astype(jnp.bfloat16)

    keys_back = incoming[:, :tok_rows].transpose(1, 0, 2).reshape(tok_rows, model_width)
    values_back = values_in.transpose(1, 0, 2).reshape(tok_rows, model_width)
    grad_keyval = jnp.concatenate([keys_back, values_back], axis=1)
    all_member = (
        incoming[:, tok_rows:].reshape(head_count, CLUSTERS, head_dim).astype(jnp.float32)
    )
    grad_queries = jnp.einsum(
        "hct,hcd->thd", member_float, all_member, precision=lax.Precision.HIGHEST
    )
    grad_queries = grad_queries.reshape(tok_rows, model_width).astype(jnp.bfloat16)
    grad_query_bias = jnp.sum(grad_queries.astype(jnp.float32), axis=0)
    grad_value_bias = jnp.sum(grad_keyval[:, model_width:].astype(jnp.float32), axis=0)
    grad_w_attn = jnp.einsum(
        "td,te->de",
        first,
        jnp.concatenate([grad_queries, grad_keyval], axis=1),
        preferred_element_type=jnp.float32,
    )
    grad_first = jnp.einsum("te,de->td", grad_queries, w_query, preferred_element_type=jnp.float32)
    grad_first = grad_first + jnp.einsum(
        "te,de->td", grad_keyval, w_keyval, preferred_element_type=jnp.float32
    )
    input_norm_grad, grad_gain_one, grad_shift_one = norm_backward(
        grad_first, standard_one, factor_one, ln1_gain
    )
    input_grad = grad_middle + input_norm_grad
    vectors = jnp.stack(
        [
            grad_gain_one,
            grad_shift_one,
            grad_query_bias,
            grad_value_bias,
            grad_out_bias,
            grad_gain_two,
            grad_shift_two,
            grad_down_bias,
        ],
        axis=1,
    )
    up_bias_cols = grad_up_bias.reshape(model_width, -1)
    small_grads = jnp.concatenate([vectors, up_bias_cols], axis=1)

    dp_reduced = lax.psum_scatter(grad_w_attn, "dp", scatter_dimension=0, tiled=True)
    dp_rows = dp_reduced.shape[0]
    small_sum = lax.dynamic_slice_in_dim(
        lax.psum(small_grads, "dp"), lax.axis_index("dp") * dp_rows, dp_rows, 0
    )
    reduced = scatter_sum(jnp.concatenate([dp_reduced, ff_grads[2], small_sum], axis=1), group_size)
    up_share = ff_grads[0]
    down_share = ff_grads[1].T
    col = 0
    pieces = []
    for width in (model_width, 2 * model_width, model_width):
        pieces.append(reduced[:, col : col + width])
        col += width
    vec = [reduced[:, col + i] for i in range(8)]
    col += 8
    up_bias_share = reduced[:, col:].reshape(-1)
    return (
        block_output,
        input_grad,
        vec[0],
        vec[1],
        pieces[0],
        vec[2],
        pieces[1],
        vec[3],
        pieces[2],
        vec[4],
        vec[5],
        vec[6],
        up_share,
        up_bias_share,
        down_share,
        vec[7],
    )


def solution(mesh):
    placed = (
        P(("dp", "mp"), None),
        P(("dp", "mp"), None),
        P(),
        P(),
        P(),
        P(),
        P(),
        P(),
        P(),
        P(),
        P(),
        P(),
        P(None, "mp"),
        P("mp"),
        P("mp", None),
        P(),
        P(("dp", "mp"), None),
    )
    return jax.shard_map(
        block_body,
        mesh=mesh,
        in_specs=placed,
        out_specs=(
            P(("dp", "mp"), None),
            P(("dp", "mp"), None),
            P(("dp", "mp")),
            P(("dp", "mp")),
            P(("dp", "mp"), None),
            P(("dp", "mp")),
            P(("dp", "mp"), None),
            P(("dp", "mp")),
            P(("dp", "mp"), None),
            P(("dp", "mp")),
            P(("dp", "mp")),
            P(("dp", "mp")),
            P("dp", "mp"),
            P(("dp", "mp")),
            P("mp", "dp"),
            P(("dp", "mp")),
        ),
        check_vma=False,
    )
```

```python
import math

import jax
import jax.numpy as jnp
from jax import lax
from jax.sharding import PartitionSpec as P


CLUSTERS = 100


epsilon = 1e-05


def norm_forward(inputs, gain_vec, offset):
    center = inputs - jnp.mean(inputs, axis=-1, keepdims=True)
    factor = lax.rsqrt(jnp.mean(center * center, axis=-1, keepdims=True) + epsilon)
    standard = center * factor
    return (standard * gain_vec + offset, standard, factor)


def norm_backward(upstream, standard, factor, gain_vec):
    scaled = upstream * gain_vec
    centred = scaled - jnp.mean(scaled, axis=-1, keepdims=True)
    centred = centred - standard * jnp.mean(scaled * standard, axis=-1, keepdims=True)
    return (factor * centred, jnp.sum(upstream * standard, axis=0), jnp.sum(upstream, axis=0))


def gelu_parts(before):
    cumulative = 0.5 * (1.0 + jax.scipy.special.erf(before / math.sqrt(2.0)))
    density = jnp.exp(-0.5 * before * before) / math.sqrt(2.0 * math.pi)
    return (before * cumulative, cumulative + before * density)


def scatter_sum(partial, group_size):
    pieces = partial.reshape((group_size, -1) + partial.shape[1:])
    arrived = lax.all_to_all(pieces, "mp", split_axis=0, concat_axis=0, tiled=True)
    return jnp.sum(arrived.astype(jnp.float32), axis=0)


def shift_sum(partial, group_size):
    me = lax.axis_index("mp")
    pieces = partial.reshape((group_size, -1) + partial.shape[1:])
    total = lax.dynamic_index_in_dim(pieces, me, 0, keepdims=False).astype(jnp.float32)
    for step in range(1, group_size):
        sent = lax.dynamic_index_in_dim(
            pieces, jnp.remainder(me + step, group_size), 0, keepdims=False
        )
        moved = lax.ppermute(
            sent, "mp", [(i, (i + step) % group_size) for i in range(group_size)]
        )
        total = total + moved.astype(jnp.float32)
    return total


def broadcast_gather(local, group_size):
    sent = jnp.broadcast_to(local[None], (group_size,) + local.shape)
    arrived = lax.all_to_all(sent, "mp", split_axis=0, concat_axis=0, tiled=True)
    return arrived.reshape((group_size * local.shape[0],) + local.shape[1:])


def block_body(
    block_input,
    clusters,
    ln1_gain,
    ln1_bias,
    w_query,
    query_bias,
    w_keyval,
    value_bias,
    w_out,
    out_bias,
    ln2_gain,
    ln2_bias,
    w_up,
    up_bias,
    w_down,
    down_bias,
    cotangent,
):
    group_size = lax.axis_size("mp")
    tok_rows = block_input.shape[0]
    model_width = block_input.shape[1]
    head_count = clusters.shape[1]
    head_dim = model_width // head_count
    local_heads = head_count // group_size
    score_scale = float(head_dim) ** (-0.5)

    split = model_width // 2
    grad_rows = jnp.concatenate(
        [
            lax.all_gather(cotangent[:, :split], "mp", axis=0, tiled=True),
            lax.all_gather(cotangent[:, split:], "mp", axis=0, tiled=True),
        ],
        axis=1,
    )

    inputs = block_input.astype(jnp.float32)
    normed_one, standard_one, factor_one = norm_forward(inputs, ln1_gain, ln1_bias)
    first = normed_one.astype(jnp.bfloat16)
    queries = (
        jnp.dot(first, w_query, preferred_element_type=jnp.float32) + query_bias
    ).astype(jnp.bfloat16)
    keyval = jnp.dot(first, w_keyval, preferred_element_type=jnp.float32)
    keyval = (keyval + jnp.concatenate([jnp.zeros_like(value_bias), value_bias])).astype(
        jnp.bfloat16
    )
    member_float = (
        clusters.T[:, None, :] == jnp.arange(CLUSTERS, dtype=jnp.int32)[None, :, None]
    ).astype(jnp.float32)
    membership = member_float.astype(jnp.bfloat16)
    query_sums = jnp.einsum(
        "hct,thd->hcd",
        membership,
        queries.reshape(tok_rows, head_count, head_dim),
        preferred_element_type=jnp.float32,
    )
    cluster_sizes = jnp.sum(member_float, axis=2)
    packed = keyval.reshape(tok_rows, 2, group_size, local_heads * head_dim)

    arrived = lax.all_to_all(packed, "mp", split_axis=2, concat_axis=0, tiled=True)
    sums_and_sizes = scatter_sum(
        jnp.concatenate([query_sums, cluster_sizes[:, :, None]], axis=2), group_size
    )

    query_sums = sums_and_sizes[:, :, :head_dim]
    cluster_sizes = sums_and_sizes[:, :, head_dim]
    divisor = jnp.maximum(cluster_sizes, 1.0)
    centroids = (query_sums / divisor[:, :, None]).astype(jnp.bfloat16)
    length = arrived.shape[0]
    key_rows = arrived[:, 0, 0].reshape(length, local_heads, head_dim)
    value_rows = arrived[:, 1, 0].reshape(length, local_heads, head_dim)
    scores = score_scale * jnp.einsum(
        "hcd,jhd->hcj", centroids, key_rows, preferred_element_type=jnp.float32
    )
    score_peak = jnp.max(scores, axis=-1, keepdims=True)
    exponent = jnp.exp(scores - score_peak)
    denominator = jnp.sum(exponent, axis=-1, keepdims=True)
    probs = exponent / denominator
    logsum = score_peak + jnp.log(denominator)
    summary = jnp.einsum(
        "hcj,jhd->hcd",
        probs.astype(jnp.bfloat16),
        value_rows,
        preferred_element_type=jnp.float32,
    ).astype(jnp.bfloat16)

    everyone = broadcast_gather(summary, group_size)

    spread = (
        jnp.einsum("hct,hcd->thd", membership, everyone, preferred_element_type=jnp.float32)
        .astype(jnp.bfloat16)
        .reshape(tok_rows, model_width)
    )
    attended = jnp.dot(spread, w_out, preferred_element_type=jnp.float32) + out_bias
    middle = inputs + attended
    normed_two, standard_two, factor_two = norm_forward(middle, ln2_gain, ln2_bias)
    second = normed_two.astype(jnp.bfloat16)
    residual = lax.optimization_barrier(middle + down_bias)

    gathered = lax.all_gather(second, "mp", axis=0, tiled=True)

    before = jnp.dot(gathered, w_up, preferred_element_type=jnp.float32) + up_bias.astype(
        jnp.float32
    )
    activated, gelu_slope = gelu_parts(before)
    hidden = activated.astype(jnp.bfloat16)
    grad_hidden = jnp.einsum("td,fd->tf", grad_rows, w_down, preferred_element_type=jnp.float32)
    grad_before = (grad_hidden * gelu_slope).astype(jnp.bfloat16)
    grad_second = lax.psum_scatter(
        jnp.einsum("tf,df->td", grad_before, w_up, preferred_element_type=jnp.float32).astype(
            jnp.bfloat16
        ),
        "mp",
        scatter_dimension=0,
        tiled=True,
    ).astype(jnp.float32)

    out_partial = jnp.dot(hidden, w_down, preferred_element_type=jnp.float32)

    upstream = cotangent.astype(jnp.float32)
    grad_down_bias = jnp.sum(upstream, axis=0)
    grad_down_t = jnp.einsum("td,tf->df", grad_rows, hidden, preferred_element_type=jnp.float32)
    bias_part = jnp.sum(grad_before.astype(jnp.float32), axis=0)
    grad_up = jnp.einsum("td,tf->df", gathered, grad_before, preferred_element_type=jnp.float32)
    grad_up_bias = lax.dynamic_update_slice(
        jnp.zeros((group_size * bias_part.shape[0],), jnp.float32),
        bias_part,
        (lax.axis_index("mp") * bias_part.shape[0],),
    )

    scores_again = score_scale * jnp.einsum(
        "hcd,jhd->hcj", centroids, key_rows, preferred_element_type=jnp.float32
    )
    probs_again = jnp.exp(scores_again - logsum)

    middle_norm_grad, grad_gain_two, grad_shift_two = norm_backward(
        grad_second, standard_two, factor_two, ln2_gain
    )
    grad_middle = upstream + middle_norm_grad
    attn_grad = grad_middle.astype(jnp.bfloat16)
    grad_out_bias = jnp.sum(attn_grad.astype(jnp.float32), axis=0)
    grad_w_out = jnp.einsum("td,te->de", spread, attn_grad, preferred_element_type=jnp.float32)
    grad_spread = jnp.einsum(
        "te,de->td", attn_grad, w_out, preferred_element_type=jnp.float32
    ).astype(jnp.bfloat16)
    summary_grad = jnp.einsum(
        "hct,thd->hcd",
        membership,
        grad_spread.reshape(tok_rows, head_count, head_dim),
        preferred_element_type=jnp.float32,
    )

    ff_grads = lax.psum_scatter(
        jnp.stack([grad_up, grad_down_t, grad_w_out]), "dp", scatter_dimension=1, tiled=True
    )

    summary_grad = scatter_sum(summary_grad, group_size).astype(jnp.bfloat16)

    grad_values = jnp.einsum(
        "hcj,hcd->jhd",
        probs_again.astype(jnp.bfloat16),
        summary_grad,
        preferred_element_type=jnp.float32,
    )
    half_width = local_heads * head_dim
    values_out = grad_values.astype(jnp.bfloat16).reshape(group_size, tok_rows, half_width)

    values_in = lax.all_to_all(values_out, "mp", split_axis=0, concat_axis=0, tiled=True)

    grad_probs = jnp.einsum(
        "hcd,jhd->hcj", summary_grad, value_rows, preferred_element_type=jnp.float32
    )
    grad_scores = probs_again * (
        grad_probs - jnp.sum(probs_again * grad_probs, axis=-1, keepdims=True)
    )
    grad_scores = grad_scores.astype(jnp.bfloat16)
    grad_centroids = (
        score_scale
        * jnp.einsum("hcj,jhd->hcd", grad_scores, key_rows, preferred_element_type=jnp.float32)
    ).astype(jnp.bfloat16)
    grad_keys = score_scale * jnp.einsum(
        "hcj,hcd->jhd", grad_scores, centroids, preferred_element_type=jnp.float32
    )
    per_member = (grad_centroids.astype(jnp.float32) / divisor[:, :, None]).astype(
        jnp.bfloat16
    )
    member_rows = per_member.size // half_width
    outgoing = jnp.concatenate(
        [
            grad_keys.astype(jnp.bfloat16).reshape(group_size, tok_rows, half_width),
            jnp.broadcast_to(
                per_member.reshape(1, member_rows, half_width),
                (group_size, member_rows, half_width),
            ),
        ],
        axis=1,
    )

    incoming = lax.all_to_all(outgoing, "mp", split_axis=0, concat_axis=0, tiled=True)

    out_pieces, _ = lax.optimization_barrier((out_partial.astype(jnp.bfloat16), incoming))
    result = shift_sum(out_pieces, group_size)
    block_output = (residual + result).astype(jnp.bfloat16)

    keys_back = incoming[:, :tok_rows].transpose(1, 0, 2).reshape(tok_rows, model_width)
    values_back = values_in.transpose(1, 0, 2).reshape(tok_rows, model_width)
    grad_keyval = jnp.concatenate([keys_back, values_back], axis=1)
    all_member = (
        incoming[:, tok_rows:].reshape(head_count, CLUSTERS, head_dim).astype(jnp.float32)
    )
    grad_queries = jnp.einsum(
        "hct,hcd->thd", member_float, all_member, precision=lax.Precision.HIGHEST
    )
    grad_queries = grad_queries.reshape(tok_rows, model_width).astype(jnp.bfloat16)
    grad_query_bias = jnp.sum(grad_queries.astype(jnp.float32), axis=0)
    grad_value_bias = jnp.sum(grad_keyval[:, model_width:].astype(jnp.float32), axis=0)
    grad_w_attn = jnp.einsum(
        "td,te->de",
        first,
        jnp.concatenate([grad_queries, grad_keyval], axis=1),
        preferred_element_type=jnp.float32,
    )
    grad_first = jnp.einsum("te,de->td", grad_queries, w_query, preferred_element_type=jnp.float32)
    grad_first = grad_first + jnp.einsum(
        "te,de->td", grad_keyval, w_keyval, preferred_element_type=jnp.float32
    )
    input_norm_grad, grad_gain_one, grad_shift_one = norm_backward(
        grad_first, standard_one, factor_one, ln1_gain
    )
    input_grad = grad_middle + input_norm_grad
    vectors = jnp.stack(
        [
            grad_gain_one,
            grad_shift_one,
            grad_query_bias,
            grad_value_bias,
            grad_out_bias,
            grad_gain_two,
            grad_shift_two,
            grad_down_bias,
        ],
        axis=1,
    )
    up_bias_cols = grad_up_bias.reshape(model_width, -1)
    small_grads = jnp.concatenate([vectors, up_bias_cols], axis=1)

    dp_reduced = lax.psum_scatter(grad_w_attn, "dp", scatter_dimension=0, tiled=True)
    dp_rows = dp_reduced.shape[0]
    small_sum = lax.dynamic_slice_in_dim(
        lax.psum(small_grads, "dp"), lax.axis_index("dp") * dp_rows, dp_rows, 0
    )
    reduced = shift_sum(jnp.concatenate([dp_reduced, ff_grads[2], small_sum], axis=1), group_size)
    up_share = ff_grads[0]
    down_share = ff_grads[1].T
    col = 0
    pieces = []
    for width in (model_width, 2 * model_width, model_width):
        pieces.append(reduced[:, col : col + width])
        col += width
    vec = [reduced[:, col + i] for i in range(8)]
    col += 8
    up_bias_share = reduced[:, col:].reshape(-1)
    return (
        block_output,
        input_grad,
        vec[0],
        vec[1],
        pieces[0],
        vec[2],
        pieces[1],
        vec[3],
        pieces[2],
        vec[4],
        vec[5],
        vec[6],
        up_share,
        up_bias_share,
        down_share,
        vec[7],
    )


def solution(mesh):
    placed = (
        P(("dp", "mp"), None),
        P(("dp", "mp"), None),
        P(),
        P(),
        P(),
        P(),
        P(),
        P(),
        P(),
        P(),
        P(),
        P(),
        P(None, "mp"),
        P("mp"),
        P("mp", None),
        P(),
        P(("dp", "mp"), None),
    )
    return jax.shard_map(
        block_body,
        mesh=mesh,
        in_specs=placed,
        out_specs=(
            P(("dp", "mp"), None),
            P(("dp", "mp"), None),
            P(("dp", "mp")),
            P(("dp", "mp")),
            P(("dp", "mp"), None),
            P(("dp", "mp")),
            P(("dp", "mp"), None),
            P(("dp", "mp")),
            P(("dp", "mp"), None),
            P(("dp", "mp")),
            P(("dp", "mp")),
            P(("dp", "mp")),
            P("dp", "mp"),
            P(("dp", "mp")),
            P("mp", "dp"),
            P(("dp", "mp")),
        ),
        check_vma=False,
    )
```

```python
import math

import jax
import jax.numpy as jnp
from jax import lax
from jax.sharding import PartitionSpec as P


CLUSTERS = 100


epsilon = 1e-05


def norm_forward(inputs, gain_vec, offset):
    center = inputs - jnp.mean(inputs, axis=-1, keepdims=True)
    factor = lax.rsqrt(jnp.mean(center * center, axis=-1, keepdims=True) + epsilon)
    standard = center * factor
    return (standard * gain_vec + offset, standard, factor)


def norm_backward(upstream, standard, factor, gain_vec):
    scaled = upstream * gain_vec
    centred = scaled - jnp.mean(scaled, axis=-1, keepdims=True)
    centred = centred - standard * jnp.mean(scaled * standard, axis=-1, keepdims=True)
    return (factor * centred, jnp.sum(upstream * standard, axis=0), jnp.sum(upstream, axis=0))


def gelu_parts(before):
    cumulative = 0.5 * (1.0 + jax.scipy.special.erf(before / math.sqrt(2.0)))
    density = jnp.exp(-0.5 * before * before) / math.sqrt(2.0 * math.pi)
    return (before * cumulative, cumulative + before * density)


def shift_sum(partial, group_size):
    me = lax.axis_index("mp")
    pieces = partial.reshape((group_size, -1) + partial.shape[1:])
    total = lax.dynamic_index_in_dim(pieces, me, 0, keepdims=False).astype(jnp.float32)
    for step in range(1, group_size):
        sent = lax.dynamic_index_in_dim(
            pieces, jnp.remainder(me + step, group_size), 0, keepdims=False
        )
        moved = lax.ppermute(
            sent, "mp", [(i, (i + step) % group_size) for i in range(group_size)]
        )
        total = total + moved.astype(jnp.float32)
    return total


def shift_exchange(pieces, group_size):
    me = lax.axis_index("mp")
    out = jnp.zeros_like(pieces)
    out = lax.dynamic_update_index_in_dim(
        out, lax.dynamic_index_in_dim(pieces, me, 0, keepdims=False), me, 0
    )
    for step in range(1, group_size):
        sent = lax.dynamic_index_in_dim(
            pieces, jnp.remainder(me + step, group_size), 0, keepdims=False
        )
        moved = lax.ppermute(
            sent, "mp", [(i, (i + step) % group_size) for i in range(group_size)]
        )
        out = lax.dynamic_update_index_in_dim(
            out, moved, jnp.remainder(me + group_size - step, group_size), 0
        )
    return out


def broadcast_gather(local, group_size):
    me = lax.axis_index("mp")
    out = jnp.zeros((group_size,) + local.shape, local.dtype)
    out = lax.dynamic_update_index_in_dim(out, local, me, 0)
    for step in range(1, group_size):
        moved = lax.ppermute(
            local, "mp", [(i, (i + step) % group_size) for i in range(group_size)]
        )
        out = lax.dynamic_update_index_in_dim(
            out, moved, jnp.remainder(me + group_size - step, group_size), 0
        )
    return out.reshape((group_size * local.shape[0],) + local.shape[1:])


def block_body(
    block_input,
    clusters,
    ln1_gain,
    ln1_bias,
    w_query,
    query_bias,
    w_keyval,
    value_bias,
    w_out,
    out_bias,
    ln2_gain,
    ln2_bias,
    w_up,
    up_bias,
    w_down,
    down_bias,
    cotangent,
):
    group_size = lax.axis_size("mp")
    tok_rows = block_input.shape[0]
    model_width = block_input.shape[1]
    head_count = clusters.shape[1]
    head_dim = model_width // head_count
    local_heads = head_count // group_size
    score_scale = float(head_dim) ** (-0.5)

    split = model_width // 2
    grad_rows = jnp.concatenate(
        [
            lax.all_gather(cotangent[:, :split], "mp", axis=0, tiled=True),
            lax.all_gather(cotangent[:, split:], "mp", axis=0, tiled=True),
        ],
        axis=1,
    )

    inputs = block_input.astype(jnp.float32)
    normed_one, standard_one, factor_one = norm_forward(inputs, ln1_gain, ln1_bias)
    first = normed_one.astype(jnp.bfloat16)
    queries = (
        jnp.dot(first, w_query, preferred_element_type=jnp.float32) + query_bias
    ).astype(jnp.bfloat16)
    keyval = jnp.dot(first, w_keyval, preferred_element_type=jnp.float32)
    keyval = (keyval + jnp.concatenate([jnp.zeros_like(value_bias), value_bias])).astype(
        jnp.bfloat16
    )
    member_float = (
        clusters.T[:, None, :] == jnp.arange(CLUSTERS, dtype=jnp.int32)[None, :, None]
    ).astype(jnp.float32)
    membership = member_float.astype(jnp.bfloat16)
    query_sums = jnp.einsum(
        "hct,thd->hcd",
        membership,
        queries.reshape(tok_rows, head_count, head_dim),
        preferred_element_type=jnp.float32,
    )
    cluster_sizes = jnp.sum(member_float, axis=2)
    packed = keyval.reshape(tok_rows, 2, group_size, local_heads * head_dim)

    arrived = (
        shift_exchange(packed.transpose(2, 0, 1, 3), group_size)
        .reshape(group_size * tok_rows, 2, 1, local_heads * head_dim)
    )
    sums_and_sizes = shift_sum(
        jnp.concatenate([query_sums, cluster_sizes[:, :, None]], axis=2), group_size
    )

    query_sums = sums_and_sizes[:, :, :head_dim]
    cluster_sizes = sums_and_sizes[:, :, head_dim]
    divisor = jnp.maximum(cluster_sizes, 1.0)
    centroids = (query_sums / divisor[:, :, None]).astype(jnp.bfloat16)
    length = arrived.shape[0]
    key_rows = arrived[:, 0, 0].reshape(length, local_heads, head_dim)
    value_rows = arrived[:, 1, 0].reshape(length, local_heads, head_dim)
    scores = score_scale * jnp.einsum(
        "hcd,jhd->hcj", centroids, key_rows, preferred_element_type=jnp.float32
    )
    score_peak = jnp.max(scores, axis=-1, keepdims=True)
    exponent = jnp.exp(scores - score_peak)
    denominator = jnp.sum(exponent, axis=-1, keepdims=True)
    probs = exponent / denominator
    logsum = score_peak + jnp.log(denominator)
    summary = jnp.einsum(
        "hcj,jhd->hcd",
        probs.astype(jnp.bfloat16),
        value_rows,
        preferred_element_type=jnp.float32,
    ).astype(jnp.bfloat16)

    everyone = broadcast_gather(summary, group_size)

    spread = (
        jnp.einsum("hct,hcd->thd", membership, everyone, preferred_element_type=jnp.float32)
        .astype(jnp.bfloat16)
        .reshape(tok_rows, model_width)
    )
    attended = jnp.dot(spread, w_out, preferred_element_type=jnp.float32) + out_bias
    middle = inputs + attended
    normed_two, standard_two, factor_two = norm_forward(middle, ln2_gain, ln2_bias)
    second = normed_two.astype(jnp.bfloat16)
    residual = lax.optimization_barrier(middle + down_bias)

    gathered = lax.all_gather(second, "mp", axis=0, tiled=True)

    before = jnp.dot(gathered, w_up, preferred_element_type=jnp.float32) + up_bias.astype(
        jnp.float32
    )
    activated, gelu_slope = gelu_parts(before)
    hidden = activated.astype(jnp.bfloat16)
    grad_hidden = jnp.einsum("td,fd->tf", grad_rows, w_down, preferred_element_type=jnp.float32)
    grad_before = (grad_hidden * gelu_slope).astype(jnp.bfloat16)
    grad_second = lax.psum_scatter(
        jnp.einsum("tf,df->td", grad_before, w_up, preferred_element_type=jnp.float32).astype(
            jnp.bfloat16
        ),
        "mp",
        scatter_dimension=0,
        tiled=True,
    ).astype(jnp.float32)

    out_partial = jnp.dot(hidden, w_down, preferred_element_type=jnp.float32)

    upstream = cotangent.astype(jnp.float32)
    grad_down_bias = jnp.sum(upstream, axis=0)
    grad_down_t = jnp.einsum("td,tf->df", grad_rows, hidden, preferred_element_type=jnp.float32)
    bias_part = jnp.sum(grad_before.astype(jnp.float32), axis=0)
    grad_up = jnp.einsum("td,tf->df", gathered, grad_before, preferred_element_type=jnp.float32)
    grad_up_bias = lax.dynamic_update_slice(
        jnp.zeros((group_size * bias_part.shape[0],), jnp.float32),
        bias_part,
        (lax.axis_index("mp") * bias_part.shape[0],),
    )

    scores_again = score_scale * jnp.einsum(
        "hcd,jhd->hcj", centroids, key_rows, preferred_element_type=jnp.float32
    )
    probs_again = jnp.exp(scores_again - logsum)

    middle_norm_grad, grad_gain_two, grad_shift_two = norm_backward(
        grad_second, standard_two, factor_two, ln2_gain
    )
    grad_middle = upstream + middle_norm_grad
    attn_grad = grad_middle.astype(jnp.bfloat16)
    grad_out_bias = jnp.sum(attn_grad.astype(jnp.float32), axis=0)
    grad_w_out = jnp.einsum("td,te->de", spread, attn_grad, preferred_element_type=jnp.float32)
    grad_spread = jnp.einsum(
        "te,de->td", attn_grad, w_out, preferred_element_type=jnp.float32
    ).astype(jnp.bfloat16)
    summary_grad = jnp.einsum(
        "hct,thd->hcd",
        membership,
        grad_spread.reshape(tok_rows, head_count, head_dim),
        preferred_element_type=jnp.float32,
    )

    ff_grads = lax.psum_scatter(
        jnp.stack([grad_up, grad_down_t, grad_w_out]), "dp", scatter_dimension=1, tiled=True
    )

    summary_grad = shift_sum(summary_grad, group_size).astype(jnp.bfloat16)

    grad_values = jnp.einsum(
        "hcj,hcd->jhd",
        probs_again.astype(jnp.bfloat16),
        summary_grad,
        preferred_element_type=jnp.float32,
    )
    half_width = local_heads * head_dim
    values_out = grad_values.astype(jnp.bfloat16).reshape(group_size, tok_rows, half_width)

    values_in = shift_exchange(values_out, group_size)

    grad_probs = jnp.einsum(
        "hcd,jhd->hcj", summary_grad, value_rows, preferred_element_type=jnp.float32
    )
    grad_scores = probs_again * (
        grad_probs - jnp.sum(probs_again * grad_probs, axis=-1, keepdims=True)
    )
    grad_scores = grad_scores.astype(jnp.bfloat16)
    grad_centroids = (
        score_scale
        * jnp.einsum("hcj,jhd->hcd", grad_scores, key_rows, preferred_element_type=jnp.float32)
    ).astype(jnp.bfloat16)
    grad_keys = score_scale * jnp.einsum(
        "hcj,hcd->jhd", grad_scores, centroids, preferred_element_type=jnp.float32
    )
    per_member = (grad_centroids.astype(jnp.float32) / divisor[:, :, None]).astype(
        jnp.bfloat16
    )
    member_rows = per_member.size // half_width
    outgoing = jnp.concatenate(
        [
            grad_keys.astype(jnp.bfloat16).reshape(group_size, tok_rows, half_width),
            jnp.broadcast_to(
                per_member.reshape(1, member_rows, half_width),
                (group_size, member_rows, half_width),
            ),
        ],
        axis=1,
    )

    incoming = shift_exchange(outgoing, group_size)

    out_pieces, _ = lax.optimization_barrier((out_partial.astype(jnp.bfloat16), incoming))
    result = shift_sum(out_pieces, group_size)
    block_output = (residual + result).astype(jnp.bfloat16)

    keys_back = incoming[:, :tok_rows].transpose(1, 0, 2).reshape(tok_rows, model_width)
    values_back = values_in.transpose(1, 0, 2).reshape(tok_rows, model_width)
    grad_keyval = jnp.concatenate([keys_back, values_back], axis=1)
    all_member = (
        incoming[:, tok_rows:].reshape(head_count, CLUSTERS, head_dim).astype(jnp.float32)
    )
    grad_queries = jnp.einsum(
        "hct,hcd->thd", member_float, all_member, precision=lax.Precision.HIGHEST
    )
    grad_queries = grad_queries.reshape(tok_rows, model_width).astype(jnp.bfloat16)
    grad_query_bias = jnp.sum(grad_queries.astype(jnp.float32), axis=0)
    grad_value_bias = jnp.sum(grad_keyval[:, model_width:].astype(jnp.float32), axis=0)
    grad_w_attn = jnp.einsum(
        "td,te->de",
        first,
        jnp.concatenate([grad_queries, grad_keyval], axis=1),
        preferred_element_type=jnp.float32,
    )
    grad_first = jnp.einsum("te,de->td", grad_queries, w_query, preferred_element_type=jnp.float32)
    grad_first = grad_first + jnp.einsum(
        "te,de->td", grad_keyval, w_keyval, preferred_element_type=jnp.float32
    )
    input_norm_grad, grad_gain_one, grad_shift_one = norm_backward(
        grad_first, standard_one, factor_one, ln1_gain
    )
    input_grad = grad_middle + input_norm_grad
    vectors = jnp.stack(
        [
            grad_gain_one,
            grad_shift_one,
            grad_query_bias,
            grad_value_bias,
            grad_out_bias,
            grad_gain_two,
            grad_shift_two,
            grad_down_bias,
        ],
        axis=1,
    )
    up_bias_cols = grad_up_bias.reshape(model_width, -1)
    small_grads = jnp.concatenate([vectors, up_bias_cols], axis=1)

    dp_reduced = lax.psum_scatter(grad_w_attn, "dp", scatter_dimension=0, tiled=True)
    dp_rows = dp_reduced.shape[0]
    small_sum = lax.dynamic_slice_in_dim(
        lax.psum(small_grads, "dp"), lax.axis_index("dp") * dp_rows, dp_rows, 0
    )
    reduced = shift_sum(jnp.concatenate([dp_reduced, ff_grads[2], small_sum], axis=1), group_size)
    up_share = ff_grads[0]
    down_share = ff_grads[1].T
    col = 0
    pieces = []
    for width in (model_width, 2 * model_width, model_width):
        pieces.append(reduced[:, col : col + width])
        col += width
    vec = [reduced[:, col + i] for i in range(8)]
    col += 8
    up_bias_share = reduced[:, col:].reshape(-1)
    return (
        block_output,
        input_grad,
        vec[0],
        vec[1],
        pieces[0],
        vec[2],
        pieces[1],
        vec[3],
        pieces[2],
        vec[4],
        vec[5],
        vec[6],
        up_share,
        up_bias_share,
        down_share,
        vec[7],
    )


def solution(mesh):
    placed = (
        P(("dp", "mp"), None),
        P(("dp", "mp"), None),
        P(),
        P(),
        P(),
        P(),
        P(),
        P(),
        P(),
        P(),
        P(),
        P(),
        P(None, "mp"),
        P("mp"),
        P("mp", None),
        P(),
        P(("dp", "mp"), None),
    )
    return jax.shard_map(
        block_body,
        mesh=mesh,
        in_specs=placed,
        out_specs=(
            P(("dp", "mp"), None),
            P(("dp", "mp"), None),
            P(("dp", "mp")),
            P(("dp", "mp")),
            P(("dp", "mp"), None),
            P(("dp", "mp")),
            P(("dp", "mp"), None),
            P(("dp", "mp")),
            P(("dp", "mp"), None),
            P(("dp", "mp")),
            P(("dp", "mp")),
            P(("dp", "mp")),
            P("dp", "mp"),
            P(("dp", "mp")),
            P("mp", "dp"),
            P(("dp", "mp")),
        ),
        check_vma=False,
    )
```

```python
import math

import jax
import jax.numpy as jnp
from jax import lax
from jax.sharding import PartitionSpec as P


CLUSTERS = 100


epsilon = 1e-05


def norm_forward(inputs, gain_vec, offset):
    center = inputs - jnp.mean(inputs, axis=-1, keepdims=True)
    factor = lax.rsqrt(jnp.mean(center * center, axis=-1, keepdims=True) + epsilon)
    standard = center * factor
    return (standard * gain_vec + offset, standard, factor)


def norm_backward(upstream, standard, factor, gain_vec):
    scaled = upstream * gain_vec
    centred = scaled - jnp.mean(scaled, axis=-1, keepdims=True)
    centred = centred - standard * jnp.mean(scaled * standard, axis=-1, keepdims=True)
    return (factor * centred, jnp.sum(upstream * standard, axis=0), jnp.sum(upstream, axis=0))


def gelu_parts(before):
    cumulative = 0.5 * (1.0 + jax.scipy.special.erf(before / math.sqrt(2.0)))
    density = jnp.exp(-0.5 * before * before) / math.sqrt(2.0 * math.pi)
    return (before * cumulative, cumulative + before * density)


def scatter_sum(partial, group_size):
    pieces = partial.reshape((group_size, -1) + partial.shape[1:])
    arrived = lax.all_to_all(pieces, "mp", split_axis=0, concat_axis=0, tiled=True)
    return jnp.sum(arrived.astype(jnp.float32), axis=0)


def shift_sum(partial, group_size):
    me = lax.axis_index("mp")
    pieces = partial.reshape((group_size, -1) + partial.shape[1:])
    total = lax.dynamic_index_in_dim(pieces, me, 0, keepdims=False).astype(jnp.float32)
    for step in range(1, group_size):
        sent = lax.dynamic_index_in_dim(
            pieces, jnp.remainder(me + step, group_size), 0, keepdims=False
        )
        moved = lax.ppermute(
            sent, "mp", [(i, (i + step) % group_size) for i in range(group_size)]
        )
        total = total + moved.astype(jnp.float32)
    return total


def shift_exchange(pieces, group_size):
    me = lax.axis_index("mp")
    out = jnp.zeros_like(pieces)
    out = lax.dynamic_update_index_in_dim(
        out, lax.dynamic_index_in_dim(pieces, me, 0, keepdims=False), me, 0
    )
    for step in range(1, group_size):
        sent = lax.dynamic_index_in_dim(
            pieces, jnp.remainder(me + step, group_size), 0, keepdims=False
        )
        moved = lax.ppermute(
            sent, "mp", [(i, (i + step) % group_size) for i in range(group_size)]
        )
        out = lax.dynamic_update_index_in_dim(
            out, moved, jnp.remainder(me + group_size - step, group_size), 0
        )
    return out


def broadcast_gather(local, group_size):
    sent = jnp.broadcast_to(local[None], (group_size,) + local.shape)
    arrived = lax.all_to_all(sent, "mp", split_axis=0, concat_axis=0, tiled=True)
    return arrived.reshape((group_size * local.shape[0],) + local.shape[1:])


def block_body(
    block_input,
    clusters,
    ln1_gain,
    ln1_bias,
    w_query,
    query_bias,
    w_keyval,
    value_bias,
    w_out,
    out_bias,
    ln2_gain,
    ln2_bias,
    w_up,
    up_bias,
    w_down,
    down_bias,
    cotangent,
):
    group_size = lax.axis_size("mp")
    tok_rows = block_input.shape[0]
    model_width = block_input.shape[1]
    head_count = clusters.shape[1]
    head_dim = model_width // head_count
    local_heads = head_count // group_size
    score_scale = float(head_dim) ** (-0.5)

    split = model_width // 2
    grad_rows = jnp.concatenate(
        [
            lax.all_gather(cotangent[:, :split], "mp", axis=0, tiled=True),
            lax.all_gather(cotangent[:, split:], "mp", axis=0, tiled=True),
        ],
        axis=1,
    )

    inputs = block_input.astype(jnp.float32)
    normed_one, standard_one, factor_one = norm_forward(inputs, ln1_gain, ln1_bias)
    first = normed_one.astype(jnp.bfloat16)
    queries = (
        jnp.dot(first, w_query, preferred_element_type=jnp.float32) + query_bias
    ).astype(jnp.bfloat16)
    keyval = jnp.dot(first, w_keyval, preferred_element_type=jnp.float32)
    keyval = (keyval + jnp.concatenate([jnp.zeros_like(value_bias), value_bias])).astype(
        jnp.bfloat16
    )
    member_float = (
        clusters.T[:, None, :] == jnp.arange(CLUSTERS, dtype=jnp.int32)[None, :, None]
    ).astype(jnp.float32)
    membership = member_float.astype(jnp.bfloat16)
    query_sums = jnp.einsum(
        "hct,thd->hcd",
        membership,
        queries.reshape(tok_rows, head_count, head_dim),
        preferred_element_type=jnp.float32,
    )
    cluster_sizes = jnp.sum(member_float, axis=2)
    packed = keyval.reshape(tok_rows, 2, group_size, local_heads * head_dim)

    arrived = lax.all_to_all(packed, "mp", split_axis=2, concat_axis=0, tiled=True)
    sums_and_sizes = scatter_sum(
        jnp.concatenate([query_sums, cluster_sizes[:, :, None]], axis=2), group_size
    )

    query_sums = sums_and_sizes[:, :, :head_dim]
    cluster_sizes = sums_and_sizes[:, :, head_dim]
    divisor = jnp.maximum(cluster_sizes, 1.0)
    centroids = (query_sums / divisor[:, :, None]).astype(jnp.bfloat16)
    length = arrived.shape[0]
    key_rows = arrived[:, 0, 0].reshape(length, local_heads, head_dim)
    value_rows = arrived[:, 1, 0].reshape(length, local_heads, head_dim)
    scores = score_scale * jnp.einsum(
        "hcd,jhd->hcj", centroids, key_rows, preferred_element_type=jnp.float32
    )
    score_peak = jnp.max(scores, axis=-1, keepdims=True)
    exponent = jnp.exp(scores - score_peak)
    denominator = jnp.sum(exponent, axis=-1, keepdims=True)
    probs = exponent / denominator
    logsum = score_peak + jnp.log(denominator)
    summary = jnp.einsum(
        "hcj,jhd->hcd",
        probs.astype(jnp.bfloat16),
        value_rows,
        preferred_element_type=jnp.float32,
    ).astype(jnp.bfloat16)

    everyone = broadcast_gather(summary, group_size)

    spread = (
        jnp.einsum("hct,hcd->thd", membership, everyone, preferred_element_type=jnp.float32)
        .astype(jnp.bfloat16)
        .reshape(tok_rows, model_width)
    )
    attended = jnp.dot(spread, w_out, preferred_element_type=jnp.float32) + out_bias
    middle = inputs + attended
    normed_two, standard_two, factor_two = norm_forward(middle, ln2_gain, ln2_bias)
    second = normed_two.astype(jnp.bfloat16)
    residual = lax.optimization_barrier(middle + down_bias)

    gathered = lax.all_gather(second, "mp", axis=0, tiled=True)

    before = jnp.dot(gathered, w_up, preferred_element_type=jnp.float32) + up_bias.astype(
        jnp.float32
    )
    activated, gelu_slope = gelu_parts(before)
    hidden = activated.astype(jnp.bfloat16)
    grad_hidden = jnp.einsum("td,fd->tf", grad_rows, w_down, preferred_element_type=jnp.float32)
    grad_before = (grad_hidden * gelu_slope).astype(jnp.bfloat16)
    grad_second = lax.psum_scatter(
        jnp.einsum("tf,df->td", grad_before, w_up, preferred_element_type=jnp.float32).astype(
            jnp.bfloat16
        ),
        "mp",
        scatter_dimension=0,
        tiled=True,
    ).astype(jnp.float32)

    out_partial = jnp.dot(hidden, w_down, preferred_element_type=jnp.float32)

    upstream = cotangent.astype(jnp.float32)
    grad_down_bias = jnp.sum(upstream, axis=0)
    grad_down_t = jnp.einsum("td,tf->df", grad_rows, hidden, preferred_element_type=jnp.float32)
    bias_part = jnp.sum(grad_before.astype(jnp.float32), axis=0)
    grad_up = jnp.einsum("td,tf->df", gathered, grad_before, preferred_element_type=jnp.float32)
    grad_up_bias = lax.dynamic_update_slice(
        jnp.zeros((group_size * bias_part.shape[0],), jnp.float32),
        bias_part,
        (lax.axis_index("mp") * bias_part.shape[0],),
    )

    scores_again = score_scale * jnp.einsum(
        "hcd,jhd->hcj", centroids, key_rows, preferred_element_type=jnp.float32
    )
    probs_again = jnp.exp(scores_again - logsum)

    middle_norm_grad, grad_gain_two, grad_shift_two = norm_backward(
        grad_second, standard_two, factor_two, ln2_gain
    )
    grad_middle = upstream + middle_norm_grad
    attn_grad = grad_middle.astype(jnp.bfloat16)
    grad_out_bias = jnp.sum(attn_grad.astype(jnp.float32), axis=0)
    grad_w_out = jnp.einsum("td,te->de", spread, attn_grad, preferred_element_type=jnp.float32)
    grad_spread = jnp.einsum(
        "te,de->td", attn_grad, w_out, preferred_element_type=jnp.float32
    ).astype(jnp.bfloat16)
    summary_grad = jnp.einsum(
        "hct,thd->hcd",
        membership,
        grad_spread.reshape(tok_rows, head_count, head_dim),
        preferred_element_type=jnp.float32,
    )

    ff_grads = lax.psum_scatter(
        jnp.stack([grad_up, grad_down_t, grad_w_out]), "dp", scatter_dimension=1, tiled=True
    )

    summary_grad = shift_sum(summary_grad, group_size).astype(jnp.bfloat16)

    grad_values = jnp.einsum(
        "hcj,hcd->jhd",
        probs_again.astype(jnp.bfloat16),
        summary_grad,
        preferred_element_type=jnp.float32,
    )
    half_width = local_heads * head_dim
    values_out = grad_values.astype(jnp.bfloat16).reshape(group_size, tok_rows, half_width)

    values_in = shift_exchange(values_out, group_size)

    grad_probs = jnp.einsum(
        "hcd,jhd->hcj", summary_grad, value_rows, preferred_element_type=jnp.float32
    )
    grad_scores = probs_again * (
        grad_probs - jnp.sum(probs_again * grad_probs, axis=-1, keepdims=True)
    )
    grad_scores = grad_scores.astype(jnp.bfloat16)
    grad_centroids = (
        score_scale
        * jnp.einsum("hcj,jhd->hcd", grad_scores, key_rows, preferred_element_type=jnp.float32)
    ).astype(jnp.bfloat16)
    grad_keys = score_scale * jnp.einsum(
        "hcj,hcd->jhd", grad_scores, centroids, preferred_element_type=jnp.float32
    )
    per_member = (grad_centroids.astype(jnp.float32) / divisor[:, :, None]).astype(
        jnp.bfloat16
    )
    member_rows = per_member.size // half_width
    outgoing = jnp.concatenate(
        [
            grad_keys.astype(jnp.bfloat16).reshape(group_size, tok_rows, half_width),
            jnp.broadcast_to(
                per_member.reshape(1, member_rows, half_width),
                (group_size, member_rows, half_width),
            ),
        ],
        axis=1,
    )

    incoming = shift_exchange(outgoing, group_size)

    out_pieces, _ = lax.optimization_barrier((out_partial.astype(jnp.bfloat16), incoming))
    result = shift_sum(out_pieces, group_size)
    block_output = (residual + result).astype(jnp.bfloat16)

    keys_back = incoming[:, :tok_rows].transpose(1, 0, 2).reshape(tok_rows, model_width)
    values_back = values_in.transpose(1, 0, 2).reshape(tok_rows, model_width)
    grad_keyval = jnp.concatenate([keys_back, values_back], axis=1)
    all_member = (
        incoming[:, tok_rows:].reshape(head_count, CLUSTERS, head_dim).astype(jnp.float32)
    )
    grad_queries = jnp.einsum(
        "hct,hcd->thd", member_float, all_member, precision=lax.Precision.HIGHEST
    )
    grad_queries = grad_queries.reshape(tok_rows, model_width).astype(jnp.bfloat16)
    grad_query_bias = jnp.sum(grad_queries.astype(jnp.float32), axis=0)
    grad_value_bias = jnp.sum(grad_keyval[:, model_width:].astype(jnp.float32), axis=0)
    grad_w_attn = jnp.einsum(
        "td,te->de",
        first,
        jnp.concatenate([grad_queries, grad_keyval], axis=1),
        preferred_element_type=jnp.float32,
    )
    grad_first = jnp.einsum("te,de->td", grad_queries, w_query, preferred_element_type=jnp.float32)
    grad_first = grad_first + jnp.einsum(
        "te,de->td", grad_keyval, w_keyval, preferred_element_type=jnp.float32
    )
    input_norm_grad, grad_gain_one, grad_shift_one = norm_backward(
        grad_first, standard_one, factor_one, ln1_gain
    )
    input_grad = grad_middle + input_norm_grad
    vectors = jnp.stack(
        [
            grad_gain_one,
            grad_shift_one,
            grad_query_bias,
            grad_value_bias,
            grad_out_bias,
            grad_gain_two,
            grad_shift_two,
            grad_down_bias,
        ],
        axis=1,
    )
    up_bias_cols = grad_up_bias.reshape(model_width, -1)
    small_grads = jnp.concatenate([vectors, up_bias_cols], axis=1)

    dp_reduced = lax.psum_scatter(grad_w_attn, "dp", scatter_dimension=0, tiled=True)
    dp_rows = dp_reduced.shape[0]
    small_sum = lax.dynamic_slice_in_dim(
        lax.psum(small_grads, "dp"), lax.axis_index("dp") * dp_rows, dp_rows, 0
    )
    reduced = shift_sum(jnp.concatenate([dp_reduced, ff_grads[2], small_sum], axis=1), group_size)
    up_share = ff_grads[0]
    down_share = ff_grads[1].T
    col = 0
    pieces = []
    for width in (model_width, 2 * model_width, model_width):
        pieces.append(reduced[:, col : col + width])
        col += width
    vec = [reduced[:, col + i] for i in range(8)]
    col += 8
    up_bias_share = reduced[:, col:].reshape(-1)
    return (
        block_output,
        input_grad,
        vec[0],
        vec[1],
        pieces[0],
        vec[2],
        pieces[1],
        vec[3],
        pieces[2],
        vec[4],
        vec[5],
        vec[6],
        up_share,
        up_bias_share,
        down_share,
        vec[7],
    )


def solution(mesh):
    placed = (
        P(("dp", "mp"), None),
        P(("dp", "mp"), None),
        P(),
        P(),
        P(),
        P(),
        P(),
        P(),
        P(),
        P(),
        P(),
        P(),
        P(None, "mp"),
        P("mp"),
        P("mp", None),
        P(),
        P(("dp", "mp"), None),
    )
    return jax.shard_map(
        block_body,
        mesh=mesh,
        in_specs=placed,
        out_specs=(
            P(("dp", "mp"), None),
            P(("dp", "mp"), None),
            P(("dp", "mp")),
            P(("dp", "mp")),
            P(("dp", "mp"), None),
            P(("dp", "mp")),
            P(("dp", "mp"), None),
            P(("dp", "mp")),
            P(("dp", "mp"), None),
            P(("dp", "mp")),
            P(("dp", "mp")),
            P(("dp", "mp")),
            P("dp", "mp"),
            P(("dp", "mp")),
            P("mp", "dp"),
            P(("dp", "mp")),
        ),
        check_vma=False,
    )
```

```python
import math

import jax
import jax.numpy as jnp
from jax import lax
from jax.sharding import PartitionSpec as P


CLUSTERS = 100


epsilon = 1e-05


def norm_forward(inputs, gain_vec, offset):
    center = inputs - jnp.mean(inputs, axis=-1, keepdims=True)
    factor = lax.rsqrt(jnp.mean(center * center, axis=-1, keepdims=True) + epsilon)
    standard = center * factor
    return (standard * gain_vec + offset, standard, factor)


def norm_backward(upstream, standard, factor, gain_vec):
    scaled = upstream * gain_vec
    centred = scaled - jnp.mean(scaled, axis=-1, keepdims=True)
    centred = centred - standard * jnp.mean(scaled * standard, axis=-1, keepdims=True)
    return (factor * centred, jnp.sum(upstream * standard, axis=0), jnp.sum(upstream, axis=0))


def gelu_parts(before):
    cumulative = 0.5 * (1.0 + jax.scipy.special.erf(before / math.sqrt(2.0)))
    density = jnp.exp(-0.5 * before * before) / math.sqrt(2.0 * math.pi)
    return (before * cumulative, cumulative + before * density)


def shift_sum(partial, group_size):
    me = lax.axis_index("mp")
    pieces = partial.reshape((group_size, -1) + partial.shape[1:])
    total = lax.dynamic_index_in_dim(pieces, me, 0, keepdims=False).astype(jnp.float32)
    for step in range(1, group_size):
        sent = lax.dynamic_index_in_dim(
            pieces, jnp.remainder(me + step, group_size), 0, keepdims=False
        )
        moved = lax.ppermute(
            sent, "mp", [(i, (i + step) % group_size) for i in range(group_size)]
        )
        total = total + moved.astype(jnp.float32)
    return total


def shift_exchange(pieces, group_size):
    me = lax.axis_index("mp")
    out = jnp.zeros_like(pieces)
    out = lax.dynamic_update_index_in_dim(
        out, lax.dynamic_index_in_dim(pieces, me, 0, keepdims=False), me, 0
    )
    for step in range(1, group_size):
        sent = lax.dynamic_index_in_dim(
            pieces, jnp.remainder(me + step, group_size), 0, keepdims=False
        )
        moved = lax.ppermute(
            sent, "mp", [(i, (i + step) % group_size) for i in range(group_size)]
        )
        out = lax.dynamic_update_index_in_dim(
            out, moved, jnp.remainder(me + group_size - step, group_size), 0
        )
    return out


def broadcast_gather(local, group_size):
    me = lax.axis_index("mp")
    out = jnp.zeros((group_size,) + local.shape, local.dtype)
    out = lax.dynamic_update_index_in_dim(out, local, me, 0)
    for step in range(1, group_size):
        moved = lax.ppermute(
            local, "mp", [(i, (i + step) % group_size) for i in range(group_size)]
        )
        out = lax.dynamic_update_index_in_dim(
            out, moved, jnp.remainder(me + group_size - step, group_size), 0
        )
    return out.reshape((group_size * local.shape[0],) + local.shape[1:])


def block_body(
    block_input,
    clusters,
    ln1_gain,
    ln1_bias,
    w_query,
    query_bias,
    w_keyval,
    value_bias,
    w_out,
    out_bias,
    ln2_gain,
    ln2_bias,
    w_up,
    up_bias,
    w_down,
    down_bias,
    cotangent,
):
    group_size = lax.axis_size("mp")
    tok_rows = block_input.shape[0]
    model_width = block_input.shape[1]
    head_count = clusters.shape[1]
    head_dim = model_width // head_count
    local_heads = head_count // group_size
    score_scale = float(head_dim) ** (-0.5)

    split = model_width // 2
    grad_rows = jnp.concatenate(
        [
            lax.all_gather(cotangent[:, :split], "mp", axis=0, tiled=True),
            lax.all_gather(cotangent[:, split:], "mp", axis=0, tiled=True),
        ],
        axis=1,
    )

    inputs = block_input.astype(jnp.float32)
    normed_one, standard_one, factor_one = norm_forward(inputs, ln1_gain, ln1_bias)
    first = normed_one.astype(jnp.bfloat16)
    queries = (
        jnp.dot(first, w_query, preferred_element_type=jnp.float32) + query_bias
    ).astype(jnp.bfloat16)
    keyval = jnp.dot(first, w_keyval, preferred_element_type=jnp.float32)
    keyval = (keyval + jnp.concatenate([jnp.zeros_like(value_bias), value_bias])).astype(
        jnp.bfloat16
    )
    member_float = (
        clusters.T[:, None, :] == jnp.arange(CLUSTERS, dtype=jnp.int32)[None, :, None]
    ).astype(jnp.float32)
    membership = member_float.astype(jnp.bfloat16)
    query_sums = jnp.einsum(
        "hct,thd->hcd",
        membership,
        queries.reshape(tok_rows, head_count, head_dim),
        preferred_element_type=jnp.float32,
    )
    cluster_sizes = jnp.sum(member_float, axis=2)
    half_width = local_heads * head_dim
    packed = (
        keyval.reshape(tok_rows, 2, group_size, half_width)
        .transpose(2, 0, 1, 3)
        .reshape(group_size, tok_rows, 2 * half_width)
    )

    arrived = shift_exchange(packed, group_size)
    sums_and_sizes = shift_sum(
        jnp.concatenate([query_sums, cluster_sizes[:, :, None]], axis=2), group_size
    )

    query_sums = sums_and_sizes[:, :, :head_dim]
    cluster_sizes = sums_and_sizes[:, :, head_dim]
    divisor = jnp.maximum(cluster_sizes, 1.0)
    centroids = (query_sums / divisor[:, :, None]).astype(jnp.bfloat16)
    length = group_size * tok_rows
    key_rows = arrived[:, :, :half_width].reshape(length, local_heads, head_dim)
    value_rows = arrived[:, :, half_width:].reshape(length, local_heads, head_dim)
    scores = score_scale * jnp.einsum(
        "hcd,jhd->hcj", centroids, key_rows, preferred_element_type=jnp.float32
    )
    score_peak = jnp.max(scores, axis=-1, keepdims=True)
    exponent = jnp.exp(scores - score_peak)
    denominator = jnp.sum(exponent, axis=-1, keepdims=True)
    probs = exponent / denominator
    logsum = score_peak + jnp.log(denominator)
    summary = jnp.einsum(
        "hcj,jhd->hcd",
        probs.astype(jnp.bfloat16),
        value_rows,
        preferred_element_type=jnp.float32,
    ).astype(jnp.bfloat16)

    everyone = broadcast_gather(summary, group_size)

    spread = (
        jnp.einsum("hct,hcd->thd", membership, everyone, preferred_element_type=jnp.float32)
        .astype(jnp.bfloat16)
        .reshape(tok_rows, model_width)
    )
    attended = jnp.dot(spread, w_out, preferred_element_type=jnp.float32) + out_bias
    middle = inputs + attended
    normed_two, standard_two, factor_two = norm_forward(middle, ln2_gain, ln2_bias)
    second = normed_two.astype(jnp.bfloat16)
    residual = lax.optimization_barrier(middle + down_bias)

    gathered = lax.all_gather(second, "mp", axis=0, tiled=True)

    before = jnp.dot(gathered, w_up, preferred_element_type=jnp.float32) + up_bias.astype(
        jnp.float32
    )
    activated, gelu_slope = gelu_parts(before)
    hidden = activated.astype(jnp.bfloat16)
    grad_hidden = jnp.einsum("td,fd->tf", grad_rows, w_down, preferred_element_type=jnp.float32)
    grad_before = (grad_hidden * gelu_slope).astype(jnp.bfloat16)
    grad_second = lax.psum_scatter(
        jnp.einsum("tf,df->td", grad_before, w_up, preferred_element_type=jnp.float32).astype(
            jnp.bfloat16
        ),
        "mp",
        scatter_dimension=0,
        tiled=True,
    ).astype(jnp.float32)

    out_partial = jnp.dot(hidden, w_down, preferred_element_type=jnp.float32)

    upstream = cotangent.astype(jnp.float32)
    grad_down_bias = jnp.sum(upstream, axis=0)
    grad_down_t = jnp.einsum("td,tf->df", grad_rows, hidden, preferred_element_type=jnp.float32)
    bias_part = jnp.sum(grad_before.astype(jnp.float32), axis=0)
    grad_up = jnp.einsum("td,tf->df", gathered, grad_before, preferred_element_type=jnp.float32)
    grad_up_bias = lax.dynamic_update_slice(
        jnp.zeros((group_size * bias_part.shape[0],), jnp.float32),
        bias_part,
        (lax.axis_index("mp") * bias_part.shape[0],),
    )

    scores_again = score_scale * jnp.einsum(
        "hcd,jhd->hcj", centroids, key_rows, preferred_element_type=jnp.float32
    )
    probs_again = jnp.exp(scores_again - logsum)

    middle_norm_grad, grad_gain_two, grad_shift_two = norm_backward(
        grad_second, standard_two, factor_two, ln2_gain
    )
    grad_middle = upstream + middle_norm_grad
    attn_grad = grad_middle.astype(jnp.bfloat16)
    grad_out_bias = jnp.sum(attn_grad.astype(jnp.float32), axis=0)
    grad_w_out = jnp.einsum("td,te->de", spread, attn_grad, preferred_element_type=jnp.float32)
    grad_spread = jnp.einsum(
        "te,de->td", attn_grad, w_out, preferred_element_type=jnp.float32
    ).astype(jnp.bfloat16)
    summary_grad = jnp.einsum(
        "hct,thd->hcd",
        membership,
        grad_spread.reshape(tok_rows, head_count, head_dim),
        preferred_element_type=jnp.float32,
    )

    ff_grads = lax.psum_scatter(
        jnp.stack([grad_up, grad_down_t, grad_w_out]), "dp", scatter_dimension=1, tiled=True
    )

    summary_grad = shift_sum(summary_grad, group_size).astype(jnp.bfloat16)

    grad_values = jnp.einsum(
        "hcj,hcd->jhd",
        probs_again.astype(jnp.bfloat16),
        summary_grad,
        preferred_element_type=jnp.float32,
    )
    half_width = local_heads * head_dim
    values_out = grad_values.astype(jnp.bfloat16).reshape(group_size, tok_rows, half_width)

    values_in = shift_exchange(values_out, group_size)

    grad_probs = jnp.einsum(
        "hcd,jhd->hcj", summary_grad, value_rows, preferred_element_type=jnp.float32
    )
    grad_scores = probs_again * (
        grad_probs - jnp.sum(probs_again * grad_probs, axis=-1, keepdims=True)
    )
    grad_scores = grad_scores.astype(jnp.bfloat16)
    grad_centroids = (
        score_scale
        * jnp.einsum("hcj,jhd->hcd", grad_scores, key_rows, preferred_element_type=jnp.float32)
    ).astype(jnp.bfloat16)
    grad_keys = score_scale * jnp.einsum(
        "hcj,hcd->jhd", grad_scores, centroids, preferred_element_type=jnp.float32
    )
    per_member = (grad_centroids.astype(jnp.float32) / divisor[:, :, None]).astype(
        jnp.bfloat16
    )
    member_rows = per_member.size // half_width
    outgoing = jnp.concatenate(
        [
            grad_keys.astype(jnp.bfloat16).reshape(group_size, tok_rows, half_width),
            jnp.broadcast_to(
                per_member.reshape(1, member_rows, half_width),
                (group_size, member_rows, half_width),
            ),
        ],
        axis=1,
    )

    incoming = shift_exchange(outgoing, group_size)

    out_pieces, _ = lax.optimization_barrier((out_partial.astype(jnp.bfloat16), incoming))
    result = shift_sum(out_pieces, group_size)
    block_output = (residual + result).astype(jnp.bfloat16)

    keys_back = incoming[:, :tok_rows].transpose(1, 0, 2).reshape(tok_rows, model_width)
    values_back = values_in.transpose(1, 0, 2).reshape(tok_rows, model_width)
    grad_keyval = jnp.concatenate([keys_back, values_back], axis=1)
    all_member = (
        incoming[:, tok_rows:].reshape(head_count, CLUSTERS, head_dim).astype(jnp.float32)
    )
    grad_queries = jnp.einsum(
        "hct,hcd->thd", member_float, all_member, precision=lax.Precision.HIGHEST
    )
    grad_queries = grad_queries.reshape(tok_rows, model_width).astype(jnp.bfloat16)
    grad_query_bias = jnp.sum(grad_queries.astype(jnp.float32), axis=0)
    grad_value_bias = jnp.sum(grad_keyval[:, model_width:].astype(jnp.float32), axis=0)
    grad_w_attn = jnp.einsum(
        "td,te->de",
        first,
        jnp.concatenate([grad_queries, grad_keyval], axis=1),
        preferred_element_type=jnp.float32,
    )
    grad_first = jnp.einsum("te,de->td", grad_queries, w_query, preferred_element_type=jnp.float32)
    grad_first = grad_first + jnp.einsum(
        "te,de->td", grad_keyval, w_keyval, preferred_element_type=jnp.float32
    )
    input_norm_grad, grad_gain_one, grad_shift_one = norm_backward(
        grad_first, standard_one, factor_one, ln1_gain
    )
    input_grad = grad_middle + input_norm_grad
    vectors = jnp.stack(
        [
            grad_gain_one,
            grad_shift_one,
            grad_query_bias,
            grad_value_bias,
            grad_out_bias,
            grad_gain_two,
            grad_shift_two,
            grad_down_bias,
        ],
        axis=1,
    )
    up_bias_cols = grad_up_bias.reshape(model_width, -1)
    small_grads = jnp.concatenate([vectors, up_bias_cols], axis=1)

    dp_reduced = lax.psum_scatter(grad_w_attn, "dp", scatter_dimension=0, tiled=True)
    dp_rows = dp_reduced.shape[0]
    small_sum = lax.dynamic_slice_in_dim(
        lax.psum(small_grads, "dp"), lax.axis_index("dp") * dp_rows, dp_rows, 0
    )
    reduced = shift_sum(jnp.concatenate([dp_reduced, ff_grads[2], small_sum], axis=1), group_size)
    up_share = ff_grads[0]
    down_share = ff_grads[1].T
    col = 0
    pieces = []
    for width in (model_width, 2 * model_width, model_width):
        pieces.append(reduced[:, col : col + width])
        col += width
    vec = [reduced[:, col + i] for i in range(8)]
    col += 8
    up_bias_share = reduced[:, col:].reshape(-1)
    return (
        block_output,
        input_grad,
        vec[0],
        vec[1],
        pieces[0],
        vec[2],
        pieces[1],
        vec[3],
        pieces[2],
        vec[4],
        vec[5],
        vec[6],
        up_share,
        up_bias_share,
        down_share,
        vec[7],
    )


def solution(mesh):
    placed = (
        P(("dp", "mp"), None),
        P(("dp", "mp"), None),
        P(),
        P(),
        P(),
        P(),
        P(),
        P(),
        P(),
        P(),
        P(),
        P(),
        P(None, "mp"),
        P("mp"),
        P("mp", None),
        P(),
        P(("dp", "mp"), None),
    )
    return jax.shard_map(
        block_body,
        mesh=mesh,
        in_specs=placed,
        out_specs=(
            P(("dp", "mp"), None),
            P(("dp", "mp"), None),
            P(("dp", "mp")),
            P(("dp", "mp")),
            P(("dp", "mp"), None),
            P(("dp", "mp")),
            P(("dp", "mp"), None),
            P(("dp", "mp")),
            P(("dp", "mp"), None),
            P(("dp", "mp")),
            P(("dp", "mp")),
            P(("dp", "mp")),
            P("dp", "mp"),
            P(("dp", "mp")),
            P("mp", "dp"),
            P(("dp", "mp")),
        ),
        check_vma=False,
    )
```

```python
import math

import jax
import jax.numpy as jnp
from jax import lax
from jax.sharding import PartitionSpec as P


CLUSTERS = 100


epsilon = 1e-05


def norm_forward(inputs, gain_vec, offset):
    center = inputs - jnp.mean(inputs, axis=-1, keepdims=True)
    factor = lax.rsqrt(jnp.mean(center * center, axis=-1, keepdims=True) + epsilon)
    standard = center * factor
    return (standard * gain_vec + offset, standard, factor)


def norm_backward(upstream, standard, factor, gain_vec):
    scaled = upstream * gain_vec
    centred = scaled - jnp.mean(scaled, axis=-1, keepdims=True)
    centred = centred - standard * jnp.mean(scaled * standard, axis=-1, keepdims=True)
    return (factor * centred, jnp.sum(upstream * standard, axis=0), jnp.sum(upstream, axis=0))


def gelu_parts(before):
    cumulative = 0.5 * (1.0 + jax.scipy.special.erf(before / math.sqrt(2.0)))
    density = jnp.exp(-0.5 * before * before) / math.sqrt(2.0 * math.pi)
    return (before * cumulative, cumulative + before * density)


def shift_sum(partial, group_size):
    me = lax.axis_index("mp")
    pieces = partial.reshape((group_size, -1) + partial.shape[1:])
    total = lax.dynamic_index_in_dim(pieces, me, 0, keepdims=False).astype(jnp.float32)
    for step in range(1, group_size):
        sent = lax.dynamic_index_in_dim(
            pieces, jnp.remainder(me + step, group_size), 0, keepdims=False
        )
        moved = lax.ppermute(
            sent, "mp", [(i, (i + step) % group_size) for i in range(group_size)]
        )
        total = total + moved.astype(jnp.float32)
    return total


def shift_exchange(pieces, group_size):
    me = lax.axis_index("mp")
    out = jnp.zeros_like(pieces)
    out = lax.dynamic_update_index_in_dim(
        out, lax.dynamic_index_in_dim(pieces, me, 0, keepdims=False), me, 0
    )
    for step in range(1, group_size):
        sent = lax.dynamic_index_in_dim(
            pieces, jnp.remainder(me + step, group_size), 0, keepdims=False
        )
        moved = lax.ppermute(
            sent, "mp", [(i, (i + step) % group_size) for i in range(group_size)]
        )
        out = lax.dynamic_update_index_in_dim(
            out, moved, jnp.remainder(me + group_size - step, group_size), 0
        )
    return out


def broadcast_gather(local, group_size):
    sent = jnp.broadcast_to(local[None], (group_size,) + local.shape)
    arrived = lax.all_to_all(sent, "mp", split_axis=0, concat_axis=0, tiled=True)
    return arrived.reshape((group_size * local.shape[0],) + local.shape[1:])


def block_body(
    block_input,
    clusters,
    ln1_gain,
    ln1_bias,
    w_query,
    query_bias,
    w_keyval,
    value_bias,
    w_out,
    out_bias,
    ln2_gain,
    ln2_bias,
    w_up,
    up_bias,
    w_down,
    down_bias,
    cotangent,
):
    group_size = lax.axis_size("mp")
    tok_rows = block_input.shape[0]
    model_width = block_input.shape[1]
    head_count = clusters.shape[1]
    head_dim = model_width // head_count
    local_heads = head_count // group_size
    score_scale = float(head_dim) ** (-0.5)

    split = model_width // 2
    grad_rows = jnp.concatenate(
        [
            lax.all_gather(cotangent[:, :split], "mp", axis=0, tiled=True),
            lax.all_gather(cotangent[:, split:], "mp", axis=0, tiled=True),
        ],
        axis=1,
    )

    inputs = block_input.astype(jnp.float32)
    normed_one, standard_one, factor_one = norm_forward(inputs, ln1_gain, ln1_bias)
    first = normed_one.astype(jnp.bfloat16)
    queries = (
        jnp.dot(first, w_query, preferred_element_type=jnp.float32) + query_bias
    ).astype(jnp.bfloat16)
    keyval = jnp.dot(first, w_keyval, preferred_element_type=jnp.float32)
    keyval = (keyval + jnp.concatenate([jnp.zeros_like(value_bias), value_bias])).astype(
        jnp.bfloat16
    )
    member_float = (
        clusters.T[:, None, :] == jnp.arange(CLUSTERS, dtype=jnp.int32)[None, :, None]
    ).astype(jnp.float32)
    membership = member_float.astype(jnp.bfloat16)
    query_sums = jnp.einsum(
        "hct,thd->hcd",
        membership,
        queries.reshape(tok_rows, head_count, head_dim),
        preferred_element_type=jnp.float32,
    )
    cluster_sizes = jnp.sum(member_float, axis=2)
    packed = keyval.reshape(tok_rows, 2, group_size, local_heads * head_dim)

    arrived = lax.all_to_all(packed, "mp", split_axis=2, concat_axis=0, tiled=True)
    sums_and_sizes = shift_sum(
        jnp.concatenate([query_sums, cluster_sizes[:, :, None]], axis=2), group_size
    )

    query_sums = sums_and_sizes[:, :, :head_dim]
    cluster_sizes = sums_and_sizes[:, :, head_dim]
    divisor = jnp.maximum(cluster_sizes, 1.0)
    centroids = (query_sums / divisor[:, :, None]).astype(jnp.bfloat16)
    length = arrived.shape[0]
    key_rows = arrived[:, 0, 0].reshape(length, local_heads, head_dim)
    value_rows = arrived[:, 1, 0].reshape(length, local_heads, head_dim)
    scores = score_scale * jnp.einsum(
        "hcd,jhd->hcj", centroids, key_rows, preferred_element_type=jnp.float32
    )
    score_peak = jnp.max(scores, axis=-1, keepdims=True)
    exponent = jnp.exp(scores - score_peak)
    denominator = jnp.sum(exponent, axis=-1, keepdims=True)
    probs = exponent / denominator
    logsum = score_peak + jnp.log(denominator)
    summary = jnp.einsum(
        "hcj,jhd->hcd",
        probs.astype(jnp.bfloat16),
        value_rows,
        preferred_element_type=jnp.float32,
    ).astype(jnp.bfloat16)

    everyone = broadcast_gather(summary, group_size)

    spread = (
        jnp.einsum("hct,hcd->thd", membership, everyone, preferred_element_type=jnp.float32)
        .astype(jnp.bfloat16)
        .reshape(tok_rows, model_width)
    )
    attended = jnp.dot(spread, w_out, preferred_element_type=jnp.float32) + out_bias
    middle = inputs + attended
    normed_two, standard_two, factor_two = norm_forward(middle, ln2_gain, ln2_bias)
    second = normed_two.astype(jnp.bfloat16)
    residual = lax.optimization_barrier(middle + down_bias)

    gathered = lax.all_gather(second, "mp", axis=0, tiled=True)

    before = jnp.dot(gathered, w_up, preferred_element_type=jnp.float32) + up_bias.astype(
        jnp.float32
    )
    activated, gelu_slope = gelu_parts(before)
    hidden = activated.astype(jnp.bfloat16)
    grad_hidden = jnp.einsum("td,fd->tf", grad_rows, w_down, preferred_element_type=jnp.float32)
    grad_before = (grad_hidden * gelu_slope).astype(jnp.bfloat16)
    grad_second = lax.psum_scatter(
        jnp.einsum("tf,df->td", grad_before, w_up, preferred_element_type=jnp.float32).astype(
            jnp.bfloat16
        ),
        "mp",
        scatter_dimension=0,
        tiled=True,
    ).astype(jnp.float32)

    out_partial = jnp.dot(hidden, w_down, preferred_element_type=jnp.float32)

    upstream = cotangent.astype(jnp.float32)
    grad_down_bias = jnp.sum(upstream, axis=0)
    grad_down_t = jnp.einsum("td,tf->df", grad_rows, hidden, preferred_element_type=jnp.float32)
    bias_part = jnp.sum(grad_before.astype(jnp.float32), axis=0)
    grad_up = jnp.einsum("td,tf->df", gathered, grad_before, preferred_element_type=jnp.float32)
    grad_up_bias = lax.dynamic_update_slice(
        jnp.zeros((group_size * bias_part.shape[0],), jnp.float32),
        bias_part,
        (lax.axis_index("mp") * bias_part.shape[0],),
    )

    scores_again = score_scale * jnp.einsum(
        "hcd,jhd->hcj", centroids, key_rows, preferred_element_type=jnp.float32
    )
    probs_again = jnp.exp(scores_again - logsum)

    middle_norm_grad, grad_gain_two, grad_shift_two = norm_backward(
        grad_second, standard_two, factor_two, ln2_gain
    )
    grad_middle = upstream + middle_norm_grad
    attn_grad = grad_middle.astype(jnp.bfloat16)
    grad_out_bias = jnp.sum(attn_grad.astype(jnp.float32), axis=0)
    grad_w_out = jnp.einsum("td,te->de", spread, attn_grad, preferred_element_type=jnp.float32)
    grad_spread = jnp.einsum(
        "te,de->td", attn_grad, w_out, preferred_element_type=jnp.float32
    ).astype(jnp.bfloat16)
    summary_grad = jnp.einsum(
        "hct,thd->hcd",
        membership,
        grad_spread.reshape(tok_rows, head_count, head_dim),
        preferred_element_type=jnp.float32,
    )

    ff_grads = lax.psum_scatter(
        jnp.stack([grad_up, grad_down_t, grad_w_out]), "dp", scatter_dimension=1, tiled=True
    )

    summary_grad = shift_sum(summary_grad, group_size).astype(jnp.bfloat16)

    grad_values = jnp.einsum(
        "hcj,hcd->jhd",
        probs_again.astype(jnp.bfloat16),
        summary_grad,
        preferred_element_type=jnp.float32,
    )
    half_width = local_heads * head_dim
    values_out = grad_values.astype(jnp.bfloat16).reshape(group_size, tok_rows, half_width)

    values_in = shift_exchange(values_out, group_size)

    grad_probs = jnp.einsum(
        "hcd,jhd->hcj", summary_grad, value_rows, preferred_element_type=jnp.float32
    )
    grad_scores = probs_again * (
        grad_probs - jnp.sum(probs_again * grad_probs, axis=-1, keepdims=True)
    )
    grad_scores = grad_scores.astype(jnp.bfloat16)
    grad_centroids = (
        score_scale
        * jnp.einsum("hcj,jhd->hcd", grad_scores, key_rows, preferred_element_type=jnp.float32)
    ).astype(jnp.bfloat16)
    grad_keys = score_scale * jnp.einsum(
        "hcj,hcd->jhd", grad_scores, centroids, preferred_element_type=jnp.float32
    )
    per_member = (grad_centroids.astype(jnp.float32) / divisor[:, :, None]).astype(
        jnp.bfloat16
    )
    member_rows = per_member.size // half_width
    outgoing = jnp.concatenate(
        [
            grad_keys.astype(jnp.bfloat16).reshape(group_size, tok_rows, half_width),
            jnp.broadcast_to(
                per_member.reshape(1, member_rows, half_width),
                (group_size, member_rows, half_width),
            ),
        ],
        axis=1,
    )

    incoming = shift_exchange(outgoing, group_size)

    out_pieces, _ = lax.optimization_barrier((out_partial.astype(jnp.bfloat16), incoming))
    result = shift_sum(out_pieces, group_size)
    block_output = (residual + result).astype(jnp.bfloat16)

    keys_back = incoming[:, :tok_rows].transpose(1, 0, 2).reshape(tok_rows, model_width)
    values_back = values_in.transpose(1, 0, 2).reshape(tok_rows, model_width)
    grad_keyval = jnp.concatenate([keys_back, values_back], axis=1)
    all_member = (
        incoming[:, tok_rows:].reshape(head_count, CLUSTERS, head_dim).astype(jnp.float32)
    )
    grad_queries = jnp.einsum(
        "hct,hcd->thd", member_float, all_member, precision=lax.Precision.HIGHEST
    )
    grad_queries = grad_queries.reshape(tok_rows, model_width).astype(jnp.bfloat16)
    grad_query_bias = jnp.sum(grad_queries.astype(jnp.float32), axis=0)
    grad_value_bias = jnp.sum(grad_keyval[:, model_width:].astype(jnp.float32), axis=0)
    grad_w_attn = jnp.einsum(
        "td,te->de",
        first,
        jnp.concatenate([grad_queries, grad_keyval], axis=1),
        preferred_element_type=jnp.float32,
    )
    grad_first = jnp.einsum("te,de->td", grad_queries, w_query, preferred_element_type=jnp.float32)
    grad_first = grad_first + jnp.einsum(
        "te,de->td", grad_keyval, w_keyval, preferred_element_type=jnp.float32
    )
    input_norm_grad, grad_gain_one, grad_shift_one = norm_backward(
        grad_first, standard_one, factor_one, ln1_gain
    )
    input_grad = grad_middle + input_norm_grad
    vectors = jnp.stack(
        [
            grad_gain_one,
            grad_shift_one,
            grad_query_bias,
            grad_value_bias,
            grad_out_bias,
            grad_gain_two,
            grad_shift_two,
            grad_down_bias,
        ],
        axis=1,
    )
    up_bias_cols = grad_up_bias.reshape(model_width, -1)
    small_grads = jnp.concatenate([vectors, up_bias_cols], axis=1)

    dp_reduced = lax.psum_scatter(grad_w_attn, "dp", scatter_dimension=0, tiled=True)
    dp_rows = dp_reduced.shape[0]
    small_sum = lax.dynamic_slice_in_dim(
        lax.psum(small_grads, "dp"), lax.axis_index("dp") * dp_rows, dp_rows, 0
    )
    reduced = shift_sum(jnp.concatenate([dp_reduced, ff_grads[2], small_sum], axis=1), group_size)
    up_share = ff_grads[0]
    down_share = ff_grads[1].T
    col = 0
    pieces = []
    for width in (model_width, 2 * model_width, model_width):
        pieces.append(reduced[:, col : col + width])
        col += width
    vec = [reduced[:, col + i] for i in range(8)]
    col += 8
    up_bias_share = reduced[:, col:].reshape(-1)
    return (
        block_output,
        input_grad,
        vec[0],
        vec[1],
        pieces[0],
        vec[2],
        pieces[1],
        vec[3],
        pieces[2],
        vec[4],
        vec[5],
        vec[6],
        up_share,
        up_bias_share,
        down_share,
        vec[7],
    )


def solution(mesh):
    placed = (
        P(("dp", "mp"), None),
        P(("dp", "mp"), None),
        P(),
        P(),
        P(),
        P(),
        P(),
        P(),
        P(),
        P(),
        P(),
        P(),
        P(None, "mp"),
        P("mp"),
        P("mp", None),
        P(),
        P(("dp", "mp"), None),
    )
    return jax.shard_map(
        block_body,
        mesh=mesh,
        in_specs=placed,
        out_specs=(
            P(("dp", "mp"), None),
            P(("dp", "mp"), None),
            P(("dp", "mp")),
            P(("dp", "mp")),
            P(("dp", "mp"), None),
            P(("dp", "mp")),
            P(("dp", "mp"), None),
            P(("dp", "mp")),
            P(("dp", "mp"), None),
            P(("dp", "mp")),
            P(("dp", "mp")),
            P(("dp", "mp")),
            P("dp", "mp"),
            P(("dp", "mp")),
            P("mp", "dp"),
            P(("dp", "mp")),
        ),
        check_vma=False,
    )
```

```python
import math

import jax
import jax.numpy as jnp
from jax import lax
from jax.sharding import PartitionSpec as P


CLUSTERS = 100


epsilon = 1e-05


def norm_forward(inputs, gain_vec, offset):
    center = inputs - jnp.mean(inputs, axis=-1, keepdims=True)
    factor = lax.rsqrt(jnp.mean(center * center, axis=-1, keepdims=True) + epsilon)
    standard = center * factor
    return (standard * gain_vec + offset, standard, factor)


def norm_backward(upstream, standard, factor, gain_vec):
    scaled = upstream * gain_vec
    centred = scaled - jnp.mean(scaled, axis=-1, keepdims=True)
    centred = centred - standard * jnp.mean(scaled * standard, axis=-1, keepdims=True)
    return (factor * centred, jnp.sum(upstream * standard, axis=0), jnp.sum(upstream, axis=0))


def gelu_parts(before):
    cumulative = 0.5 * (1.0 + jax.scipy.special.erf(before / math.sqrt(2.0)))
    density = jnp.exp(-0.5 * before * before) / math.sqrt(2.0 * math.pi)
    return (before * cumulative, cumulative + before * density)


def shift_sum(partial, group_size):
    me = lax.axis_index("mp")
    pieces = partial.reshape((group_size, -1) + partial.shape[1:])
    total = lax.dynamic_index_in_dim(pieces, me, 0, keepdims=False).astype(jnp.float32)
    for step in range(1, group_size):
        sent = lax.dynamic_index_in_dim(
            pieces, jnp.remainder(me + step, group_size), 0, keepdims=False
        )
        moved = lax.ppermute(
            sent, "mp", [(i, (i + step) % group_size) for i in range(group_size)]
        )
        total = total + moved.astype(jnp.float32)
    return total


def shift_exchange(pieces, group_size):
    me = lax.axis_index("mp")
    out = jnp.zeros_like(pieces)
    out = lax.dynamic_update_index_in_dim(
        out, lax.dynamic_index_in_dim(pieces, me, 0, keepdims=False), me, 0
    )
    for step in range(1, group_size):
        sent = lax.dynamic_index_in_dim(
            pieces, jnp.remainder(me + step, group_size), 0, keepdims=False
        )
        moved = lax.ppermute(
            sent, "mp", [(i, (i + step) % group_size) for i in range(group_size)]
        )
        out = lax.dynamic_update_index_in_dim(
            out, moved, jnp.remainder(me + group_size - step, group_size), 0
        )
    return out


def broadcast_gather(local, group_size):
    me = lax.axis_index("mp")
    out = jnp.zeros((group_size,) + local.shape, local.dtype)
    out = lax.dynamic_update_index_in_dim(out, local, me, 0)
    for step in range(1, group_size):
        moved = lax.ppermute(
            local, "mp", [(i, (i + step) % group_size) for i in range(group_size)]
        )
        out = lax.dynamic_update_index_in_dim(
            out, moved, jnp.remainder(me + group_size - step, group_size), 0
        )
    return out.reshape((group_size * local.shape[0],) + local.shape[1:])


def block_body(
    block_input,
    clusters,
    ln1_gain,
    ln1_bias,
    w_query,
    query_bias,
    w_keyval,
    value_bias,
    w_out,
    out_bias,
    ln2_gain,
    ln2_bias,
    w_up,
    up_bias,
    w_down,
    down_bias,
    cotangent,
):
    group_size = lax.axis_size("mp")
    tok_rows = block_input.shape[0]
    model_width = block_input.shape[1]
    head_count = clusters.shape[1]
    head_dim = model_width // head_count
    local_heads = head_count // group_size
    score_scale = float(head_dim) ** (-0.5)

    split = model_width // 2
    grad_rows = jnp.concatenate(
        [
            lax.all_gather(cotangent[:, :split], "mp", axis=0, tiled=True),
            lax.all_gather(cotangent[:, split:], "mp", axis=0, tiled=True),
        ],
        axis=1,
    )

    inputs = block_input.astype(jnp.float32)
    normed_one, standard_one, factor_one = norm_forward(inputs, ln1_gain, ln1_bias)
    first = normed_one.astype(jnp.bfloat16)
    queries = (
        jnp.dot(first, w_query, preferred_element_type=jnp.float32) + query_bias
    ).astype(jnp.bfloat16)
    keyval = jnp.dot(first, w_keyval, preferred_element_type=jnp.float32)
    keyval = (keyval + jnp.concatenate([jnp.zeros_like(value_bias), value_bias])).astype(
        jnp.bfloat16
    )
    member_float = (
        clusters.T[:, None, :] == jnp.arange(CLUSTERS, dtype=jnp.int32)[None, :, None]
    ).astype(jnp.float32)
    membership = member_float.astype(jnp.bfloat16)
    query_sums = jnp.einsum(
        "hct,thd->hcd",
        membership,
        queries.reshape(tok_rows, head_count, head_dim),
        preferred_element_type=jnp.float32,
    )
    cluster_sizes = jnp.sum(member_float, axis=2)
    packed = keyval.reshape(tok_rows, 2, group_size, local_heads * head_dim)

    arrived = lax.all_to_all(packed, "mp", split_axis=2, concat_axis=0, tiled=True)
    sums_and_sizes = shift_sum(
        jnp.concatenate([query_sums, cluster_sizes[:, :, None]], axis=2), group_size
    )

    query_sums = sums_and_sizes[:, :, :head_dim]
    cluster_sizes = sums_and_sizes[:, :, head_dim]
    divisor = jnp.maximum(cluster_sizes, 1.0)
    centroids = (query_sums / divisor[:, :, None]).astype(jnp.bfloat16)
    length = arrived.shape[0]
    key_rows = arrived[:, 0, 0].reshape(length, local_heads, head_dim)
    value_rows = arrived[:, 1, 0].reshape(length, local_heads, head_dim)
    scores = score_scale * jnp.einsum(
        "hcd,jhd->hcj", centroids, key_rows, preferred_element_type=jnp.float32
    )
    score_peak = jnp.max(scores, axis=-1, keepdims=True)
    exponent = jnp.exp(scores - score_peak)
    denominator = jnp.sum(exponent, axis=-1, keepdims=True)
    probs = exponent / denominator
    logsum = score_peak + jnp.log(denominator)
    summary = jnp.einsum(
        "hcj,jhd->hcd",
        probs.astype(jnp.bfloat16),
        value_rows,
        preferred_element_type=jnp.float32,
    ).astype(jnp.bfloat16)

    everyone = broadcast_gather(summary, group_size)

    spread = (
        jnp.einsum("hct,hcd->thd", membership, everyone, preferred_element_type=jnp.float32)
        .astype(jnp.bfloat16)
        .reshape(tok_rows, model_width)
    )
    attended = jnp.dot(spread, w_out, preferred_element_type=jnp.float32) + out_bias
    middle = inputs + attended
    normed_two, standard_two, factor_two = norm_forward(middle, ln2_gain, ln2_bias)
    second = normed_two.astype(jnp.bfloat16)
    residual = lax.optimization_barrier(middle + down_bias)

    gathered = lax.all_gather(second, "mp", axis=0, tiled=True)

    before = jnp.dot(gathered, w_up, preferred_element_type=jnp.float32) + up_bias.astype(
        jnp.float32
    )
    activated, gelu_slope = gelu_parts(before)
    hidden = activated.astype(jnp.bfloat16)
    grad_hidden = jnp.einsum("td,fd->tf", grad_rows, w_down, preferred_element_type=jnp.float32)
    grad_before = (grad_hidden * gelu_slope).astype(jnp.bfloat16)
    grad_second = lax.psum_scatter(
        jnp.einsum("tf,df->td", grad_before, w_up, preferred_element_type=jnp.float32).astype(
            jnp.bfloat16
        ),
        "mp",
        scatter_dimension=0,
        tiled=True,
    ).astype(jnp.float32)

    out_partial = jnp.dot(hidden, w_down, preferred_element_type=jnp.float32)

    upstream = cotangent.astype(jnp.float32)
    grad_down_bias = jnp.sum(upstream, axis=0)
    grad_down_t = jnp.einsum("td,tf->df", grad_rows, hidden, preferred_element_type=jnp.float32)
    bias_part = jnp.sum(grad_before.astype(jnp.float32), axis=0)
    grad_up = jnp.einsum("td,tf->df", gathered, grad_before, preferred_element_type=jnp.float32)
    grad_up_bias = lax.dynamic_update_slice(
        jnp.zeros((group_size * bias_part.shape[0],), jnp.float32),
        bias_part,
        (lax.axis_index("mp") * bias_part.shape[0],),
    )

    scores_again = score_scale * jnp.einsum(
        "hcd,jhd->hcj", centroids, key_rows, preferred_element_type=jnp.float32
    )
    probs_again = jnp.exp(scores_again - logsum)

    middle_norm_grad, grad_gain_two, grad_shift_two = norm_backward(
        grad_second, standard_two, factor_two, ln2_gain
    )
    grad_middle = upstream + middle_norm_grad
    attn_grad = grad_middle.astype(jnp.bfloat16)
    grad_out_bias = jnp.sum(attn_grad.astype(jnp.float32), axis=0)
    grad_w_out = jnp.einsum("td,te->de", spread, attn_grad, preferred_element_type=jnp.float32)
    grad_spread = jnp.einsum(
        "te,de->td", attn_grad, w_out, preferred_element_type=jnp.float32
    ).astype(jnp.bfloat16)
    summary_grad = jnp.einsum(
        "hct,thd->hcd",
        membership,
        grad_spread.reshape(tok_rows, head_count, head_dim),
        preferred_element_type=jnp.float32,
    )

    ff_grads = lax.psum_scatter(
        jnp.stack([grad_up, grad_down_t, grad_w_out]), "dp", scatter_dimension=1, tiled=True
    )

    summary_grad = shift_sum(summary_grad, group_size).astype(jnp.bfloat16)

    grad_values = jnp.einsum(
        "hcj,hcd->jhd",
        probs_again.astype(jnp.bfloat16),
        summary_grad,
        preferred_element_type=jnp.float32,
    )
    half_width = local_heads * head_dim
    values_out = grad_values.astype(jnp.bfloat16).reshape(group_size, tok_rows, half_width)

    values_in = shift_exchange(values_out, group_size)

    grad_probs = jnp.einsum(
        "hcd,jhd->hcj", summary_grad, value_rows, preferred_element_type=jnp.float32
    )
    grad_scores = probs_again * (
        grad_probs - jnp.sum(probs_again * grad_probs, axis=-1, keepdims=True)
    )
    grad_scores = grad_scores.astype(jnp.bfloat16)
    grad_centroids = (
        score_scale
        * jnp.einsum("hcj,jhd->hcd", grad_scores, key_rows, preferred_element_type=jnp.float32)
    ).astype(jnp.bfloat16)
    grad_keys = score_scale * jnp.einsum(
        "hcj,hcd->jhd", grad_scores, centroids, preferred_element_type=jnp.float32
    )
    per_member = (grad_centroids.astype(jnp.float32) / divisor[:, :, None]).astype(
        jnp.bfloat16
    )
    member_rows = per_member.size // half_width
    outgoing = jnp.concatenate(
        [
            grad_keys.astype(jnp.bfloat16).reshape(group_size, tok_rows, half_width),
            jnp.broadcast_to(
                per_member.reshape(1, member_rows, half_width),
                (group_size, member_rows, half_width),
            ),
        ],
        axis=1,
    )

    incoming = shift_exchange(outgoing, group_size)

    out_pieces, _ = lax.optimization_barrier((out_partial.astype(jnp.bfloat16), incoming))
    result = shift_sum(out_pieces, group_size)
    block_output = (residual + result).astype(jnp.bfloat16)

    keys_back = incoming[:, :tok_rows].transpose(1, 0, 2).reshape(tok_rows, model_width)
    values_back = values_in.transpose(1, 0, 2).reshape(tok_rows, model_width)
    grad_keyval = jnp.concatenate([keys_back, values_back], axis=1)
    all_member = (
        incoming[:, tok_rows:].reshape(head_count, CLUSTERS, head_dim).astype(jnp.float32)
    )
    grad_queries = jnp.einsum(
        "hct,hcd->thd", member_float, all_member, precision=lax.Precision.HIGHEST
    )
    grad_queries = grad_queries.reshape(tok_rows, model_width).astype(jnp.bfloat16)
    grad_query_bias = jnp.sum(grad_queries.astype(jnp.float32), axis=0)
    grad_value_bias = jnp.sum(grad_keyval[:, model_width:].astype(jnp.float32), axis=0)
    grad_w_attn = jnp.einsum(
        "td,te->de",
        first,
        jnp.concatenate([grad_queries, grad_keyval], axis=1),
        preferred_element_type=jnp.float32,
    )
    grad_first = jnp.einsum("te,de->td", grad_queries, w_query, preferred_element_type=jnp.float32)
    grad_first = grad_first + jnp.einsum(
        "te,de->td", grad_keyval, w_keyval, preferred_element_type=jnp.float32
    )
    input_norm_grad, grad_gain_one, grad_shift_one = norm_backward(
        grad_first, standard_one, factor_one, ln1_gain
    )
    input_grad = grad_middle + input_norm_grad
    vectors = jnp.stack(
        [
            grad_gain_one,
            grad_shift_one,
            grad_query_bias,
            grad_value_bias,
            grad_out_bias,
            grad_gain_two,
            grad_shift_two,
            grad_down_bias,
        ],
        axis=1,
    )
    up_bias_cols = grad_up_bias.reshape(model_width, -1)
    small_grads = jnp.concatenate([vectors, up_bias_cols], axis=1)

    dp_reduced = lax.psum_scatter(grad_w_attn, "dp", scatter_dimension=0, tiled=True)
    dp_rows = dp_reduced.shape[0]
    small_sum = lax.dynamic_slice_in_dim(
        lax.psum(small_grads, "dp"), lax.axis_index("dp") * dp_rows, dp_rows, 0
    )
    reduced = shift_sum(jnp.concatenate([dp_reduced, ff_grads[2], small_sum], axis=1), group_size)
    up_share = ff_grads[0]
    down_share = ff_grads[1].T
    col = 0
    pieces = []
    for width in (model_width, 2 * model_width, model_width):
        pieces.append(reduced[:, col : col + width])
        col += width
    vec = [reduced[:, col + i] for i in range(8)]
    col += 8
    up_bias_share = reduced[:, col:].reshape(-1)
    return (
        block_output,
        input_grad,
        vec[0],
        vec[1],
        pieces[0],
        vec[2],
        pieces[1],
        vec[3],
        pieces[2],
        vec[4],
        vec[5],
        vec[6],
        up_share,
        up_bias_share,
        down_share,
        vec[7],
    )


def solution(mesh):
    placed = (
        P(("dp", "mp"), None),
        P(("dp", "mp"), None),
        P(),
        P(),
        P(),
        P(),
        P(),
        P(),
        P(),
        P(),
        P(),
        P(),
        P(None, "mp"),
        P("mp"),
        P("mp", None),
        P(),
        P(("dp", "mp"), None),
    )
    return jax.shard_map(
        block_body,
        mesh=mesh,
        in_specs=placed,
        out_specs=(
            P(("dp", "mp"), None),
            P(("dp", "mp"), None),
            P(("dp", "mp")),
            P(("dp", "mp")),
            P(("dp", "mp"), None),
            P(("dp", "mp")),
            P(("dp", "mp"), None),
            P(("dp", "mp")),
            P(("dp", "mp"), None),
            P(("dp", "mp")),
            P(("dp", "mp")),
            P(("dp", "mp")),
            P("dp", "mp"),
            P(("dp", "mp")),
            P("mp", "dp"),
            P(("dp", "mp")),
        ),
        check_vma=False,
    )
```
